32 devices in a mesh: dp: 16 (over z, y, x), tensor: 2 (over core).
Axes of the slice: x: 2, y: 2, z: 4, core: 2. Of those that a mesh axis runs over, the one named last changes fastest.
Arguments:
- residual: bfloat16 [16384, 1536], P(('dp', 'tensor')), may hold values from -6 to 6
- cotangent: bfloat16 [16384, 1536], P(('dp', 'tensor')), may hold values from -6 to 6
- segment_ids: int32 [16, 1024], P('dp'), may hold values from 0 to 3, never falling along the last dimension, each value on 1 to 800 neighbouring positions
- adapter_ids: int32 [16], P('dp'), may hold values from 0 to 7
- conv_gain: float32 [1536], replicated, may hold values from 0.1 to 1.9
- proj_in: bfloat16 [1536, 3, 1536], P('dp', None, 'tensor'), may hold values from -0.15625 to 0.15625
- conv_taps: bfloat16 [3, 1536], P(None, 'tensor'), may hold values from -3.5 to 3.5
- proj_out: bfloat16 [1536, 1536], P('dp', 'tensor'), may hold values from -0.15625 to 0.15625
- ffn_gain: float32 [1536], replicated, may hold values from 0.1 to 1.9
- gate_up: bfloat16 [1536, 2, 6912], P('dp', None, 'tensor'), may hold values from -0.15625 to 0.15625
- proj_down: bfloat16 [1536, 6912], P('dp', 'tensor'), may hold values from -0.109375 to 0.109375
- in_shrink: bfloat16 [1536, 8, 16], replicated, may hold values from -0.15625 to 0.15625
- input_lift_weight: bfloat16 [8, 16, 3, 1536], P(None, None, None, 'tensor'), may hold values from -1 to 1
- output_reduce_weight: bfloat16 [1536, 8, 16], P('tensor'), may hold values from -0.15625 to 0.15625
- output_lift_weight: bfloat16 [8, 16, 1536], replicated, may hold values from -1 to 1
- ffn_reduce_weight: bfloat16 [1536, 2, 8, 16], replicated, may hold values from -0.15625 to 0.15625
- ffn_expand: bfloat16 [2, 8, 16, 6912], P(None, None, None, 'tensor'), may hold values from -1 to 1
- down_shrink: bfloat16 [6912, 8, 16], P('tensor'), may hold values from -0.078125 to 0.078125
- down_lift_weight: bfloat16 [8, 16, 1536], replicated, may hold values from -1 to 1
Outputs:
- block_output: bfloat16 [16384, 1536], P(('dp', 'tensor'))
- grad_residual: bfloat16 [16384, 1536], P(('dp', 'tensor'))
- grad_in_shrink: float32 [1536, 8, 16], replicated
- grad_in_expand: float32 [8, 16, 3, 1536], P(None, None, None, 'tensor')
- grad_out_shrink: float32 [1536, 8, 16], P('tensor')
- grad_out_expand: float32 [8, 16, 1536], replicated
- grad_ffn_shrink: float32 [1536, 2, 8, 16], replicated
- grad_ffn_expand: float32 [2, 8, 16, 6912], P(None, None, None, 'tensor')
- grad_down_shrink: float32 [6912, 8, 16], P('tensor')
- grad_down_expand: float32 [8, 16, 1536], replicated
The draws below stay inside these ranges and needn't reach their ends.
Inputs may be any that keep to these rules, and one draw needn't show every extreme that they name: `segment_ids`: within a sequence the ids never fall; each sequence holds four documents of 1 to 800 tokens, one exactly 800.
All inputs are finite; a program needn't handle non-finite values.
Results may differ from the reference program's by a relative error of at most 0.015.
Values may be sent and summed in bfloat16 or wider, within the bound.
A program may use at most 320 MiB of HBM per device.

```python
import math
import jax
import jax.numpy as jnp
import numpy as np
from jax import lax

D = 1536
FF = 6912
ADAPTER_COUNT = 8
ADAPTER_RANK = 16
LEN = 1024
DOC_MOST = 800
SEQS = 16
TOKENS = 16384


def plant(drawn, stream_key, low, high):
    dims = drawn.shape
    spot = [jax.random.randint(jax.random.fold_in(stream_key, axis), (), 0, dims[axis]) for axis in range(len(dims))]
    drawn = drawn.at[tuple(spot)].set(low)
    longest = dims.index(max(dims))
    spot[longest] = (spot[longest] + 1) % dims[longest]
    return drawn.at[tuple(spot)].set(high)


def block_scale(key, dims, cuts, low, high):
    def one(axis_at, parts):
        draws = jax.random.uniform(jax.random.fold_in(jax.random.fold_in(key, 6), axis_at), (parts,), jnp.float32, low / len(cuts), high / len(cuts))
        return jnp.repeat(jnp.exp(draws), dims[axis_at] // parts).reshape((-1,) + (1,) * (len(dims) - axis_at - 1))

    level = one(*cuts[0])
    for cut in cuts[1:]:
        level = level * one(*cut)
    return level


def length_profile(number_of, total, bound, slope):
    loads = [(1 << 20) // math.isqrt(grade ** slope) + 1 for grade in range(2, number_of + 1)]
    rest, given = total - bound - (number_of - 1), [1] * (number_of - 1)
    while rest > 0:
        free = [i for i in range(number_of - 1) if given[i] < bound]
        whole, remaining = sum([loads[i] for i in free]), rest
        for i in free:
            addition = min(bound - given[i], max(1, remaining * loads[i] // whole), rest)
            given[i] = given[i] + addition
            rest = rest - addition
    return np.array([bound] + given)


def uneven_parts(stream_key, amount, total, limit, skew):
    if amount == 2:
        one = jax.random.randint(stream_key, (), max(1, total - limit), min(limit, total - 1) + 1)
        return jnp.stack([one, total - one])
    lengths = jnp.asarray(length_profile(amount, total, limit, skew), jnp.int32)
    twos = (amount - 1) // 2
    giver, sink = lengths[1:1 + 2 * twos:2], lengths[2:2 + 2 * twos:2]
    slack = jnp.minimum(giver - 1, limit - sink)
    shifted = jax.random.randint(jax.random.fold_in(stream_key, 1), (twos,), 0, 1 << 20) % (slack + 1)
    lengths = lengths.at[1:1 + 2 * twos:2].set(giver - shifted).at[2:2 + 2 * twos:2].set(sink + shifted)
    return lengths[jax.random.permutation(jax.random.fold_in(stream_key, 2), amount)]


def gaussian(own_key, extent, deviation, most, cuts=(), kind=jnp.bfloat16):
    level = block_scale(own_key, extent, cuts, -0.22, 0.18) if cuts else 1.0
    values = jax.random.normal(own_key, extent, jnp.float32) * deviation * level
    return jnp.minimum(jnp.maximum(values, -most), most).astype(kind)


def setup_inputs(seed: int = 0) -> dict:
    seeds = jax.random.split(jax.random.key(seed), 20)
    return {
        "residual": gaussian(seeds[0], (TOKENS, D), 1.0, 6.0, ((0, 32),)),
        "cotangent": gaussian(seeds[1], (TOKENS, D), 1.0, 6.0, ((0, 32),)),
        "segment_ids": jax.vmap(lambda own: jnp.searchsorted(jnp.cumsum(uneven_parts(own, 4, LEN, DOC_MOST, 1)), jnp.arange(LEN), side="right"))(jax.random.split(seeds[2], SEQS)).reshape((SEQS, LEN)).astype(jnp.int32),
        "adapter_ids": plant(jax.random.randint(seeds[3], (SEQS,), 0, ADAPTER_COUNT), jax.random.fold_in(seeds[3], 1), 0, ADAPTER_COUNT - 1).astype(jnp.int32),
        "conv_gain": jnp.clip(1.0 + 0.18 * jax.random.normal(seeds[4], (D,), jnp.float32), 0.1, 1.9),
        "proj_in": gaussian(seeds[5], (D, 3, D), D ** -0.5, 0.15625, ((0, 16), (2, 2))),
        "conv_taps": gaussian(seeds[6], (3, D), 3 ** -0.5, 3.5, ((1, 2),)),
        "proj_out": gaussian(seeds[7], (D, D), D ** -0.5, 0.15625, ((0, 16), (1, 2))),
        "ffn_gain": jnp.clip(1.0 + 0.18 * jax.random.normal(seeds[8], (D,), jnp.float32), 0.1, 1.9),
        "gate_up": gaussian(seeds[9], (D, 2, FF), D ** -0.5, 0.15625, ((0, 16), (2, 2))),
        "proj_down": gaussian(seeds[10], (D, FF), (FF // 2) ** -0.5, 0.109375, ((0, 16), (1, 2))),
        "in_shrink": gaussian(seeds[11], (D, ADAPTER_COUNT, ADAPTER_RANK), D ** -0.5, 0.15625),
        "input_lift_weight": gaussian(seeds[12], (ADAPTER_COUNT, ADAPTER_RANK, 3, D), (2 * ADAPTER_RANK) ** -0.5, 1.0, ((3, 2),)),
        "output_reduce_weight": gaussian(seeds[13], (D, ADAPTER_COUNT, ADAPTER_RANK), D ** -0.5, 0.15625, ((0, 2),)),
        "output_lift_weight": gaussian(seeds[14], (ADAPTER_COUNT, ADAPTER_RANK, D), (2 * ADAPTER_RANK) ** -0.5, 1.0),
        "ffn_reduce_weight": gaussian(seeds[15], (D, 2, ADAPTER_COUNT, ADAPTER_RANK), D ** -0.5, 0.15625),
        "ffn_expand": gaussian(seeds[16], (2, ADAPTER_COUNT, ADAPTER_RANK, FF), (2 * ADAPTER_RANK) ** -0.5, 1.0, ((3, 2),)),
        "down_shrink": gaussian(seeds[17], (FF, ADAPTER_COUNT, ADAPTER_RANK), FF ** -0.5, 0.078125, ((0, 2),)),
        "down_lift_weight": gaussian(seeds[18], (ADAPTER_COUNT, ADAPTER_RANK, D), (2 * ADAPTER_RANK) ** -0.5, 1.0),
    }


EPSILON = 1e-05

@jax.custom_vjp
def low(v):
    return lax.optimization_barrier(v.astype(jnp.bfloat16)).astype(jnp.float32)

@jax.custom_vjp
def low_back(v):
    return v

def low_keep(v):
    return (low(v), None)

def low_pass(kept, grad):
    return (grad,)

def back_keep(v):
    return (v, None)

def back_low(kept, grad):
    return (low(grad),)
low.defvjp(low_keep, low_pass)
low_back.defvjp(back_keep, back_low)

def matmul(left, right):
    return jnp.dot(left, right, precision=lax.Precision.HIGHEST)

def rms_scale(values, gain):
    return values * lax.rsqrt(lax.optimization_barrier(jnp.mean(values * values, axis=-1, keepdims=True)) + EPSILON) * gain

def masked_rows(codes, adapter_selector, groups):
    count = codes.shape[0]
    return (codes.reshape(count, groups, ADAPTER_COUNT, ADAPTER_RANK) * adapter_selector[:, None, :, None]).reshape(count, groups * ADAPTER_COUNT * ADAPTER_RANK)

def lagged(values, lag):
    return jnp.pad(values, ((lag, 0), (0, 0)))[:values.shape[0]]

def forward_block(rows, adapter_selector, first_same_sequence, second_same_sequence, conv_gain, proj_in, conv_taps, proj_out, ffn_gain, gate_up, proj_down, in_shrink, input_lift_weight, output_reduce_weight, output_lift_weight, ffn_reduce_weight, ffn_expand, down_shrink, down_lift_weight):
    first_norm = low(rms_scale(rows, conv_gain))
    input_latent = low(masked_rows(matmul(first_norm, in_shrink.reshape(D, ADAPTER_COUNT * ADAPTER_RANK)), adapter_selector, 1))
    residual_lanes = matmul(first_norm, proj_in.reshape(D, 3 * D)) + matmul(input_latent, input_lift_weight.reshape(ADAPTER_COUNT * ADAPTER_RANK, 3 * D))
    residual_lanes = low_back(residual_lanes).reshape(-1, 3, D)
    bgate, cgate, xval = (residual_lanes[:, 0], residual_lanes[:, 1], residual_lanes[:, 2])
    product = bgate * xval
    mixed = conv_taps[0] * product + conv_taps[1] * lagged(product, 1) * first_same_sequence + conv_taps[2] * lagged(product, 2) * second_same_sequence
    convolved_rows = low(cgate * mixed)
    branch = low_back(matmul(convolved_rows, proj_out.T))
    output_latent = low(low_back(masked_rows(matmul(convolved_rows, output_reduce_weight.reshape(D, ADAPTER_COUNT * ADAPTER_RANK)), adapter_selector, 1)))
    second_input = rows + branch + matmul(output_latent, output_lift_weight.reshape(ADAPTER_COUNT * ADAPTER_RANK, D))
    second_norm = low(rms_scale(second_input, ffn_gain))
    ffn_latent = low(masked_rows(matmul(second_norm, ffn_reduce_weight.reshape(D, 2 * ADAPTER_COUNT * ADAPTER_RANK)), adapter_selector, 2))
    expand = ffn_expand.reshape(2, ADAPTER_COUNT * ADAPTER_RANK, FF)
    base_sum = matmul(second_norm, gate_up.reshape(D, 2 * FF))
    gate_sum = base_sum[:, :FF] + matmul(ffn_latent[:, :ADAPTER_COUNT * ADAPTER_RANK], expand[0])
    up_sum = base_sum[:, FF:] + matmul(ffn_latent[:, ADAPTER_COUNT * ADAPTER_RANK:], expand[1])
    both = low_back(jnp.concatenate([gate_sum, up_sum], axis=1))
    gate_sum, up_sum = (both[:, :FF], both[:, FF:])
    activation_rows = low(jax.nn.silu(gate_sum) * up_sum)
    down_branch = low_back(matmul(activation_rows, proj_down.T))
    down_latent = low(low_back(masked_rows(matmul(activation_rows, down_shrink.reshape(FF, ADAPTER_COUNT * ADAPTER_RANK)), adapter_selector, 1)))
    return second_input + down_branch + matmul(down_latent, down_lift_weight.reshape(ADAPTER_COUNT * ADAPTER_RANK, D))

def reference(residual, cotangent, segment_ids, adapter_ids, conv_gain, proj_in, conv_taps, proj_out, ffn_gain, gate_up, proj_down, in_shrink, input_lift_weight, output_reduce_weight, output_lift_weight, ffn_reduce_weight, ffn_expand, down_shrink, down_lift_weight):
    frozen_params = tuple((item.astype(jnp.float32) for item in (conv_gain, proj_in, conv_taps, proj_out, ffn_gain, gate_up, proj_down)))
    adapters = tuple((item.astype(jnp.float32) for item in (in_shrink, input_lift_weight, output_reduce_weight, output_lift_weight, ffn_reduce_weight, ffn_expand, down_shrink, down_lift_weight)))
    inputs = residual.astype(jnp.float32).reshape(SEQS, LEN, D)
    grads_in = cotangent.astype(jnp.float32).reshape(SEQS, LEN, D)

    def one_sequence(totals, item):
        rows, grad_rows, segments, which = item
        shift_one = jnp.pad(segments, (1, 0), constant_values=-1)[:LEN]
        shift_two = jnp.pad(segments, (2, 0), constant_values=-1)[:LEN]
        first_same_sequence = (segments == shift_one).astype(jnp.float32)[:, None]
        second_same_sequence = (segments == shift_two).astype(jnp.float32)[:, None]
        adapter_selector = jnp.broadcast_to((jnp.arange(ADAPTER_COUNT, dtype=jnp.int32) == which).astype(jnp.float32)[None, :], (LEN, ADAPTER_COUNT))

        def execute_block(input_rows, *adapter_params):
            return forward_block(input_rows, adapter_selector, first_same_sequence, second_same_sequence, *frozen_params, *adapter_params)
        result, pullback = jax.vjp(execute_block, rows, *adapters)
        grads = pullback(grad_rows)
        totals = tuple((total + part for total, part in zip(totals, grads[1:])))
        return (totals, (result.astype(jnp.bfloat16), grads[0].astype(jnp.bfloat16)))
    initial = tuple((jnp.zeros(item.shape, jnp.float32) for item in adapters))
    totals, (outputs, grad_rows) = lax.scan(one_sequence, initial, (inputs, grads_in, segment_ids, adapter_ids))
    return (outputs.reshape(TOKENS, D), grad_rows.reshape(TOKENS, D), totals[0], totals[1], totals[2], totals[3], totals[4], totals[5], totals[6], totals[7])
```

```python
import functools

import jax
import jax.numpy as jnp
from jax import lax
from jax.experimental import pallas as pl
from jax.experimental.pallas import tpu as pltpu
from jax.sharding import PartitionSpec as P

MESH = pl.DeviceIdType.MESH


def split_ring(count):
    if count % 16 == 0 and count >= 16:
        return (4, count // 8, 2)
    return (count, 1, 1)


def position(index, dims):
    return (index // (dims[1] * dims[2]), (index // dims[2]) % dims[1], index % dims[2])


def flat(spot, dims):
    return (spot[0] * dims[1] + spot[1]) * dims[2] + spot[2]


def routes(column_ranges, dims):
    out = []
    for which, first, width in column_ranges:
        half = (width // 256) * 128
        out.append((which, first, half, (0, 1, 2)))
        out.append((which, first + half, width - half, (0, 2, 1)))
    return out


def cut(which, columns, step):
    return [(which, i, min(step, columns - i)) for i in range(0, columns, step)]


class Gather:
    def __init__(self, dims, spot, shards, wholes, pieces, send, recv):
        self.dims, self.spot, self.shards, self.wholes = dims, spot, shards, wholes
        self.pieces, self.send, self.recv = pieces, send, recv

    def stage(self, piece, step):
        which, first, width, order = self.pieces[piece]
        axis = order[step]
        columns = pl.ds(first, width)
        place = tuple(
            slice(None) if other in order[:step] else self.spot[other] for other in range(3)
        )
        whole = self.wholes[which].at[place + (slice(None), columns)]
        base = sum(self.dims[other] - 1 for other in order[:step])
        copies = []
        for offset in range(1, self.dims[axis]):
            peer = list(self.spot)
            peer[axis] = lax.rem(self.spot[axis] + offset, self.dims[axis])
            source = self.shards[which].at[:, columns] if step == 0 else whole
            copies.append(
                pltpu.make_async_remote_copy(
                    src_ref=source,
                    dst_ref=whole,
                    send_sem=self.send.at[piece, base + offset - 1],
                    recv_sem=self.recv.at[piece, base + offset - 1],
                    device_id={"dp": flat(peer, self.dims)},
                    device_id_type=MESH,
                )
            )
        return copies

    def start(self, piece, step):
        for copy in self.stage(piece, step):
            copy.start()

    def arrive(self, piece, step):
        for copy in self.stage(piece, step):
            copy.wait_recv()

    def drain(self, piece):
        for step in range(3):
            for copy in self.stage(piece, step):
                copy.wait_send()

    def greet(self):
        barrier = pltpu.get_barrier_semaphore()
        count = 0
        for axis in range(3):
            for offset in range(1, self.dims[axis]):
                peer = list(self.spot)
                peer[axis] = lax.rem(self.spot[axis] + offset, self.dims[axis])
                pl.semaphore_signal(
                    barrier, inc=1, device_id={"dp": flat(peer, self.dims)}, device_id_type=MESH
                )
                count += 1
        pl.semaphore_wait(barrier, count)


def gather_kernel(dims, pieces, amount, *refs):
    shards, wholes = refs[:amount], refs[amount : 2 * amount]
    held = refs[2 * amount : 3 * amount]
    send, recv, local = refs[3 * amount :]
    spot = position(lax.axis_index("dp"), dims)
    gather = Gather(dims, spot, shards, wholes, pieces, send, recv)
    gather.greet()
    loads = [
        pltpu.make_async_copy(shards[i], held[i], local.at[i]) for i in range(amount)
    ]
    for load in loads:
        load.start()
    for piece in range(len(pieces)):
        gather.start(piece, 0)
    stores = []
    for i in range(amount):
        loads[i].wait()
        store = pltpu.make_async_copy(held[i], wholes[i].at[spot], local.at[i])
        store.start()
        stores.append(store)
    for store in stores:
        store.wait()
    for piece in range(0, len(pieces) + 2, 2):
        for part in (piece, piece + 1):
            if part < len(pieces):
                gather.arrive(part, 0)
                gather.start(part, 1)
        for part in (piece - 2, piece - 1):
            if 0 <= part < len(pieces):
                gather.arrive(part, 1)
                gather.start(part, 2)
    for piece in range(len(pieces)):
        gather.arrive(piece, 2)
        gather.drain(piece)


def gather_all(shards, column_ranges, count):
    dims = split_ring(count)
    pieces = routes(column_ranges, dims)
    amount = len(shards)
    lanes = sum(d - 1 for d in dims)
    anywhere = pl.BlockSpec(memory_space=pl.ANY)
    outs = pl.pallas_call(
        functools.partial(gather_kernel, dims, pieces, amount),
        out_shape=[jax.ShapeDtypeStruct(dims + s.shape, s.dtype) for s in shards],
        in_specs=[anywhere] * amount,
        out_specs=[anywhere] * amount,
        scratch_shapes=[pltpu.VMEM(s.shape, s.dtype) for s in shards]
        + [
            pltpu.SemaphoreType.DMA((len(pieces), lanes)),
            pltpu.SemaphoreType.DMA((len(pieces), lanes)),
            pltpu.SemaphoreType.DMA((amount,)),
        ],
        compiler_params=pltpu.CompilerParams(collective_id=0, has_side_effects=True),
    )(*shards)
    return [o.reshape(count * s.shape[0], s.shape[1]) for o, s in zip(outs, shards)]

ADAPTER_COUNT = 8
ADAPTER_RANK = 16


EPSILON = 1e-05


def contract_simple(left, right):
    return jnp.dot(left, right, preferred_element_type=jnp.float32)


def contract_against(left, right):
    return lax.dot_general(
        left, right, (((1,), (1,)), ((), ())), preferred_element_type=jnp.float32
    )


def dot_over_rows(left, right):
    return lax.dot_general(
        left, right, (((0,), (0,)), ((), ())), preferred_element_type=jnp.float32
    )


def split_pair(values):
    upper = values.astype(jnp.bfloat16)
    lower = (values - upper.astype(jnp.float32)).astype(jnp.bfloat16)
    return (upper, lower)


def broad_contract(values, right):
    upper, lower = split_pair(values)
    return contract_against(upper, right) + contract_against(lower, right)


def wide_over_rows(left, values):
    upper, lower = split_pair(values)
    return dot_over_rows(left, upper) + dot_over_rows(left, lower)


def normalize(values, gain):
    factor = lax.rsqrt(jnp.mean(values * values, axis=-1, keepdims=True) + EPSILON)
    return (values * factor * gain, factor)


def normalize_back(values, factor, gain, grad):
    unit = values * factor
    scaled = grad * gain
    return factor * (scaled - unit * jnp.mean(scaled * unit, axis=-1, keepdims=True))


def masked_rows(codes, adapter_selector, groups):
    count = codes.shape[0]
    return (
        codes.reshape(count, groups, ADAPTER_COUNT, ADAPTER_RANK)
        * adapter_selector[:, None, :, None]
    ).reshape(count, groups * ADAPTER_COUNT * ADAPTER_RANK)


def lagged(values, lag):
    return jnp.pad(values, ((0, 0), (lag, 0), (0, 0)))[:, : values.shape[1]]


def leading(values, lag):
    return jnp.pad(values, ((0, 0), (0, lag), (0, 0)))[:, lag:]


def same_document(segment_ids, lag):
    shifted = jnp.pad(segment_ids, ((0, 0), (lag, 0)), constant_values=-1)[
        :, : segment_ids.shape[1]
    ]
    return (segment_ids == shifted).astype(jnp.float32)[:, :, None]


def per_device(
    residual,
    cotangent,
    segment_ids,
    adapter_ids,
    conv_gain,
    proj_in,
    conv_taps,
    proj_out,
    ffn_gain,
    gate_up,
    proj_down,
    in_shrink,
    input_lift_weight,
    output_reduce_weight,
    output_lift_weight,
    ffn_reduce_weight,
    ffn_expand,
    down_shrink,
    down_lift_weight,
):
    quarter = residual.shape[0]
    sequences, length = segment_ids.shape
    row_count = sequences * length
    hidden_width = residual.shape[1]
    channel_count = proj_in.shape[2]
    hidden_shard = gate_up.shape[2]
    first_row = lax.axis_index("tensor") * quarter
    adapter_row = (
        adapter_ids[:, None] == jnp.arange(ADAPTER_COUNT, dtype=jnp.int32)[None, :]
    ).astype(jnp.float32)
    adapter_selector_total = jnp.broadcast_to(
        adapter_row[:, None, :], (sequences, length, ADAPTER_COUNT)
    ).reshape(row_count, ADAPTER_COUNT)
    local_adapter_selector = lax.dynamic_slice_in_dim(adapter_selector_total, first_row, quarter, 0)
    first_same_sequence = same_document(segment_ids, 1)
    second_same_sequence = same_document(segment_ids, 2)
    tap_values = conv_taps.astype(jnp.float32)
    local_input = residual.astype(jnp.float32)
    normed_one, factor_one = normalize(local_input, conv_gain)
    first_norm = lax.all_gather(normed_one.astype(jnp.bfloat16), "tensor", axis=0, tiled=True)
    count = lax.axis_size("dp")
    shard_rows = proj_in.shape[0]
    hidden_shard_columns = proj_down.shape[1]
    shards = [
        jnp.concatenate([proj_in.reshape(shard_rows, 3 * channel_count), proj_out], axis=1),
        gate_up.reshape(shard_rows, 2 * hidden_shard_columns),
        proj_down,
    ]
    ranges = cut(0, 4 * channel_count, 512)
    ranges += cut(1, 2 * hidden_shard_columns, 1152)
    ranges += cut(2, hidden_shard_columns, 1152)
    io_full, gu_rows, down_full = gather_all(shards, ranges, count)
    in_full, out_full = io_full[:, : 3 * channel_count], io_full[:, 3 * channel_count :]
    gu_full = gu_rows.reshape(hidden_width, 2, hidden_shard_columns)
    input_latent = masked_rows(
        contract_simple(first_norm, in_shrink.reshape(hidden_width, ADAPTER_COUNT * ADAPTER_RANK)),
        adapter_selector_total,
        1,
    ).astype(jnp.bfloat16)
    input_projection_matrix = in_full.reshape(hidden_width, 3 * channel_count)
    input_adapter_term = input_lift_weight.reshape(ADAPTER_COUNT * ADAPTER_RANK, 3 * channel_count)
    residual_lanes = contract_simple(first_norm, input_projection_matrix) + contract_simple(
        input_latent, input_adapter_term
    )
    residual_lanes = residual_lanes.reshape(sequences, length, 3, channel_count)
    bgate, cgate, xval = (residual_lanes[:, :, 0], residual_lanes[:, :, 1], residual_lanes[:, :, 2])
    product = bgate * xval
    mixed_sum = (
        tap_values[0] * product
        + tap_values[1] * lagged(product, 1) * first_same_sequence
        + tap_values[2] * lagged(product, 2) * second_same_sequence
    )
    convolved_rows = (cgate * mixed_sum).astype(jnp.bfloat16).reshape(row_count, channel_count)
    output_adapter_input = output_reduce_weight.reshape(channel_count, ADAPTER_COUNT * ADAPTER_RANK)
    branch_part = contract_against(convolved_rows, out_full)
    latent_slice = contract_simple(convolved_rows, output_adapter_input)
    local_branch, code_own = (
        lax.psum_scatter(branch_part, "tensor", scatter_dimension=0, tiled=True),
        lax.psum_scatter(latent_slice, "tensor", scatter_dimension=0, tiled=True),
    )
    output_latent = masked_rows(code_own, local_adapter_selector, 1).astype(jnp.bfloat16)
    output_adapter_term = output_lift_weight.reshape(ADAPTER_COUNT * ADAPTER_RANK, hidden_width)
    second_input = local_input + local_branch + contract_simple(output_latent, output_adapter_term)
    normed_two, factor_two = normalize(second_input, ffn_gain)
    norm_local = normed_two.astype(jnp.bfloat16)
    expand_weights, down_reduce_weight = (ffn_expand, down_shrink)
    second_norm = lax.all_gather(norm_local, "tensor", axis=0, tiled=True)
    hidden_rows = gu_full.shape[2]
    ffn_adapter_input = ffn_reduce_weight.reshape(hidden_width, 2 * ADAPTER_COUNT * ADAPTER_RANK)
    ffn_latent = masked_rows(
        contract_simple(second_norm, ffn_adapter_input), adapter_selector_total, 2
    ).astype(jnp.bfloat16)
    expand = expand_weights.reshape(2, ADAPTER_COUNT * ADAPTER_RANK, hidden_rows)
    base_sum = contract_simple(second_norm, gu_full.reshape(hidden_width, 2 * hidden_rows))
    gate_sum = base_sum[:, :hidden_rows] + contract_simple(
        ffn_latent[:, : ADAPTER_COUNT * ADAPTER_RANK], expand[0]
    )
    up_sum = base_sum[:, hidden_rows:] + contract_simple(
        ffn_latent[:, ADAPTER_COUNT * ADAPTER_RANK :], expand[1]
    )
    sigmoid_gate = jax.nn.sigmoid(gate_sum)
    silu_gate = gate_sum * sigmoid_gate
    activation_rows = (silu_gate * up_sum).astype(jnp.bfloat16)
    down_adapter_input = down_reduce_weight.reshape(hidden_rows, ADAPTER_COUNT * ADAPTER_RANK)
    down_part = contract_against(activation_rows, down_full)
    down_latent_slice = contract_simple(activation_rows, down_adapter_input)
    local_down, down_code_own = (
        lax.psum_scatter(
            down_part.astype(jnp.bfloat16), "tensor", scatter_dimension=0, tiled=True
        ).astype(jnp.float32),
        lax.psum_scatter(
            down_latent_slice.astype(jnp.bfloat16), "tensor", scatter_dimension=0, tiled=True
        ).astype(jnp.float32),
    )
    down_latent = masked_rows(down_code_own, local_adapter_selector, 1).astype(jnp.bfloat16)
    down_adapter_term = down_lift_weight.reshape(ADAPTER_COUNT * ADAPTER_RANK, hidden_width)
    block_output = (
        second_input + local_down + contract_simple(down_latent, down_adapter_term)
    ).astype(jnp.bfloat16)
    grad_top = cotangent.astype(jnp.float32)
    grad_down_expand = dot_over_rows(down_latent, cotangent)
    down_latent_gradient = masked_rows(
        contract_against(cotangent, down_adapter_term), local_adapter_selector, 1
    ).astype(jnp.bfloat16)
    grad_branch_all, down_latent_gradient_total = (
        lax.all_gather(cotangent, "tensor", axis=0, tiled=True),
        lax.all_gather(down_latent_gradient, "tensor", axis=0, tiled=True),
    )
    grad_activation = contract_simple(grad_branch_all, down_full) + contract_against(
        down_latent_gradient_total, down_adapter_input
    )
    grad_down_shrink = dot_over_rows(activation_rows, down_latent_gradient_total)
    grad_gate = grad_activation * up_sum * sigmoid_gate * (1.0 + gate_sum * (1.0 - sigmoid_gate))
    grad_up = grad_activation * silu_gate
    grad_gu = jnp.concatenate([grad_gate, grad_up], axis=1).astype(jnp.bfloat16)
    ffn_latent_gradient = masked_rows(
        jnp.concatenate(
            [
                contract_against(grad_gu[:, :hidden_rows], expand[0]),
                contract_against(grad_gu[:, hidden_rows:], expand[1]),
            ],
            axis=1,
        ),
        adapter_selector_total,
        2,
    )
    grad_ffn_expand = jnp.stack(
        [
            dot_over_rows(ffn_latent[:, : ADAPTER_COUNT * ADAPTER_RANK], grad_gu[:, :hidden_rows]),
            dot_over_rows(ffn_latent[:, ADAPTER_COUNT * ADAPTER_RANK :], grad_gu[:, hidden_rows:]),
        ]
    )
    grad_ffn_shrink = wide_over_rows(second_norm, ffn_latent_gradient)
    grad_norm_two = contract_against(
        grad_gu, gu_full.reshape(hidden_width, 2 * hidden_rows)
    ) + broad_contract(ffn_latent_gradient, ffn_adapter_input)
    grad_norm_two_own = lax.psum_scatter(grad_norm_two, "tensor", scatter_dimension=0, tiled=True)
    second_input_gradient = grad_top + normalize_back(
        second_input, factor_two, ffn_gain, grad_norm_two_own
    )
    grad_out_expand = wide_over_rows(output_latent, second_input_gradient)
    output_latent_gradient = masked_rows(
        broad_contract(second_input_gradient, output_adapter_term), local_adapter_selector, 1
    ).astype(jnp.bfloat16)
    grad_branch_conv, output_latent_gradient_total = (
        lax.all_gather(second_input_gradient.astype(jnp.bfloat16), "tensor", axis=0, tiled=True),
        lax.all_gather(output_latent_gradient, "tensor", axis=0, tiled=True),
    )
    input_projection_matrix = in_full.reshape(hidden_width, 3 * channel_count)
    grad_conv_out = contract_simple(grad_branch_conv, out_full) + contract_against(
        output_latent_gradient_total, output_adapter_input
    )
    grad_out_shrink = dot_over_rows(convolved_rows, output_latent_gradient_total)
    grad_conv_out = grad_conv_out.reshape(sequences, length, channel_count)
    grad_cgate = grad_conv_out * mixed_sum
    grad_mixed = grad_conv_out * cgate
    grad_product = (
        tap_values[0] * grad_mixed
        + leading(tap_values[1] * grad_mixed * first_same_sequence, 1)
        + leading(tap_values[2] * grad_mixed * second_same_sequence, 2)
    )
    gradient_lanes = jnp.stack([grad_product * xval, grad_cgate, grad_product * bgate], axis=2)
    gradient_lanes = gradient_lanes.reshape(row_count, 3 * channel_count).astype(jnp.bfloat16)
    input_latent_gradient = masked_rows(
        contract_against(gradient_lanes, input_adapter_term), adapter_selector_total, 1
    )
    grad_in_expand = dot_over_rows(input_latent, gradient_lanes)
    grad_in_shrink = wide_over_rows(first_norm, input_latent_gradient)
    grad_norm_one = contract_against(gradient_lanes, input_projection_matrix) + broad_contract(
        input_latent_gradient, in_shrink.reshape(hidden_width, ADAPTER_COUNT * ADAPTER_RANK)
    )
    grad_norm_one_own = lax.psum_scatter(
        grad_norm_one.astype(jnp.bfloat16), "tensor", scatter_dimension=0, tiled=True
    ).astype(jnp.float32)
    grad_residual = (
        second_input_gradient
        + normalize_back(local_input, factor_one, conv_gain, grad_norm_one_own)
    ).astype(jnp.bfloat16)
    whole_in_shrink, whole_ffn_shrink, whole_out_expand, whole_down_expand = lax.psum(
        (grad_in_shrink, grad_ffn_shrink, grad_out_expand, grad_down_expand), ("dp", "tensor")
    )
    whole_in_expand, whole_ffn_expand, whole_out_shrink, whole_down_shrink = (
        lax.psum(grad_in_expand.astype(jnp.bfloat16), "dp").astype(jnp.float32),
        lax.psum(grad_ffn_expand.astype(jnp.bfloat16), "dp").astype(jnp.float32),
        lax.psum(grad_out_shrink.astype(jnp.bfloat16), "dp").astype(jnp.float32),
        lax.psum(grad_down_shrink.astype(jnp.bfloat16), "dp").astype(jnp.float32),
    )
    return (
        block_output,
        grad_residual,
        whole_in_shrink.reshape(hidden_width, ADAPTER_COUNT, ADAPTER_RANK),
        whole_in_expand.reshape(ADAPTER_COUNT, ADAPTER_RANK, 3, channel_count),
        whole_out_shrink.reshape(channel_count, ADAPTER_COUNT, ADAPTER_RANK),
        whole_out_expand.reshape(ADAPTER_COUNT, ADAPTER_RANK, hidden_width),
        whole_ffn_shrink.reshape(hidden_width, 2, ADAPTER_COUNT, ADAPTER_RANK),
        whole_ffn_expand.reshape(2, ADAPTER_COUNT, ADAPTER_RANK, hidden_shard),
        whole_down_shrink.reshape(hidden_shard, ADAPTER_COUNT, ADAPTER_RANK),
        whole_down_expand.reshape(ADAPTER_COUNT, ADAPTER_RANK, hidden_width),
    )


def solution(mesh):
    placed = (
        P(("dp", "tensor"), None),
        P(("dp", "tensor"), None),
        P("dp", None),
        P("dp"),
        P(),
        P("dp", None, "tensor"),
        P(None, "tensor"),
        P("dp", "tensor"),
        P(),
        P("dp", None, "tensor"),
        P("dp", "tensor"),
        P(),
        P(None, None, None, "tensor"),
        P("tensor", None, None),
        P(),
        P(),
        P(None, None, None, "tensor"),
        P("tensor", None, None),
        P(),
    )
    return jax.shard_map(
        per_device,
        mesh=mesh,
        in_specs=placed,
        out_specs=(
            P(("dp", "tensor"), None),
            P(("dp", "tensor"), None),
            P(),
            P(None, None, None, "tensor"),
            P("tensor", None, None),
            P(),
            P(),
            P(None, None, None, "tensor"),
            P("tensor", None, None),
            P(),
        ),
        check_vma=False,
    )
```

```python
import functools
import types

import jax
import jax.numpy as jnp
from jax import lax
from jax.experimental import pallas as pl
from jax.experimental.pallas import tpu as pltpu
from jax.sharding import PartitionSpec as P

ADAPTER_COUNT = 8
ADAPTER_RANK = 16
EPSILON = 1e-05
MESH = pl.DeviceIdType.MESH
LANES = 128
HIDDEN_CHUNK = 384
ROW_TILE = 256


def dot(left, right):
    return jnp.dot(left, right, preferred_element_type=jnp.float32)


def dot_against(left, right):
    return lax.dot_general(
        left, right, (((1,), (1,)), ((), ())), preferred_element_type=jnp.float32
    )


def split_pair(values):
    upper = values.astype(jnp.bfloat16)
    lower = (values - upper.astype(jnp.float32)).astype(jnp.bfloat16)
    return (upper, lower)


def norm_factor(values):
    return lax.rsqrt(jnp.mean(values * values, axis=-1, keepdims=True) + EPSILON)


def normalize_back(values, factor, gain, grad):
    unit = values * factor
    scaled = grad * gain
    return factor * (scaled - unit * jnp.mean(scaled * unit, axis=-1, keepdims=True))


def split_ring(count):
    if count % 16 == 0:
        return (4, count // 8, 2)
    return (count, 1, 1)


def position(index, dims):
    return (index // (dims[1] * dims[2]), (index // dims[2]) % dims[1], index % dims[2])


def flat(spot, dims):
    return (spot[0] * dims[1] + spot[1]) * dims[2] + spot[2]


class Gather:
    def __init__(self, dims, spot, send, recv):
        self.dims, self.spot, self.send, self.recv = dims, spot, send, recv

    def copies(self, piece, step):
        shard, whole, columns, order, row = piece
        axis = order[step]
        place = tuple(
            slice(None) if other in order[:step] else self.spot[other] for other in range(3)
        )
        target = whole.at[place + (slice(None), columns)]
        base = sum(self.dims[other] - 1 for other in order[:step])
        out = []
        for offset in range(1, self.dims[axis]):
            peer = list(self.spot)
            peer[axis] = lax.rem(self.spot[axis] + offset, self.dims[axis])
            out.append(
                pltpu.make_async_remote_copy(
                    src_ref=shard.at[:, columns] if step == 0 else target,
                    dst_ref=target,
                    send_sem=self.send.at[row, base + offset - 1],
                    recv_sem=self.recv.at[row, base + offset - 1],
                    device_id={"dp": flat(peer, self.dims)},
                    device_id_type=MESH,
                )
            )
        return out

    def start(self, pieces, step):
        for piece in pieces:
            for copy in self.copies(piece, step):
                copy.start()

    def arrive(self, pieces, step):
        for piece in pieces:
            for copy in self.copies(piece, step):
                copy.wait_recv()

    def drain(self, pieces):
        for piece in pieces:
            for step in range(3):
                for copy in self.copies(piece, step):
                    copy.wait_send()


def greet(dims, spot, team, member):
    barrier = pltpu.get_barrier_semaphore()
    count = 0
    for axis in range(3):
        for offset in range(1, dims[axis]):
            peer = list(spot)
            peer[axis] = lax.rem(spot[axis] + offset, dims[axis])
            pl.semaphore_signal(
                barrier, inc=1, device_id={"dp": flat(peer, dims)}, device_id_type=MESH
            )
            count += 1
    for offset in range(1, team):
        pl.semaphore_signal(
            barrier,
            inc=1,
            device_id={"tensor": lax.rem(member + offset, team)},
            device_id_type=MESH,
        )
        count += 1
    pl.semaphore_wait(barrier, count)


NAMES = (
    "io_shard",
    "ff_shard",
    "x_own",
    "g_own",
    "expand",
    "down_shrink",
    "same",
    "conv_gain",
    "ffn_gain",
    "taps",
    "in_reduce",
    "in_lift",
    "out_reduce",
    "out_lift",
    "ffn_reduce",
    "down_lift",
    "io_whole",
    "ff_whole",
    "streams",
    "norm_one",
    "conv_out",
    "code_in",
    "code_out",
    "block_out",
    "grad_x_two",
    "ffn_split",
    "ffn_rep",
    "x_all",
    "g_all",
    "na",
    "nb",
    "w",
    "acc_a",
    "acc_b",
    "x_two",
    "halo",
    "co",
    "cp",
    "gcf",
    "cf",
    "gd",
    "cft",
    "gdt",
    "act",
    "ggu",
    "eb",
    "dsb",
    "rb",
    "rc",
    "rd",
    "code_t",
    "send",
    "recv",
    "team_send",
    "team_recv",
    "local",
    "load_sem",
)


def forward_kernel(shape, *refs):
    s = types.SimpleNamespace(**dict(zip(NAMES, refs)))
    dims, team, width, channels, length, chunks = shape
    own = length // team
    hc = HIDDEN_CHUNK
    tile = ROW_TILE
    tiles = length // tile
    member = lax.axis_index("tensor")
    spot = position(lax.axis_index("dp"), dims)
    gather = Gather(dims, spot, s.send, s.recv)
    own_rows = pl.ds(pl.multiple_of(member * own, own), own)

    io_step = 4 * channels // 6
    io_pieces = []
    for i in range(6):
        half = io_step // 2
        io_pieces.append(
            [
                (s.io_shard, s.io_whole, pl.ds(i * io_step, half), (0, 1, 2), 2 * i),
                (s.io_shard, s.io_whole, pl.ds(i * io_step + half, half), (0, 2, 1), 2 * i + 1),
            ]
        )
    last = chunks - 1
    cut = 640

    def chunk_pieces(k, orders=((0, 1, 2), (0, 2, 1))):
        shard, whole = s.ff_shard.at[k], s.ff_whole.at[k]
        return [
            (shard, whole, pl.ds(0, cut), orders[0], 12 + 2 * k),
            (shard, whole, pl.ds(cut, 3 * hc - cut), orders[1], 13 + 2 * k),
        ]

    tail_pieces = chunk_pieces(last, ((1, 2, 0), (2, 1, 0)))

    def team_copies(row, source, target):
        out = []
        for offset in range(1, team):
            peer = lax.rem(member + offset, team)
            out.append(
                pltpu.make_async_remote_copy(
                    src_ref=source(peer, offset),
                    dst_ref=target(peer, offset),
                    send_sem=s.team_send.at[row, offset - 1],
                    recv_sem=s.team_recv.at[row, offset - 1],
                    device_id={"tensor": peer},
                    device_id_type=MESH,
                )
            )
        return out

    def rows_of(ref):
        return lambda peer, offset: ref.at[pl.ds(pl.multiple_of(peer * own, own), own)]

    def slot_of(ref):
        return lambda peer, offset: ref.at[offset - 1]

    greet(dims, spot, team, member)
    x_copies = team_copies(0, lambda p, o: s.x_own, lambda p, o: s.x_all.at[own_rows])
    g_copies = team_copies(1, lambda p, o: s.g_own, lambda p, o: s.g_all.at[own_rows])
    for copy in x_copies + g_copies:
        copy.start()
    x_here = pltpu.make_async_copy(s.x_own, s.x_all.at[own_rows], s.local.at[0])
    g_here = pltpu.make_async_copy(s.g_own, s.g_all.at[own_rows], s.local.at[1])
    x_here.start()
    g_here.start()

    def bounce(k):
        spare = s.w.at[(1 + k // 2) // (dims[1] * dims[2]), ((1 + k // 2) // dims[2]) % dims[1], (1 + k // 2) % dims[2]]
        return spare.at[:, pl.ds((k % 2) * 3 * hc, 3 * hc)]

    io_spare = s.w.at[0, 0, 0, :, pl.ds(0, 4 * channels)]
    ins = [pltpu.make_async_copy(s.io_shard, io_spare, s.local.at[2])]
    outs = [pltpu.make_async_copy(io_spare, s.io_whole.at[spot], s.local.at[2])]
    for k in range(chunks):
        ins.append(pltpu.make_async_copy(s.ff_shard.at[k], bounce(k), s.local.at[3 + k]))
        outs.append(pltpu.make_async_copy(bounce(k), s.ff_whole.at[(k,) + spot], s.local.at[3 + k]))
    for copy in ins:
        copy.start()
    for pieces in io_pieces:
        gather.start(pieces, 0)
    gather.start(tail_pieces, 0)
    for k in range(last):
        gather.start(chunk_pieces(k), 0)
    for first, second in zip(ins, outs):
        first.wait()
        second.start()

    x_here.wait()
    for copy in x_copies:
        copy.wait_recv()

    def first_norm(i, carry):
        rows = pl.ds(pl.multiple_of(i * tile, tile), tile)
        values = s.x_all[rows, :].astype(jnp.float32)
        s.na[rows, :] = (values * norm_factor(values) * s.conv_gain[...]).astype(jnp.bfloat16)
        return carry

    lax.fori_loop(0, tiles, first_norm, 0)
    norm_store = pltpu.make_async_copy(s.na, s.norm_one, s.local.at[0])
    norm_store.start()
    g_here.wait()
    for copy in g_copies:
        copy.wait_recv()

    def down_codes(i, carry):
        rows = pl.ds(pl.multiple_of(i * tile, tile), tile)
        code = dot_against(s.g_all[rows, :], s.down_lift[...])
        s.gd[rows, :] = code.astype(jnp.bfloat16)
        s.gdt[:, rows] = jnp.transpose(code)[:16].astype(jnp.bfloat16)
        return carry

    lax.fori_loop(0, tiles, down_codes, 0)
    for copy in outs:
        copy.wait()

    for i in range(7):
        if i < 6:
            gather.arrive(io_pieces[i], 0)
            gather.start(io_pieces[i], 1)
        if i > 0:
            gather.arrive(io_pieces[i - 1], 1)
            gather.start(io_pieces[i - 1], 2)
    gather.arrive(tail_pieces, 0)
    gather.start(tail_pieces, 1)
    gather.arrive(chunk_pieces(0), 0)
    gather.start(chunk_pieces(0), 1)
    io_loads = []
    for i in range(6):
        gather.arrive(io_pieces[i], 2)
        columns = pl.ds(i * io_step, io_step)
        load = pltpu.make_async_copy(
            s.io_whole.at[:, :, :, :, columns], s.w.at[:, :, :, :, columns], s.load_sem.at[i]
        )
        load.start()
        io_loads.append(load)
    gather.arrive(tail_pieces, 1)
    gather.start(tail_pieces, 2)
    gather.arrive(chunk_pieces(0), 1)
    gather.start(chunk_pieces(0), 2)
    gather.arrive(chunk_pieces(1), 0)
    gather.start(chunk_pieces(1), 1)
    norm_store.wait()
    for load in io_loads:
        load.wait()

    def weights(first, count):
        return s.w[:, :, :, :, pl.ds(first, count)].reshape(width, count)

    s.halo[pl.ds(0, 8), :] = jnp.zeros((8, channels), jnp.float32)

    def convolve(i, carry):
        rows = pl.ds(pl.multiple_of(i * tile, tile), tile)
        normed = s.na[rows, :]
        code = dot(normed, s.in_reduce[...])
        s.code_in[:, rows] = jnp.transpose(code)[:16].astype(jnp.bfloat16)
        code = code.astype(jnp.bfloat16)
        lanes = []
        for lane in range(3):
            value = dot(normed, weights(lane * channels, channels)) + dot(
                code, s.in_lift[:, pl.ds(lane * channels, channels)]
            )
            lanes.append(value)
            if lane < 2:
                s.acc_a[rows, pl.ds(lane * channels, channels)] = value
            else:
                s.acc_b[rows, pl.ds(0, channels)] = value
        product = lanes[0] * lanes[2]
        s.halo[pl.ds(8, tile), :] = product
        masks = s.same[rows, :]
        mixed = (
            s.taps[0:1, :] * product
            + s.taps[1:2, :] * s.halo[pl.ds(7, tile), :] * masks[:, 0:1]
            + s.taps[2:3, :] * s.halo[pl.ds(6, tile), :] * masks[:, 1:2]
        )
        s.halo[pl.ds(0, 8), :] = s.halo[pl.ds(tile, 8), :]
        convolved = (lanes[1] * mixed).astype(jnp.bfloat16)
        s.co[rows, :] = convolved
        s.na[rows, :] = dot_against(convolved, weights(3 * channels, channels)).astype(jnp.bfloat16)
        s.cp[rows, :] = dot(convolved, s.out_reduce[...])
        return carry

    lax.fori_loop(0, tiles, convolve, 0)
    stores = [
        pltpu.make_async_copy(s.acc_a.at[:, pl.ds(0, channels)], s.streams.at[0], s.local.at[3]),
        pltpu.make_async_copy(
            s.acc_a.at[:, pl.ds(channels, channels)], s.streams.at[1], s.local.at[4]
        ),
        pltpu.make_async_copy(s.acc_b.at[:, pl.ds(0, channels)], s.streams.at[2], s.local.at[5]),
        pltpu.make_async_copy(s.co, s.conv_out, s.local.at[6]),
    ]
    for copy in stores:
        copy.start()

    branch = team_copies(2, rows_of(s.na), slot_of(s.rb))
    codes = team_copies(3, rows_of(s.cp), slot_of(s.rc))
    for copy in codes + branch:
        copy.start()
    gather.arrive(chunk_pieces(1), 1)
    gather.start(chunk_pieces(1), 2)
    gather.arrive(chunk_pieces(2), 0)
    gather.start(chunk_pieces(2), 1)

    def load(c):
        slot = lax.rem(c, 2)
        columns = pl.ds(pl.multiple_of(slot * 3 * hc, LANES), 3 * hc)
        return [
            pltpu.make_async_copy(
                s.ff_whole.at[c], s.w.at[:, :, :, :, columns], s.load_sem.at[3 * slot]
            ),
            pltpu.make_async_copy(s.expand.at[c], s.eb.at[slot], s.load_sem.at[3 * slot + 1]),
            pltpu.make_async_copy(s.down_shrink.at[c], s.dsb.at[slot], s.load_sem.at[3 * slot + 2]),
        ]

    for copy in branch + codes:
        copy.wait_recv()
    code = s.cp[own_rows, :]
    for peer in range(team - 1):
        code = code + s.rc[peer]
    s.code_out[...] = jnp.transpose(code)[:16].astype(jnp.bfloat16)
    s.cf[pl.ds(0, own), :] = code.astype(jnp.bfloat16)

    own_tile = min(own, tile)

    def second_norm(i, carry):
        local_rows = pl.ds(pl.multiple_of(i * own_tile, own_tile), own_tile)
        rows = pl.ds(pl.multiple_of(member * own + i * own_tile, own_tile), own_tile)
        values = s.x_all[rows, :].astype(jnp.float32) + s.na[rows, :].astype(jnp.float32)
        for peer in range(team - 1):
            values = values + s.rb[peer, local_rows, :].astype(jnp.float32)
        values = values + dot(s.cf[local_rows, :], s.out_lift[...])
        s.x_two[local_rows, :] = values
        s.nb[rows, :] = (values * norm_factor(values) * s.ffn_gain[...]).astype(jnp.bfloat16)
        return carry

    lax.fori_loop(0, own // own_tile, second_norm, 0)
    norms = team_copies(4, lambda p, o: s.nb.at[own_rows], lambda p, o: s.nb.at[own_rows])
    for copy in norms:
        copy.start()
    gather.arrive(chunk_pieces(0), 2)
    for copy in load(0):
        copy.start()
    for copy in stores:
        copy.wait()
    s.acc_a[...] = jnp.zeros_like(s.acc_a)
    s.acc_b[...] = jnp.zeros_like(s.acc_b)
    for copy in branch + codes:
        copy.wait_send()
    s.cp[...] = jnp.zeros_like(s.cp)
    s.gcf[...] = jnp.zeros_like(s.gcf)
    for copy in norms:
        copy.wait_recv()

    def ffn_codes(i, carry):
        rows = pl.ds(pl.multiple_of(i * tile, tile), tile)
        value = dot(s.nb[rows, :], s.ffn_reduce[...])
        s.cf[rows, :] = value.astype(jnp.bfloat16)
        s.cft[:, rows] = jnp.transpose(value)[:32].astype(jnp.bfloat16)
        return carry

    lax.fori_loop(0, tiles, ffn_codes, 0)

    def chunk(c, carry):
        @pl.when(c + 3 < last)
        def _():
            gather.arrive(chunk_pieces(c + 3), 0)
            gather.start(chunk_pieces(c + 3), 1)

        @pl.when(c + 2 < last)
        def _():
            gather.arrive(chunk_pieces(c + 2), 1)
            gather.start(chunk_pieces(c + 2), 2)

        @pl.when(c + 1 < last)
        def _():
            gather.arrive(chunk_pieces(c + 1), 2)

        @pl.when(c + 1 == last)
        def _():
            gather.arrive(tail_pieces, 2)

        @pl.when(c + 1 < chunks)
        def _():
            for copy in load(c + 1):
                copy.start()

        for copy in load(c):
            copy.wait()
        slot = lax.rem(c, 2)
        first = pl.multiple_of(slot * 3 * hc, LANES)
        down_first = pl.multiple_of(slot * 3 * hc + 2 * hc, LANES)

        def row_tile(i, inner):
            rows = pl.ds(pl.multiple_of(i * tile, tile), tile)
            both = dot(s.nb[rows, :], weights(first, 2 * hc)) + dot(s.cf[rows, :], s.eb[slot])
            grad = dot(s.g_all[rows, :], weights(down_first, hc)) + dot_against(
                s.gd[rows, :], s.dsb[slot]
            )
            gate, up = both[:, :hc], both[:, hc:]
            gated = jax.nn.sigmoid(gate)
            silu = gate * gated
            act = (silu * up).astype(jnp.bfloat16)
            s.act[rows, :] = act
            s.ggu[rows, pl.ds(0, hc)] = (grad * up * gated * (1.0 + gate * (1.0 - gated))).astype(
                jnp.bfloat16
            )
            s.ggu[rows, pl.ds(hc, hc)] = (grad * silu).astype(jnp.bfloat16)
            s.acc_a[rows, :] += dot_against(act, weights(down_first, hc))
            s.cp[rows, :] += dot(act, s.dsb[slot])
            ggu = s.ggu[rows, :]
            s.acc_b[rows, :] += dot_against(ggu, weights(first, 2 * hc))
            s.gcf[rows, :] += dot_against(ggu, s.eb[slot])
            return inner

        lax.fori_loop(0, tiles, row_tile, 0)
        at = pl.multiple_of(c * hc, LANES)
        padded = chunks * hc
        spread = dot(s.cft[...], s.ggu[...])
        s.ffn_split[:, pl.ds(at, hc)] = spread[:16, :hc].astype(jnp.bfloat16)
        s.ffn_split[:, pl.ds(padded + at, hc)] = spread[16:, hc:].astype(jnp.bfloat16)
        shrunk = dot(s.gdt[...], s.act[...])
        s.ffn_split[:, pl.ds(2 * padded + at, hc)] = shrunk.astype(jnp.bfloat16)
        return carry

    lax.fori_loop(0, chunks, chunk, 0)

    def finish(i, carry):
        rows = pl.ds(pl.multiple_of(i * tile, tile), tile)
        s.na[rows, :] = s.acc_a[rows, :].astype(jnp.bfloat16)
        value = s.gcf[rows, :]
        s.code_t[:, rows] = jnp.transpose(value)[:32]
        upper, lower = split_pair(value)
        total = (
            s.acc_b[rows, :]
            + dot_against(upper, s.ffn_reduce[...])
            + dot_against(lower, s.ffn_reduce[...])
        )
        s.x_all[rows, :] = total.astype(jnp.bfloat16)
        return carry

    lax.fori_loop(0, tiles, finish, 0)
    grads = team_copies(5, rows_of(s.x_all), slot_of(s.rd))
    downs = team_copies(6, rows_of(s.na), slot_of(s.rb))
    codes = team_copies(7, rows_of(s.cp), slot_of(s.rc))
    for copy in grads + codes + downs:
        copy.start()
    upper, lower = split_pair(s.code_t[...])
    shrunk = (dot(upper, s.nb[...]) + dot(lower, s.nb[...])).astype(jnp.bfloat16)
    s.ffn_rep[:, pl.ds(0, width)] = shrunk[:16]
    s.ffn_rep[:, pl.ds(width, width)] = shrunk[16:]
    for copy in grads + codes + downs:
        copy.wait_recv()
    code = s.cp[own_rows, :]
    for peer in range(team - 1):
        code = code + s.rc[peer]
    rounded = code.astype(jnp.bfloat16)
    s.cf[pl.ds(0, own), :] = rounded
    turned = jnp.transpose(code)[:16].astype(jnp.bfloat16)
    s.ffn_rep[:, pl.ds(2 * width, width)] = dot(turned, s.g_all[own_rows, :]).astype(jnp.bfloat16)
    for copy in norms + grads + downs:
        copy.wait_send()

    def last_rows(i, carry):
        local_rows = pl.ds(pl.multiple_of(i * own_tile, own_tile), own_tile)
        rows = pl.ds(pl.multiple_of(member * own + i * own_tile, own_tile), own_tile)
        values = s.x_two[local_rows, :]
        down = s.acc_a[rows, :]
        grad = s.acc_b[rows, :]
        upper, lower = split_pair(s.gcf[rows, :])
        grad = grad + dot_against(upper, s.ffn_reduce[...]) + dot_against(lower, s.ffn_reduce[...])
        for peer in range(team - 1):
            down = down + s.rb[peer, local_rows, :].astype(jnp.float32)
            grad = grad + s.rd[peer, local_rows, :].astype(jnp.float32)
        out = values + down + dot(s.cf[local_rows, :], s.down_lift[...])
        s.nb[local_rows, :] = out.astype(jnp.bfloat16)
        s.x_two[local_rows, :] = s.g_all[rows, :].astype(jnp.float32) + normalize_back(
            values, norm_factor(values), s.ffn_gain[...], grad
        )
        return carry

    lax.fori_loop(0, own // own_tile, last_rows, 0)
    results = [
        pltpu.make_async_copy(s.nb.at[pl.ds(0, own)], s.block_out, s.local.at[0]),
        pltpu.make_async_copy(s.x_two, s.grad_x_two, s.local.at[1]),
    ]
    for copy in results:
        copy.start()
    for copy in x_copies + g_copies + codes:
        copy.wait_send()
    for pieces in io_pieces:
        gather.drain(pieces)
    gather.drain(tail_pieces)

    def drain(k, carry):
        gather.drain(chunk_pieces(k))
        return carry

    lax.fori_loop(0, last, drain, 0)
    for copy in results:
        copy.wait()


def forward_and_ffn(dims, team, operands):
    io_shard, ff_shard, x_own = operands[:3]
    rows = io_shard.shape[0]
    channels = io_shard.shape[1] // 4
    chunks = ff_shard.shape[0]
    own, width = x_own.shape
    length = own * team
    hc = HIDDEN_CHUNK
    columns = max(4 * channels, 6 * hc)
    lanes = sum(d - 1 for d in dims)
    shape = (dims, team, width, channels, length, chunks)
    bf16, f32 = jnp.bfloat16, jnp.float32
    anywhere = pl.BlockSpec(memory_space=pl.ANY)
    vmem = pl.BlockSpec(memory_space=pltpu.VMEM)
    outs = [
        (dims + (rows, 4 * channels), bf16, anywhere),
        ((chunks,) + dims + (rows, 3 * hc), bf16, anywhere),
        ((3, length, channels), f32, anywhere),
        ((length, width), bf16, anywhere),
        ((length, channels), bf16, anywhere),
        ((16, length), bf16, vmem),
        ((16, own), bf16, vmem),
        ((own, width), bf16, anywhere),
        ((own, width), f32, anywhere),
        ((16, 3 * chunks * hc), bf16, vmem),
        ((16, 3 * width), bf16, vmem),
    ]
    peers = max(team - 1, 1)
    row_count = 12 + 2 * chunks
    scratch = [
        pltpu.VMEM((length, width), bf16),
        pltpu.VMEM((length, width), bf16),
        pltpu.VMEM((length, width), bf16),
        pltpu.VMEM((length, width), bf16),
        pltpu.VMEM(dims + (rows, columns), bf16),
        pltpu.VMEM((length, width), f32),
        pltpu.VMEM((length, width), f32),
        pltpu.VMEM((own, width), f32),
        pltpu.VMEM((ROW_TILE + 8, channels), f32),
        pltpu.VMEM((length, channels), bf16),
        pltpu.VMEM((length, LANES), f32),
        pltpu.VMEM((length, LANES), f32),
        pltpu.VMEM((length, LANES), bf16),
        pltpu.VMEM((length, LANES), bf16),
        pltpu.VMEM((32, length), bf16),
        pltpu.VMEM((16, length), bf16),
        pltpu.VMEM((length, hc), bf16),
        pltpu.VMEM((length, 2 * hc), bf16),
        pltpu.VMEM((2, LANES, 2 * hc), bf16),
        pltpu.VMEM((2, hc, LANES), bf16),
        pltpu.VMEM((peers, own, width), bf16),
        pltpu.VMEM((peers, own, LANES), f32),
        pltpu.VMEM((peers, own, width), bf16),
        pltpu.VMEM((32, length), f32),
        pltpu.SemaphoreType.DMA((row_count, lanes)),
        pltpu.SemaphoreType.DMA((row_count, lanes)),
        pltpu.SemaphoreType.DMA((8, peers)),
        pltpu.SemaphoreType.DMA((8, peers)),
        pltpu.SemaphoreType.DMA((max(3 + chunks, 8),)),
        pltpu.SemaphoreType.DMA((6,)),
    ]
    return pl.pallas_call(
        functools.partial(forward_kernel, shape),
        out_shape=[jax.ShapeDtypeStruct(o[0], o[1]) for o in outs],
        in_specs=[anywhere] * 6 + [vmem] * 10,
        out_specs=[o[2] for o in outs],
        scratch_shapes=scratch,
        compiler_params=pltpu.CompilerParams(
            collective_id=0, has_side_effects=True, vmem_limit_bytes=67043328
        ),
    )(*operands)


BACK_NAMES = (
    "grad_x_two",
    "ffn_split",
    "ffn_rep",
    "io_whole",
    "streams",
    "norm_one",
    "conv_out",
    "x_own",
    "code_in",
    "code_out",
    "same",
    "conv_gain",
    "taps",
    "in_reduce",
    "in_lift",
    "out_reduce",
    "out_lift",
    "onehot",
    "grad_residual",
    "early",
    "late",
    "early_rep",
    "late_rep",
    "w",
    "gx",
    "gb",
    "gco",
    "gcot",
    "st",
    "gs",
    "ha",
    "hb",
    "halo",
    "na",
    "co",
    "pb",
    "gcit",
    "xo",
    "rb",
    "rep_a",
    "rep_b",
    "got_a",
    "got_b",
    "flat_a",
    "flat_b",
    "part_a",
    "part_b",
    "from_a",
    "from_b",
    "sum_a",
    "sum_b",
    "spare_a",
    "spare_b",
    "out",
    "send",
    "recv",
    "swap_send",
    "swap_recv",
    "team_send",
    "team_recv",
    "local",
)


class Share:
    def __init__(self, count, team, split, shared):
        self.split, self.shared, self.share = split, shared, shared // team
        self.total = split + self.share
        self.block = -(-self.total // (LANES * count)) * LANES
        self.first = split // self.block
        self.blocks = -(-self.total // self.block) - self.first


def backward_kernel(shape, *refs):
    s = types.SimpleNamespace(**dict(zip(BACK_NAMES, refs)))
    dims, team, width, channels, length, early, late = shape
    count = dims[0] * dims[1] * dims[2]
    own = length // team
    tile = ROW_TILE
    tiles = length // tile
    own_tile = min(own, tile)
    member = lax.axis_index("tensor")
    me = lax.axis_index("dp")
    spot = position(me, dims)
    gather = Gather(dims, spot, s.send, s.recv)
    own_rows = pl.ds(pl.multiple_of(member * own, own), own)

    barrier = pltpu.get_barrier_semaphore()
    for offset in range(1, count):
        pl.semaphore_signal(
            barrier, inc=1, device_id={"dp": lax.rem(me + offset, count)}, device_id_type=MESH
        )
    for offset in range(1, team):
        pl.semaphore_signal(
            barrier,
            inc=1,
            device_id={"tensor": lax.rem(member + offset, team)},
            device_id_type=MESH,
        )
    pl.semaphore_wait(barrier, count - 1 + team - 1)

    def team_copies(row, source, target):
        out = []
        for offset in range(1, team):
            peer = lax.rem(member + offset, team)
            out.append(
                pltpu.make_async_remote_copy(
                    src_ref=source(peer, offset),
                    dst_ref=target(peer, offset),
                    send_sem=s.team_send.at[row, offset - 1],
                    recv_sem=s.team_recv.at[row, offset - 1],
                    device_id={"tensor": peer},
                    device_id_type=MESH,
                )
            )
        return out

    def swap_copies(row, part, landing):
        out = []
        for offset in range(1, count):
            peer = lax.rem(me + offset, count)
            out.append(
                pltpu.make_async_remote_copy(
                    src_ref=part.at[peer],
                    dst_ref=landing.at[me],
                    send_sem=s.swap_send.at[row, offset - 1],
                    recv_sem=s.swap_recv.at[row, offset - 1],
                    device_id={"dp": peer},
                    device_id_type=MESH,
                )
            )
        return out

    def pieces_of(share, total, whole, row):
        cut = (share.block // 256) * 128
        if cut == 0:
            return [(total, whole, pl.ds(0, share.block), (0, 1, 2), row)]
        return [
            (total, whole, pl.ds(0, cut), (0, 1, 2), row),
            (total, whole, pl.ds(cut, share.block - cut), (0, 2, 1), row + 1),
        ]

    def hand_out(share, columns, part, landing, row):
        for peer in range(count):
            part[peer, :, pl.ds(0, share.block)] = columns[:, pl.ds(peer * share.block, share.block)]
            part[peer, :, pl.ds(share.block, LANES)] = s.onehot[...]
        landing[me] = part[me]
        copies = swap_copies(row, part, landing)
        for copy in copies:
            copy.start()
        return copies

    def take_in(share, landing, total):
        for adapter in range(ADAPTER_COUNT):

            def add(source, value):
                mask = landing[source, adapter : adapter + 1, pl.ds(share.block, LANES)]
                mask = mask.astype(jnp.float32)[:, 0:1]
                return value + mask * landing[source, :, pl.ds(0, share.block)].astype(jnp.float32)

            value = lax.fori_loop(0, count, add, jnp.zeros((16, share.block), jnp.float32))
            total[pl.ds(adapter * 16, 16), :] = value.astype(jnp.bfloat16)

    def shared_slice(share):
        return lambda peer, offset: pl.ds(pl.multiple_of(peer * share.share, LANES), share.share)

    def sum_shared(share, rep, got, columns):
        value = rep[:, pl.ds(pl.multiple_of(member * share.share, LANES), share.share)].astype(
            jnp.float32
        )
        for peer in range(team - 1):
            value = value + got[peer].astype(jnp.float32)
        columns[:, pl.ds(share.split, share.share)] = value.astype(jnp.bfloat16)
        rest = count * share.block - share.total
        if rest:
            columns[:, pl.ds(share.total, rest)] = jnp.zeros((16, rest), jnp.bfloat16)

    loads = {}
    for slot, (name, source, target) in enumerate(
        [
            ("gx", s.grad_x_two, s.gx),
            ("rep", s.ffn_rep, s.rep_a.at[:, pl.ds(0, 3 * width)]),
            ("split", s.ffn_split, s.flat_a.at[:, pl.ds(0, early.split - channels)]),
            ("co", s.conv_out, s.co),
            ("w", s.io_whole, s.w),
            ("b", s.streams.at[0], s.st.at[0, pl.ds(8, length)]),
            ("c", s.streams.at[1], s.st.at[1, pl.ds(8, length)]),
            ("x", s.streams.at[2], s.st.at[2, pl.ds(8, length)]),
            ("na", s.norm_one, s.na),
            ("xo", s.x_own, s.xo),
        ]
    ):
        loads[name] = pltpu.make_async_copy(source, target, s.local.at[slot])
        loads[name].start()
    s.st[0, pl.ds(0, 8), :] = jnp.zeros((8, channels), jnp.float32)
    s.st[2, pl.ds(0, 8), :] = jnp.zeros((8, channels), jnp.float32)
    s.ha[pl.ds(tile, 8), :] = jnp.zeros((8, channels), jnp.float32)
    s.hb[pl.ds(tile, 8), :] = jnp.zeros((8, channels), jnp.float32)

    loads["gx"].wait()

    def branch_rows(i, carry):
        local_rows = pl.ds(pl.multiple_of(i * own_tile, own_tile), own_tile)
        rows = pl.ds(pl.multiple_of(member * own + i * own_tile, own_tile), own_tile)
        upper, lower = split_pair(s.gx[local_rows, :])
        s.gb[rows, :] = upper
        code = dot_against(upper, s.out_lift[...]) + dot_against(lower, s.out_lift[...])
        s.gco[rows, :] = code.astype(jnp.bfloat16)
        return carry

    lax.fori_loop(0, own // own_tile, branch_rows, 0)
    swaps = team_copies(0, lambda p, o: s.gb.at[own_rows], lambda p, o: s.gb.at[own_rows])
    swaps += team_copies(1, lambda p, o: s.gco.at[own_rows], lambda p, o: s.gco.at[own_rows])
    for copy in swaps:
        copy.start()
    upper, lower = split_pair(s.gx[...])
    loads["rep"].wait()
    s.rep_a[:, pl.ds(3 * width, width)] = (
        dot(s.code_out[...], upper) + dot(s.code_out[...], lower)
    ).astype(jnp.bfloat16)
    cut_a = shared_slice(early)
    reps = team_copies(2, lambda p, o: s.rep_a.at[:, cut_a(p, o)], lambda p, o: s.got_a.at[o - 1])
    for copy in reps:
        copy.start()
    for copy in swaps:
        copy.wait_recv()

    def turn(i, carry):
        rows = pl.ds(pl.multiple_of(i * tile, tile), tile)
        value = jnp.transpose(s.gco[rows, :].astype(jnp.float32))[:16]
        s.gcot[:, rows] = value.astype(jnp.bfloat16)
        return carry

    lax.fori_loop(0, tiles, turn, 0)
    loads["co"].wait()
    loads["split"].wait()
    s.flat_a[:, pl.ds(early.split - channels, channels)] = dot(s.gcot[...], s.co[...]).astype(
        jnp.bfloat16
    )
    for copy in reps:
        copy.wait_recv()
    sum_shared(early, s.rep_a, s.got_a, s.flat_a)
    sent_a = hand_out(early, s.flat_a, s.part_a, s.from_a, 0)
    pieces_a = pieces_of(early, s.sum_a, s.early, 0)
    pieces_b = pieces_of(late, s.sum_b, s.late, 2)
    place_a = pltpu.make_async_copy(s.sum_a, s.early.at[spot], s.local.at[1])
    place_b = pltpu.make_async_copy(s.sum_b, s.late.at[spot], s.local.at[2])

    for name in ("w", "b", "c", "x"):
        loads[name].wait()

    def weights(first, amount):
        return s.w[:, :, :, :, pl.ds(first, amount)].reshape(width, amount)

    def back(j, carry):
        i = tiles - 1 - j
        start = pl.multiple_of(i * tile, tile)
        rows = pl.ds(start, tile)
        later = pl.ds(pl.multiple_of(start + 8, 8), tile)
        grad = dot(s.gb[rows, :], weights(3 * channels, channels)) + dot_against(
            s.gco[rows, :], s.out_reduce[...]
        )
        s.halo[pl.ds(0, 8), :] = s.st[0, pl.ds(start, 8), :] * s.st[2, pl.ds(start, 8), :]
        product = s.st[0, later, :] * s.st[2, later, :]
        s.halo[pl.ds(8, tile), :] = product
        masks = s.same[rows, :]
        mixed = (
            s.taps[0:1, :] * product
            + s.taps[1:2, :] * s.halo[pl.ds(7, tile), :] * masks[:, 0:1]
            + s.taps[2:3, :] * s.halo[pl.ds(6, tile), :] * masks[:, 1:2]
        )
        grad_mixed = grad * s.st[1, later, :]
        s.ha[pl.ds(0, tile), :] = s.taps[1:2, :] * grad_mixed * masks[:, 0:1]
        s.hb[pl.ds(0, tile), :] = s.taps[2:3, :] * grad_mixed * masks[:, 1:2]
        grad_product = (
            s.taps[0:1, :] * grad_mixed + s.ha[pl.ds(1, tile), :] + s.hb[pl.ds(2, tile), :]
        )
        s.ha[pl.ds(tile, 8), :] = s.ha[pl.ds(0, 8), :]
        s.hb[pl.ds(tile, 8), :] = s.hb[pl.ds(0, 8), :]
        s.gs[rows, pl.ds(0, channels)] = (grad_product * s.st[2, later, :]).astype(jnp.bfloat16)
        s.gs[rows, pl.ds(channels, channels)] = (grad * mixed).astype(jnp.bfloat16)
        s.gs[rows, pl.ds(2 * channels, channels)] = (grad_product * s.st[0, later, :]).astype(
            jnp.bfloat16
        )
        lanes = s.gs[rows, :]
        code = dot_against(lanes, s.in_lift[...])
        s.gcit[:, rows] = jnp.transpose(code)[:16]
        upper, lower = split_pair(code)
        s.pb[rows, :] = (
            dot_against(lanes, weights(0, 3 * channels))
            + dot_against(upper, s.in_reduce[...])
            + dot_against(lower, s.in_reduce[...])
        ).astype(jnp.bfloat16)

        @pl.when(j == tiles - 2)
        def _():
            for copy in sent_a:
                copy.wait_recv()
            take_in(early, s.from_a, s.sum_a)
            place_a.start()
            gather.start(pieces_a, 0)

        return carry

    lax.fori_loop(0, tiles, back, 0)
    grads = team_copies(
        3,
        lambda p, o: s.pb.at[pl.ds(pl.multiple_of(p * own, own), own)],
        lambda p, o: s.rb.at[o - 1],
    )
    for copy in grads:
        copy.start()
    loads["na"].wait()
    upper, lower = split_pair(s.gcit[...])
    s.rep_b[...] = (dot(upper, s.na[...]) + dot(lower, s.na[...])).astype(jnp.bfloat16)
    cut_b = shared_slice(late)
    more = team_copies(4, lambda p, o: s.rep_b.at[:, cut_b(p, o)], lambda p, o: s.got_b.at[o - 1])
    for copy in more:
        copy.start()
    s.flat_b[:, pl.ds(0, 3 * channels)] = dot(s.code_in[...], s.gs[...]).astype(jnp.bfloat16)
    for copy in more:
        copy.wait_recv()
    sum_shared(late, s.rep_b, s.got_b, s.flat_b)
    sent_b = hand_out(late, s.flat_b, s.part_b, s.from_b, 1)
    place_a.wait()
    gather.arrive(pieces_a, 0)
    gather.start(pieces_a, 1)
    loads["xo"].wait()
    for copy in grads:
        copy.wait_recv()

    def residual_rows(i, carry):
        local_rows = pl.ds(pl.multiple_of(i * own_tile, own_tile), own_tile)
        rows = pl.ds(pl.multiple_of(member * own + i * own_tile, own_tile), own_tile)
        values = s.xo[local_rows, :].astype(jnp.float32)
        grad = s.pb[rows, :].astype(jnp.float32)
        for peer in range(team - 1):
            grad = grad + s.rb[peer, local_rows, :].astype(jnp.float32)
        s.out[local_rows, :] = (
            s.gx[local_rows, :]
            + normalize_back(values, norm_factor(values), s.conv_gain[...], grad)
        ).astype(jnp.bfloat16)
        return carry

    lax.fori_loop(0, own // own_tile, residual_rows, 0)
    result = pltpu.make_async_copy(s.out, s.grad_residual, s.local.at[0])
    result.start()
    for copy in sent_b:
        copy.wait_recv()
    take_in(late, s.from_b, s.sum_b)
    place_b.start()
    gather.start(pieces_b, 0)
    gather.arrive(pieces_a, 1)
    gather.start(pieces_a, 2)
    place_b.wait()
    gather.arrive(pieces_b, 0)
    gather.start(pieces_b, 1)

    def pass_on(share, whole, reps, spare, base):
        for block in range(share.blocks):
            here = whole.at[position(share.first + block, dims)]
            load = pltpu.make_async_copy(here, spare.at[block], s.local.at[3 + block])
            load.start()
            load.wait()
        out = team_copies(base, lambda p, o: spare, lambda p, o: reps.at[member])
        for copy in out:
            copy.start()
        keep = pltpu.make_async_copy(spare, reps.at[member], s.local.at[3])
        keep.start()
        return out, keep

    gather.arrive(pieces_a, 2)
    out_a, keep_a = pass_on(early, s.early, s.early_rep, s.spare_a, 5)
    gather.arrive(pieces_b, 1)
    gather.start(pieces_b, 2)
    keep_a.wait()
    gather.arrive(pieces_b, 2)
    out_b, keep_b = pass_on(late, s.late, s.late_rep, s.spare_b, 6)
    for copy in out_a + out_b:
        copy.wait_recv()
    for copy in out_a + out_b + swaps + reps + grads + more + sent_a + sent_b:
        copy.wait_send()
    gather.drain(pieces_a)
    gather.drain(pieces_b)
    keep_b.wait()
    result.wait()


def backward(dims, team, early, late, operands):
    grad_x_two, ffn_split, ffn_rep, io_whole, streams, norm_one, conv_out, x_own = operands[:8]
    count = dims[0] * dims[1] * dims[2]
    own, width = x_own.shape
    length, channels = conv_out.shape
    lanes = sum(d - 1 for d in dims)
    bf16, f32 = jnp.bfloat16, jnp.float32
    anywhere = pl.BlockSpec(memory_space=pl.ANY)
    vmem = pl.BlockSpec(memory_space=pltpu.VMEM)
    rows = ADAPTER_COUNT * 16
    peers = max(team - 1, 1)
    outs = [
        ((own, width), bf16),
        (dims + (rows, early.block), bf16),
        (dims + (rows, late.block), bf16),
        ((team, early.blocks, rows, early.block), bf16),
        ((team, late.blocks, rows, late.block), bf16),
    ]
    scratch = [
        pltpu.VMEM(io_whole.shape, bf16),
        pltpu.VMEM((own, width), f32),
        pltpu.VMEM((length, width), bf16),
        pltpu.VMEM((length, LANES), bf16),
        pltpu.VMEM((16, length), bf16),
        pltpu.VMEM((3, length + 8, channels), f32),
        pltpu.VMEM((length, 3 * channels), bf16),
        pltpu.VMEM((ROW_TILE + 8, channels), f32),
        pltpu.VMEM((ROW_TILE + 8, channels), f32),
        pltpu.VMEM((ROW_TILE + 8, channels), f32),
        pltpu.VMEM((length, width), bf16),
        pltpu.VMEM((length, channels), bf16),
        pltpu.VMEM((length, width), bf16),
        pltpu.VMEM((16, length), f32),
        pltpu.VMEM((own, width), bf16),
        pltpu.VMEM((peers, own, width), bf16),
        pltpu.VMEM((16, early.shared), bf16),
        pltpu.VMEM((16, late.shared), bf16),
        pltpu.VMEM((peers, 16, early.share), bf16),
        pltpu.VMEM((peers, 16, late.share), bf16),
        pltpu.VMEM((16, count * early.block), bf16),
        pltpu.VMEM((16, count * late.block), bf16),
        pltpu.VMEM((count, 16, early.block + LANES), bf16),
        pltpu.VMEM((count, 16, late.block + LANES), bf16),
        pltpu.VMEM((count, 16, early.block + LANES), bf16),
        pltpu.VMEM((count, 16, late.block + LANES), bf16),
        pltpu.VMEM((rows, early.block), bf16),
        pltpu.VMEM((rows, late.block), bf16),
        pltpu.VMEM((early.blocks, rows, early.block), bf16),
        pltpu.VMEM((late.blocks, rows, late.block), bf16),
        pltpu.VMEM((own, width), bf16),
        pltpu.SemaphoreType.DMA((4, lanes)),
        pltpu.SemaphoreType.DMA((4, lanes)),
        pltpu.SemaphoreType.DMA((2, count - 1)),
        pltpu.SemaphoreType.DMA((2, count - 1)),
        pltpu.SemaphoreType.DMA((7, peers)),
        pltpu.SemaphoreType.DMA((7, peers)),
        pltpu.SemaphoreType.DMA((max(10, 3 + max(early.blocks, late.blocks)),)),
    ]
    return pl.pallas_call(
        functools.partial(backward_kernel, (dims, team, width, channels, length, early, late)),
        out_shape=[jax.ShapeDtypeStruct(*o) for o in outs],
        in_specs=[anywhere] * 8 + [vmem] * (len(operands) - 8),
        out_specs=[anywhere] * 5,
        scratch_shapes=scratch,
        compiler_params=pltpu.CompilerParams(
            collective_id=1, has_side_effects=True, vmem_limit_bytes=67043328
        ),
    )(*operands)


def lagged_segments(segment_ids, lag):
    shifted = jnp.pad(segment_ids, ((0, 0), (lag, 0)), constant_values=-1)[
        :, : segment_ids.shape[1]
    ]
    return (segment_ids == shifted).astype(jnp.float32)


def pad_axis(values, axis, size):
    widths = [(0, 0)] * values.ndim
    widths[axis] = (0, size - values.shape[axis])
    return jnp.pad(values, widths)


def per_device(
    residual,
    cotangent,
    segment_ids,
    adapter_ids,
    conv_gain,
    proj_in,
    conv_taps,
    proj_out,
    ffn_gain,
    gate_up,
    proj_down,
    in_shrink,
    input_lift_weight,
    output_reduce_weight,
    output_lift_weight,
    ffn_reduce_weight,
    ffn_expand,
    down_shrink,
    down_lift_weight,
):
    own, width = residual.shape
    length = segment_ids.shape[1]
    team = length // own
    count = lax.axis_size("dp")
    dims = split_ring(count)
    rows, _, channels = proj_in.shape
    hidden = proj_down.shape[1]
    hc = HIDDEN_CHUNK
    chunks = -(-hidden // hc)
    padded = chunks * hc
    adapter = adapter_ids[0]
    onehot = (adapter == jnp.arange(ADAPTER_COUNT, dtype=jnp.int32)).astype(jnp.float32)

    io_shard = jnp.concatenate([proj_in.reshape(rows, 3 * channels), proj_out], axis=1)
    ff_shard = jnp.concatenate([gate_up, proj_down[:, None, :]], axis=1)
    ff_shard = pad_axis(ff_shard, 2, padded).reshape(rows, 3, chunks, hc)
    ff_shard = jnp.transpose(ff_shard, (2, 0, 1, 3)).reshape(chunks, rows, 3 * hc)

    def pick(values, axis):
        return lax.dynamic_index_in_dim(values, adapter, axis, keepdims=False)

    in_reduce = pad_axis(pick(in_shrink, 1), 1, LANES)
    in_lift = pad_axis(pick(input_lift_weight, 0).reshape(ADAPTER_RANK, 3 * channels), 0, LANES)
    out_reduce = pad_axis(pick(output_reduce_weight, 1), 1, LANES)
    out_lift = pad_axis(pick(output_lift_weight, 0), 0, LANES)
    ffn_reduce = pad_axis(pick(ffn_reduce_weight, 2).reshape(width, 2 * ADAPTER_RANK), 1, LANES)
    expand = pad_axis(pick(ffn_expand, 1), 2, padded).reshape(2, ADAPTER_RANK, chunks, hc)
    expand = jnp.transpose(expand, (2, 0, 1, 3))
    blank = jnp.zeros((chunks, ADAPTER_RANK, hc), expand.dtype)
    expand = jnp.concatenate(
        [
            jnp.concatenate([expand[:, 0], blank], axis=2),
            jnp.concatenate([blank, expand[:, 1]], axis=2),
        ],
        axis=1,
    )
    expand = pad_axis(expand, 1, LANES)
    shrink = pad_axis(pad_axis(pick(down_shrink, 1), 1, LANES), 0, padded)
    shrink = shrink.reshape(chunks, hc, LANES)
    down_lift = pad_axis(pick(down_lift_weight, 0), 0, LANES)
    first_same, second_same = lagged_segments(segment_ids, 1)[0], lagged_segments(segment_ids, 2)[0]
    same = jnp.stack([first_same, second_same], axis=1)
    taps = conv_taps.astype(jnp.float32)
    (
        io_whole,
        _,
        streams,
        norm_one,
        conv_out,
        code_in,
        code_out,
        block_output,
        grad_x_two,
        ffn_split,
        ffn_rep,
    ) = forward_and_ffn(
        dims,
        team,
        (
            io_shard,
            ff_shard,
            residual,
            cotangent,
            expand,
            shrink,
            same,
            conv_gain.reshape(1, width),
            ffn_gain.reshape(1, width),
            taps,
            in_reduce,
            in_lift,
            out_reduce,
            out_lift,
            ffn_reduce,
            down_lift,
        ),
    )
    early = Share(count, team, 3 * padded + channels, 4 * width)
    late = Share(count, team, 3 * channels, width)
    marks = jnp.broadcast_to(pad_axis(onehot, 0, 16)[:, None], (16, LANES)).astype(jnp.bfloat16)
    grad_residual, early_sums, late_sums, early_shared, late_shared = backward(
        dims,
        team,
        early,
        late,
        (
            grad_x_two,
            ffn_split,
            ffn_rep,
            io_whole,
            streams,
            norm_one,
            conv_out,
            residual,
            code_in,
            code_out,
            same,
            conv_gain.reshape(1, width),
            taps,
            in_reduce,
            in_lift,
            out_reduce,
            out_lift,
            marks,
        ),
    )

    def columns_of(sums, share):
        sums = sums.reshape(count, ADAPTER_COUNT, ADAPTER_RANK, share.block)
        return jnp.transpose(sums, (1, 2, 0, 3)).reshape(
            ADAPTER_COUNT, ADAPTER_RANK, count * share.block
        )

    def shared_columns(sums, share):
        sums = sums.reshape(team, share.blocks, ADAPTER_COUNT, ADAPTER_RANK, share.block)
        sums = jnp.transpose(sums, (2, 3, 0, 1, 4)).reshape(
            ADAPTER_COUNT, ADAPTER_RANK, team, share.blocks * share.block
        )
        skip = share.split - share.first * share.block
        return sums[..., skip : skip + share.share].reshape(
            ADAPTER_COUNT, ADAPTER_RANK, share.shared
        )

    def rows_first(values):
        return jnp.transpose(values, (2, 0, 1)).astype(jnp.float32)

    early_columns, late_columns = columns_of(early_sums, early), columns_of(late_sums, late)
    early_rest, late_rest = shared_columns(early_shared, early), shared_columns(late_shared, late)
    ffn_e = jnp.stack([early_columns[..., :hidden], early_columns[..., padded : padded + hidden]])
    ffn_e = ffn_e.astype(jnp.float32)
    down_s = rows_first(early_columns[..., 2 * padded : 2 * padded + hidden])
    out_s = rows_first(early_columns[..., 3 * padded : 3 * padded + channels])
    ffn_s = jnp.stack(
        [rows_first(early_rest[..., :width]), rows_first(early_rest[..., width : 2 * width])],
        axis=1,
    )
    down_e = early_rest[..., 2 * width : 3 * width].astype(jnp.float32)
    out_e = early_rest[..., 3 * width :].astype(jnp.float32)
    in_e = late_columns[..., : 3 * channels].astype(jnp.float32)
    in_e = in_e.reshape(ADAPTER_COUNT, ADAPTER_RANK, 3, channels)
    in_s = rows_first(late_rest)
    return (block_output, grad_residual, in_s, in_e, out_s, out_e, ffn_s, ffn_e, down_s, down_e)


def solution(mesh):
    rows = P(("dp", "tensor"), None)
    placed = (
        rows,
        rows,
        P("dp", None),
        P("dp"),
        P(),
        P("dp", None, "tensor"),
        P(None, "tensor"),
        P("dp", "tensor"),
        P(),
        P("dp", None, "tensor"),
        P("dp", "tensor"),
        P(),
        P(None, None, None, "tensor"),
        P("tensor", None, None),
        P(),
        P(),
        P(None, None, None, "tensor"),
        P("tensor", None, None),
        P(),
    )
    return jax.shard_map(
        per_device,
        mesh=mesh,
        in_specs=placed,
        out_specs=(
            rows,
            rows,
            P(),
            P(None, None, None, "tensor"),
            P("tensor", None, None),
            P(),
            P(),
            P(None, None, None, "tensor"),
            P("tensor", None, None),
            P(),
        ),
        check_vma=False,
    )
```

```python
import functools
import types

import jax
import jax.numpy as jnp
from jax import lax
from jax.experimental import pallas as pl
from jax.experimental.pallas import tpu as pltpu
from jax.sharding import PartitionSpec as P

ADAPTER_COUNT = 8
ADAPTER_RANK = 16
EPSILON = 1e-05
MESH = pl.DeviceIdType.MESH
LANES = 128
HIDDEN_CHUNK = 384
ROW_TILE = 256


def dot(left, right):
    return jnp.dot(left, right, preferred_element_type=jnp.float32)


def dot_against(left, right):
    return lax.dot_general(
        left, right, (((1,), (1,)), ((), ())), preferred_element_type=jnp.float32
    )


def split_pair(values):
    upper = values.astype(jnp.bfloat16)
    lower = (values - upper.astype(jnp.float32)).astype(jnp.bfloat16)
    return (upper, lower)


def norm_factor(values):
    return lax.rsqrt(jnp.mean(values * values, axis=-1, keepdims=True) + EPSILON)


def normalize_back(values, factor, gain, grad):
    unit = values * factor
    scaled = grad * gain
    return factor * (scaled - unit * jnp.mean(scaled * unit, axis=-1, keepdims=True))


def split_ring(count):
    if count % 16 == 0:
        return (4, count // 8, 2)
    return (count, 1, 1)


def position(index, dims):
    return (index // (dims[1] * dims[2]), (index // dims[2]) % dims[1], index % dims[2])


def flat(spot, dims):
    return (spot[0] * dims[1] + spot[1]) * dims[2] + spot[2]


class Gather:
    def __init__(self, dims, spot, send, recv):
        self.dims, self.spot, self.send, self.recv = dims, spot, send, recv

    def place(self, piece, step, along=None):
        whole, columns, order = piece[:3]
        spot = list(self.spot)
        if along is not None:
            spot[order[step]] = along
        place = tuple(
            slice(None) if other in order[:step] else spot[other] for other in range(3)
        )
        return whole.at[place + (slice(None), columns)]

    def lined(self, piece, step):
        return piece[4] and piece[2][step] == 0 and self.dims[0] == 4

    def copies(self, piece, step, offsets=None):
        _, _, order, row, _ = piece
        axis = order[step]
        target = self.place(piece, step)
        base = sum(self.dims[other] - 1 for other in order[:step])
        out = []
        for offset in offsets or range(1, self.dims[axis]):
            peer = list(self.spot)
            peer[axis] = lax.rem(self.spot[axis] + offset, self.dims[axis])
            out.append(
                pltpu.make_async_remote_copy(
                    src_ref=target,
                    dst_ref=target,
                    send_sem=self.send.at[row, base + offset - 1],
                    recv_sem=self.recv.at[row, base + offset - 1],
                    device_id={"dp": flat(peer, self.dims)},
                    device_id_type=MESH,
                )
            )
        return out

    def passed(self, piece, step, here):
        _, _, order, row, _ = piece
        block = self.place(piece, step, 3 if here == 1 else 0)
        base = sum(self.dims[other] - 1 for other in order[:step])
        lanes = sum(d - 1 for d in self.dims)
        peer = list(self.spot)
        peer[0] = 0 if here == 1 else 3
        return pltpu.make_async_remote_copy(
            src_ref=block,
            dst_ref=block,
            send_sem=self.send.at[row, lanes],
            recv_sem=self.recv.at[row, base + (0 if here == 1 else 2)],
            device_id={"dp": flat(peer, self.dims)},
            device_id_type=MESH,
        )

    def own(self, piece, step, act):
        copies = self.copies(piece, step)
        if not self.lined(piece, step):
            for copy in copies:
                act(copy)
            return
        act(copies[1])
        pl.when(self.spot[0] != 3)(lambda: act(copies[0]))
        pl.when(self.spot[0] != 0)(lambda: act(copies[2]))

    def start(self, pieces, step):
        for piece in pieces:
            self.own(piece, step, lambda copy: copy.start())

    def relay(self, pieces, step):
        for piece in pieces:
            if self.lined(piece, step):
                self.copies(piece, step, (2,))[0].wait_recv()
                for here in (1, 2):
                    copy = self.passed(piece, step, here)
                    pl.when(self.spot[0] == here)(copy.start)

    def arrive(self, pieces, step):
        for piece in pieces:
            for copy in self.copies(piece, step, (1, 3) if self.lined(piece, step) else None):
                copy.wait_recv()

    def drain(self, pieces):
        for piece in pieces:
            for step in range(3):
                self.own(piece, step, lambda copy: copy.wait_send())
                if self.lined(piece, step):
                    for here in (1, 2):
                        copy = self.passed(piece, step, here)
                        pl.when(self.spot[0] == here)(copy.wait_send)


def greet(dims, spot, team, member):
    barrier = pltpu.get_barrier_semaphore()
    count = 0
    for axis in range(3):
        for offset in range(1, dims[axis]):
            peer = list(spot)
            peer[axis] = lax.rem(spot[axis] + offset, dims[axis])
            pl.semaphore_signal(
                barrier, inc=1, device_id={"dp": flat(peer, dims)}, device_id_type=MESH
            )
            count += 1
    for offset in range(1, team):
        pl.semaphore_signal(
            barrier,
            inc=1,
            device_id={"tensor": lax.rem(member + offset, team)},
            device_id_type=MESH,
        )
        count += 1
    pl.semaphore_wait(barrier, count)


NAMES = (
    "in_shard",
    "out_shard",
    "gu_shard",
    "down_shard",
    "x_own",
    "g_own",
    "expand",
    "down_shrink",
    "same",
    "conv_gain",
    "ffn_gain",
    "taps",
    "in_reduce",
    "in_lift",
    "out_reduce",
    "out_lift",
    "ffn_reduce",
    "down_lift",
    "mask",
    "pick",
    "io_whole",
    "ff_whole",
    "streams",
    "norm_one",
    "conv_out",
    "code_in",
    "code_out",
    "block_out",
    "grad_x_two",
    "ffn_flat",
    "x_all",
    "g_all",
    "na",
    "nb",
    "w",
    "acc_a",
    "acc_b",
    "x_two",
    "halo",
    "co",
    "cp",
    "gcf",
    "cf",
    "gd",
    "cft",
    "gdt",
    "act",
    "ggu",
    "eb",
    "dsb",
    "rb",
    "rc",
    "rd",
    "code_t",
    "flat",
    "rep",
    "got",
    "send",
    "recv",
    "team_send",
    "team_recv",
    "local",
    "load_sem",
)


class Plan:
    def __init__(self, chunks):
        self.crossed = [4, chunks - 2] if chunks >= 8 else [max(chunks - 2, 0)]
        self.plain = [k for k in range(chunks) if k not in self.crossed]
        self.top = [[] for _ in range(chunks)]
        self.bottom = [[] for _ in range(chunks)]
        for m, k in enumerate(self.plain):
            self.add(self.top, k, "second", m + 3)
            self.add(self.top, k, "relay", m + 4)
            self.add(self.top, k, "first", m + 6)
            self.add(self.bottom, k, "third", m + 2)
        for m, k in enumerate(self.crossed):
            self.top[1 + m].append(("cross_third", k))
            self.top[k - 1 - m].append(("cross_relay", k))

    def add(self, where, at, step, m):
        if m < len(self.plain):
            where[at].append((step, self.plain[m]))


def forward_kernel(shape, *refs):
    s = types.SimpleNamespace(**dict(zip(NAMES, refs)))
    dims, team, width, channels, length, chunks, early = shape
    own = length // team
    hc = HIDDEN_CHUNK
    tile = ROW_TILE
    tiles = length // tile
    own_tile = min(own, tile)
    member = lax.axis_index("tensor")
    spot = position(lax.axis_index("dp"), dims)
    gather = Gather(dims, spot, s.send, s.recv)
    own_rows = pl.ds(pl.multiple_of(member * own, own), own)
    plan = Plan(chunks)

    io_step = 4 * channels // 6
    half = io_step // 2
    io_pieces = [
        [
            (s.io_whole, pl.ds(i * io_step, half), (0, 1, 2), 2 * i, False),
            (s.io_whole, pl.ds(i * io_step + half, half), (0, 2, 1), 2 * i + 1, False),
        ]
        for i in range(6)
    ]
    cut = 640

    def chunk_pieces(k):
        orders = ((1, 2, 0), (2, 1, 0)) if k in plan.crossed else ((0, 1, 2), (0, 2, 1))
        whole = s.ff_whole.at[k]
        return [
            (whole, pl.ds(0, cut), orders[0], 12 + 2 * k, True),
            (whole, pl.ds(cut, 3 * hc - cut), orders[1], 13 + 2 * k, True),
        ]

    def do(step, k):
        pieces = chunk_pieces(k)
        if step == "first" or step == "cross_first":
            gather.start(pieces, 0)
        elif step == "relay":
            gather.relay(pieces, 0)
        elif step == "second" or step == "cross_second":
            gather.arrive(pieces, 0)
            gather.start(pieces, 1)
        elif step == "third" or step == "cross_third":
            gather.arrive(pieces, 1)
            gather.start(pieces, 2)
        elif step == "cross_relay":
            gather.relay(pieces, 2)
        elif step == "last":
            gather.arrive(pieces, 2)

    def do_plain(step, m):
        if m < len(plan.plain):
            do(step, plan.plain[m])

    def team_copies(row, source, target):
        out = []
        for offset in range(1, team):
            peer = lax.rem(member + offset, team)
            out.append(
                pltpu.make_async_remote_copy(
                    src_ref=source(peer, offset),
                    dst_ref=target(peer, offset),
                    send_sem=s.team_send.at[row, offset - 1],
                    recv_sem=s.team_recv.at[row, offset - 1],
                    device_id={"tensor": peer},
                    device_id_type=MESH,
                )
            )
        return out

    def rows_of(ref):
        return lambda peer, offset: ref.at[pl.ds(pl.multiple_of(peer * own, own), own)]

    def slot_of(ref):
        return lambda peer, offset: ref.at[offset - 1]

    def spare(k):
        at = position(1 + k // 2, dims)
        return lambda first, amount: s.w.at[at + (slice(None), pl.ds((k % 2) * 3 * hc + first, amount))]

    io_spare = s.w.at[0, 0, 0, :, pl.ds(0, 4 * channels)]
    ins = [
        [
            pltpu.make_async_copy(
                s.in_shard, s.w.at[0, 0, 0, :, pl.ds(0, 3 * channels)], s.local.at[2]
            ),
            pltpu.make_async_copy(
                s.out_shard, s.w.at[0, 0, 0, :, pl.ds(3 * channels, channels)], s.local.at[3]
            ),
        ]
    ]
    outs = [pltpu.make_async_copy(io_spare, s.io_whole.at[spot], s.local.at[2])]
    for k in range(chunks):
        part = pl.ds(k * hc, hc)
        sources = (s.gu_shard.at[0, :, part], s.gu_shard.at[1, :, part], s.down_shard.at[:, part])
        ins.append(
            [
                pltpu.make_async_copy(source, spare(k)(n * hc, hc), s.local.at[4 + 3 * k + n])
                for n, source in enumerate(sources)
            ]
        )
        outs.append(
            pltpu.make_async_copy(
                spare(k)(0, 3 * hc), s.ff_whole.at[(k,) + spot], s.local.at[4 + 3 * k]
            )
        )
    for copies in ins:
        for copy in copies:
            copy.start()
    greet(dims, spot, team, member)
    x_copies = team_copies(0, lambda p, o: s.x_own, lambda p, o: s.x_all.at[own_rows])
    g_copies = team_copies(1, lambda p, o: s.g_own, lambda p, o: s.g_all.at[own_rows])
    for copy in x_copies + g_copies:
        copy.start()
    x_here = pltpu.make_async_copy(s.x_own, s.x_all.at[own_rows], s.local.at[0])
    g_here = pltpu.make_async_copy(s.g_own, s.g_all.at[own_rows], s.local.at[1])
    for first, second in zip(ins, outs):
        for copy in first:
            copy.wait()
        second.start()
    x_here.start()
    g_here.start()
    outs[0].wait()
    for pieces in io_pieces:
        gather.start(pieces, 0)
    for copy in outs[1:]:
        copy.wait()
    for k in plan.crossed:
        do("cross_first", k)
    do_plain("first", 0)
    do_plain("first", 1)

    x_here.wait()
    for copy in x_copies:
        copy.wait_recv()

    def first_norm(i, carry):
        rows = pl.ds(pl.multiple_of(i * tile, tile), tile)
        values = s.x_all[rows, :].astype(jnp.float32)
        s.na[rows, :] = (values * norm_factor(values) * s.conv_gain[...]).astype(jnp.bfloat16)
        return carry

    def down_codes(i, carry):
        rows = pl.ds(pl.multiple_of(i * tile, tile), tile)
        code = dot_against(s.g_all[rows, :], s.down_lift[...]) * s.mask[...]
        code = code.astype(jnp.bfloat16)
        s.gd[rows, :] = code
        s.gdt[:, rows] = dot_against(s.pick[...], code).astype(jnp.bfloat16)
        return carry

    norm_store = pltpu.make_async_copy(s.na, s.norm_one, s.local.at[0])
    for i in range(7):
        if i == 0:
            lax.fori_loop(0, tiles, first_norm, 0)
            norm_store.start()
        if i == 1:
            g_here.wait()
            for copy in g_copies:
                copy.wait_recv()
            lax.fori_loop(0, tiles, down_codes, 0)
        if i < 6:
            gather.arrive(io_pieces[i], 0)
            gather.start(io_pieces[i], 1)
        if i > 0:
            gather.arrive(io_pieces[i - 1], 1)
            gather.start(io_pieces[i - 1], 2)
    do_plain("relay", 0)
    for k in plan.crossed:
        do("cross_second", k)
    do_plain("relay", 1)
    do_plain("first", 2)
    do_plain("second", 0)
    io_loads = []
    for i in range(6):
        gather.arrive(io_pieces[i], 2)
        columns = pl.ds(i * io_step, io_step)
        load = pltpu.make_async_copy(
            s.io_whole.at[:, :, :, :, columns], s.w.at[:, :, :, :, columns], s.load_sem.at[i]
        )
        load.start()
        io_loads.append(load)
    do_plain("second", 1)
    do_plain("first", 3)
    norm_store.wait()
    for load in io_loads:
        load.wait()

    def weights(first, count):
        return s.w[:, :, :, :, pl.ds(first, count)].reshape(width, count)

    s.halo[pl.ds(0, 8), :] = jnp.zeros((8, channels), jnp.float32)

    def convolve(i, carry):
        rows = pl.ds(pl.multiple_of(i * tile, tile), tile)
        normed = s.na[rows, :]
        code = (dot(normed, s.in_reduce[...]) * s.mask[...]).astype(jnp.bfloat16)
        s.code_in[:, rows] = dot_against(s.pick[...], code).astype(jnp.bfloat16)
        lanes = []
        for lane in range(3):
            value = dot(normed, weights(lane * channels, channels)) + dot(
                code, s.in_lift[:, pl.ds(lane * channels, channels)]
            )
            lanes.append(value)
            if lane < 2:
                s.acc_a[rows, pl.ds(lane * channels, channels)] = value
            else:
                s.acc_b[rows, pl.ds(0, channels)] = value
        product = lanes[0] * lanes[2]
        s.halo[pl.ds(8, tile), :] = product
        masks = s.same[rows, :]
        taps = s.taps[...].astype(jnp.float32)
        mixed = (
            taps[0:1, :] * product
            + taps[1:2, :] * s.halo[pl.ds(7, tile), :] * masks[:, 0:1]
            + taps[2:3, :] * s.halo[pl.ds(6, tile), :] * masks[:, 1:2]
        )
        s.halo[pl.ds(0, 8), :] = s.halo[pl.ds(tile, 8), :]
        convolved = (lanes[1] * mixed).astype(jnp.bfloat16)
        s.co[rows, :] = convolved
        s.na[rows, :] = dot_against(convolved, weights(3 * channels, channels)).astype(jnp.bfloat16)
        s.cp[rows, :] = dot(convolved, s.out_reduce[...])

        @pl.when(i == 1)
        def _():
            do_plain("relay", 2)
            do_plain("third", 0)

        @pl.when(i == 2)
        def _():
            do_plain("first", 4)
            do_plain("second", 2)

        return carry

    lax.fori_loop(0, tiles, convolve, 0)
    stores = [
        pltpu.make_async_copy(s.acc_a.at[:, pl.ds(0, channels)], s.streams.at[0], s.local.at[3]),
        pltpu.make_async_copy(
            s.acc_a.at[:, pl.ds(channels, channels)], s.streams.at[1], s.local.at[4]
        ),
        pltpu.make_async_copy(s.acc_b.at[:, pl.ds(0, channels)], s.streams.at[2], s.local.at[5]),
        pltpu.make_async_copy(s.co, s.conv_out, s.local.at[6]),
    ]
    branch = team_copies(2, rows_of(s.na), slot_of(s.rb))
    codes = team_copies(3, rows_of(s.cp), slot_of(s.rc))
    for copy in codes + branch + stores:
        copy.start()
    do_plain("relay", 3)
    do_plain("first", 5)
    do_plain("third", 1)

    def load(c):
        slot = lax.rem(c, 2)
        columns = pl.ds(pl.multiple_of(slot * 3 * hc, LANES), 3 * hc)
        part = pl.ds(pl.multiple_of(c * hc, LANES), hc)
        return [
            pltpu.make_async_copy(
                s.ff_whole.at[c], s.w.at[:, :, :, :, columns], s.load_sem.at[3 * slot]
            ),
            pltpu.make_async_copy(
                s.expand.at[:, :, part], s.eb.at[slot], s.load_sem.at[3 * slot + 1]
            ),
            pltpu.make_async_copy(s.down_shrink.at[part], s.dsb.at[slot], s.load_sem.at[3 * slot + 2]),
        ]

    for copy in branch + codes:
        copy.wait_recv()
    code = s.cp[own_rows, :]
    for peer in range(team - 1):
        code = code + s.rc[peer]
    code = (code * s.mask[...]).astype(jnp.bfloat16)
    s.code_out[...] = dot_against(s.pick[...], code).astype(jnp.bfloat16)
    s.cf[pl.ds(0, own), pl.ds(0, LANES)] = code

    def second_norm(i, carry):
        local_rows = pl.ds(pl.multiple_of(i * own_tile, own_tile), own_tile)
        rows = pl.ds(pl.multiple_of(member * own + i * own_tile, own_tile), own_tile)
        values = s.x_all[rows, :].astype(jnp.float32) + s.na[rows, :].astype(jnp.float32)
        for peer in range(team - 1):
            values = values + s.rb[peer, local_rows, :].astype(jnp.float32)
        values = values + dot(s.cf[local_rows, pl.ds(0, LANES)], s.out_lift[...])
        s.x_two[local_rows, :] = values
        s.nb[rows, :] = (values * norm_factor(values) * s.ffn_gain[...]).astype(jnp.bfloat16)
        return carry

    lax.fori_loop(0, own // own_tile, second_norm, 0)
    norms = team_copies(4, lambda p, o: s.nb.at[own_rows], lambda p, o: s.nb.at[own_rows])
    for copy in norms:
        copy.start()
    do("last", 0)
    for copy in load(0):
        copy.start()
    for copy in stores:
        copy.wait()
    s.acc_a[...] = jnp.zeros_like(s.acc_a)
    s.acc_b[...] = jnp.zeros_like(s.acc_b)
    for copy in branch + codes:
        copy.wait_send()
    s.cp[...] = jnp.zeros_like(s.cp)
    s.gcf[...] = jnp.zeros_like(s.gcf)
    for copy in norms:
        copy.wait_recv()

    def ffn_codes(i, carry):
        rows = pl.ds(pl.multiple_of(i * tile, tile), tile)
        value = dot(s.nb[rows, :], s.ffn_reduce[...])
        for n in range(2):
            code = (value[:, n * LANES : (n + 1) * LANES] * s.mask[...]).astype(jnp.bfloat16)
            s.cf[rows, pl.ds(n * LANES, LANES)] = code
            s.cft[pl.ds(16 * n, 16), rows] = dot_against(s.pick[...], code).astype(jnp.bfloat16)
        return carry

    lax.fori_loop(0, tiles, ffn_codes, 0)

    def chunk(c, carry):
        for k in range(chunks):
            if plan.top[k]:

                @pl.when(c == k)
                def _():
                    for step, which in plan.top[k]:
                        do(step, which)

        for copy in load(c):
            copy.wait()
        slot = lax.rem(c, 2)
        first = pl.multiple_of(slot * 3 * hc, LANES)
        down_first = pl.multiple_of(slot * 3 * hc + 2 * hc, LANES)

        def row_tile(i, inner):
            rows = pl.ds(pl.multiple_of(i * tile, tile), tile)
            both = dot(s.nb[rows, :], weights(first, 2 * hc))
            grad = dot(s.g_all[rows, :], weights(down_first, hc)) + dot_against(
                s.gd[rows, :], s.dsb[slot]
            )
            gate = both[:, :hc] + dot(s.cf[rows, pl.ds(0, LANES)], s.eb[slot, 0])
            up = both[:, hc:] + dot(s.cf[rows, pl.ds(LANES, LANES)], s.eb[slot, 1])
            gated = jax.nn.sigmoid(gate)
            silu = gate * gated
            act = (silu * up).astype(jnp.bfloat16)
            s.act[rows, :] = act
            grad_gate = (grad * up * gated * (1.0 + gate * (1.0 - gated))).astype(jnp.bfloat16)
            grad_up = (grad * silu).astype(jnp.bfloat16)
            s.ggu[rows, pl.ds(0, hc)] = grad_gate
            s.ggu[rows, pl.ds(hc, hc)] = grad_up
            s.acc_a[rows, :] += dot_against(act, weights(down_first, hc))
            s.cp[rows, :] += dot(act, s.dsb[slot])
            s.acc_b[rows, :] += dot_against(s.ggu[rows, :], weights(first, 2 * hc))
            s.gcf[rows, pl.ds(0, LANES)] += dot_against(grad_gate, s.eb[slot, 0])
            s.gcf[rows, pl.ds(LANES, LANES)] += dot_against(grad_up, s.eb[slot, 1])
            return inner

        lax.fori_loop(0, tiles, row_tile, 0)
        for k in range(chunks - 1):

            @pl.when(c == k)
            def _():
                for step, which in plan.bottom[k]:
                    do(step, which)
                do("last", k + 1)

        @pl.when(c + 1 < chunks)
        def _():
            for copy in load(c + 1):
                copy.start()

        at = pl.multiple_of(c * hc, LANES)
        padded = chunks * hc
        for n in range(2):
            value = dot(s.cft[pl.ds(16 * n, 16), :], s.ggu[:, pl.ds(n * hc, hc)])
            s.flat[:, pl.ds(n * padded + at, hc)] = value.astype(jnp.bfloat16)
        value = dot(s.gdt[...], s.act[...])
        s.flat[:, pl.ds(2 * padded + at, hc)] = value.astype(jnp.bfloat16)
        return carry

    lax.fori_loop(0, chunks, chunk, 0)

    codes = team_copies(7, rows_of(s.cp), slot_of(s.rc))
    for copy in codes:
        copy.start()

    def finish(i, carry):
        rows = pl.ds(pl.multiple_of(i * tile, tile), tile)
        s.na[rows, :] = s.acc_a[rows, :].astype(jnp.bfloat16)
        total = s.acc_b[rows, :]
        for n in range(2):
            lanes = pl.ds(n * LANES, LANES)
            upper, lower = split_pair(s.gcf[rows, lanes] * s.mask[...])
            s.code_t[0, pl.ds(16 * n, 16), rows] = dot_against(s.pick[...], upper).astype(
                jnp.bfloat16
            )
            s.code_t[1, pl.ds(16 * n, 16), rows] = dot_against(s.pick[...], lower).astype(
                jnp.bfloat16
            )
            total = (
                total
                + dot_against(upper, s.ffn_reduce[:, lanes])
                + dot_against(lower, s.ffn_reduce[:, lanes])
            )
        s.acc_b[rows, :] = total
        s.x_all[rows, :] = total.astype(jnp.bfloat16)
        return carry

    lax.fori_loop(0, tiles, finish, 0)
    grads = team_copies(5, rows_of(s.x_all), slot_of(s.rd))
    downs = team_copies(6, rows_of(s.na), slot_of(s.rb))
    for copy in grads + downs:
        copy.start()
    for copy in codes:
        copy.wait_recv()
    code = s.cp[own_rows, :]
    for peer in range(team - 1):
        code = code + s.rc[peer]
    rounded = (code * s.mask[...]).astype(jnp.bfloat16)
    s.cf[pl.ds(0, own), pl.ds(0, LANES)] = rounded
    turned = dot_against(s.pick[...], rounded).astype(jnp.bfloat16)
    shrunk = (dot(s.code_t[0], s.nb[...]) + dot(s.code_t[1], s.nb[...])).astype(jnp.bfloat16)
    s.rep[:, pl.ds(0, width)] = shrunk[:16]
    s.rep[:, pl.ds(width, width)] = shrunk[16:]
    s.rep[:, pl.ds(2 * width, width)] = dot(turned, s.g_all[own_rows, :]).astype(jnp.bfloat16)
    share = early.share
    reps = team_copies(
        8,
        lambda p, o: s.rep.at[:, pl.ds(pl.multiple_of(p * share, LANES), share)],
        slot_of(s.got),
    )
    for copy in reps:
        copy.start()
    for copy in grads + downs:
        copy.wait_recv()
    for copy in norms + grads + downs:
        copy.wait_send()

    def last_rows(i, carry):
        local_rows = pl.ds(pl.multiple_of(i * own_tile, own_tile), own_tile)
        rows = pl.ds(pl.multiple_of(member * own + i * own_tile, own_tile), own_tile)
        values = s.x_two[local_rows, :]
        down = s.acc_a[rows, :]
        grad = s.acc_b[rows, :]
        for peer in range(team - 1):
            down = down + s.rb[peer, local_rows, :].astype(jnp.float32)
            grad = grad + s.rd[peer, local_rows, :].astype(jnp.float32)
        out = values + down + dot(s.cf[local_rows, pl.ds(0, LANES)], s.down_lift[...])
        s.nb[local_rows, :] = out.astype(jnp.bfloat16)
        s.x_two[local_rows, :] = s.g_all[rows, :].astype(jnp.float32) + normalize_back(
            values, norm_factor(values), s.ffn_gain[...], grad
        )
        return carry

    lax.fori_loop(0, own // own_tile, last_rows, 0)
    results = [
        pltpu.make_async_copy(s.nb.at[pl.ds(0, own)], s.block_out, s.local.at[0]),
        pltpu.make_async_copy(s.x_two, s.grad_x_two, s.local.at[1]),
    ]
    for copy in results:
        copy.start()
    for copy in reps:
        copy.wait_recv()
    value = s.rep[:, pl.ds(pl.multiple_of(member * share, LANES), share)].astype(jnp.float32)
    for peer in range(team - 1):
        value = value + s.got[peer].astype(jnp.float32)
    s.flat[:, pl.ds(early.split, share)] = value.astype(jnp.bfloat16)
    rest = s.flat.shape[1] - early.total
    if rest:
        s.flat[:, pl.ds(early.total, rest)] = jnp.zeros((16, rest), jnp.bfloat16)
    flat_store = pltpu.make_async_copy(s.flat, s.ffn_flat, s.local.at[2])
    flat_store.start()
    for copy in x_copies + g_copies + codes + reps:
        copy.wait_send()
    for pieces in io_pieces:
        gather.drain(pieces)
    for k in range(chunks):
        gather.drain(chunk_pieces(k))
    for copy in results:
        copy.wait()
    flat_store.wait()


def forward_and_ffn(dims, team, early, operands):
    in_shard, out_shard, gu_shard, down_shard, x_own = operands[:5]
    rows, channels = out_shard.shape
    hc = HIDDEN_CHUNK
    chunks = down_shard.shape[1] // hc
    own, width = x_own.shape
    length = own * team
    count = dims[0] * dims[1] * dims[2]
    columns = max(4 * channels, 6 * hc)
    lanes = sum(d - 1 for d in dims) + 1
    shape = (dims, team, width, channels, length, chunks, early)
    bf16, f32 = jnp.bfloat16, jnp.float32
    anywhere = pl.BlockSpec(memory_space=pl.ANY)
    vmem = pl.BlockSpec(memory_space=pltpu.VMEM)
    outs = [
        (dims + (rows, 4 * channels), bf16, anywhere),
        ((chunks,) + dims + (rows, 3 * hc), bf16, anywhere),
        ((3, length, channels), f32, anywhere),
        ((length, width), bf16, anywhere),
        ((length, channels), bf16, anywhere),
        ((16, length), bf16, vmem),
        ((16, own), bf16, vmem),
        ((own, width), bf16, anywhere),
        ((own, width), f32, anywhere),
        ((16, count * early.block), bf16, anywhere),
    ]
    peers = max(team - 1, 1)
    row_count = 12 + 2 * chunks
    scratch = [
        pltpu.VMEM((length, width), bf16),
        pltpu.VMEM((length, width), bf16),
        pltpu.VMEM((length, width), bf16),
        pltpu.VMEM((length, width), bf16),
        pltpu.VMEM(dims + (rows, columns), bf16),
        pltpu.VMEM((length, width), f32),
        pltpu.VMEM((length, width), f32),
        pltpu.VMEM((own, width), f32),
        pltpu.VMEM((ROW_TILE + 8, channels), f32),
        pltpu.VMEM((length, channels), bf16),
        pltpu.VMEM((length, LANES), f32),
        pltpu.VMEM((length, 2 * LANES), f32),
        pltpu.VMEM((length, 2 * LANES), bf16),
        pltpu.VMEM((length, LANES), bf16),
        pltpu.VMEM((32, length), bf16),
        pltpu.VMEM((16, length), bf16),
        pltpu.VMEM((length, hc), bf16),
        pltpu.VMEM((length, 2 * hc), bf16),
        pltpu.VMEM((2, 2, LANES, hc), bf16),
        pltpu.VMEM((2, hc, LANES), bf16),
        pltpu.VMEM((peers, own, width), bf16),
        pltpu.VMEM((peers, own, LANES), f32),
        pltpu.VMEM((peers, own, width), bf16),
        pltpu.VMEM((2, 32, length), bf16),
        pltpu.VMEM((16, count * early.block), bf16),
        pltpu.VMEM((16, early.shared), bf16),
        pltpu.VMEM((peers, 16, early.share), bf16),
        pltpu.SemaphoreType.DMA((row_count, lanes)),
        pltpu.SemaphoreType.DMA((row_count, lanes)),
        pltpu.SemaphoreType.DMA((9, peers)),
        pltpu.SemaphoreType.DMA((9, peers)),
        pltpu.SemaphoreType.DMA((max(4 + 3 * chunks, 8),)),
        pltpu.SemaphoreType.DMA((6,)),
    ]
    return pl.pallas_call(
        functools.partial(forward_kernel, shape),
        out_shape=[jax.ShapeDtypeStruct(o[0], o[1]) for o in outs],
        in_specs=[anywhere] * 8 + [vmem] * 12,
        out_specs=[o[2] for o in outs],
        scratch_shapes=scratch,
        compiler_params=pltpu.CompilerParams(
            collective_id=0, has_side_effects=True, vmem_limit_bytes=67043328
        ),
    )(*operands)


BACK_NAMES = (
    "grad_x_two",
    "ffn_flat",
    "io_whole",
    "streams",
    "norm_one",
    "conv_out",
    "x_own",
    "code_in",
    "code_out",
    "same",
    "conv_gain",
    "taps",
    "in_reduce",
    "in_lift",
    "out_reduce",
    "out_lift",
    "mask",
    "pick",
    "onehot",
    "grad_residual",
    "early",
    "late",
    "early_rep",
    "late_rep",
    "w",
    "gx",
    "gb",
    "gco",
    "gcot",
    "st",
    "gs",
    "gci",
    "ha",
    "hb",
    "halo",
    "na",
    "co",
    "pb",
    "gcit",
    "xo",
    "rb",
    "rep_b",
    "got_b",
    "flat_a",
    "flat_b",
    "part_a",
    "part_b",
    "from_a",
    "from_b",
    "sum_a",
    "sum_b",
    "spare_a",
    "spare_b",
    "out",
    "send",
    "recv",
    "swap_send",
    "swap_recv",
    "team_send",
    "team_recv",
    "local",
)


class Share:
    def __init__(self, count, team, split, shared):
        self.split, self.shared, self.share = split, shared, shared // team
        self.total = split + self.share
        self.block = -(-self.total // (LANES * count)) * LANES
        self.first = split // self.block
        self.blocks = -(-self.total // self.block) - self.first


def backward_kernel(shape, *refs):
    s = types.SimpleNamespace(**dict(zip(BACK_NAMES, refs)))
    dims, team, width, channels, length, early, late = shape
    count = dims[0] * dims[1] * dims[2]
    own = length // team
    tile = ROW_TILE
    tiles = length // tile
    own_tile = min(own, tile)
    member = lax.axis_index("tensor")
    me = lax.axis_index("dp")
    spot = position(me, dims)
    gather = Gather(dims, spot, s.send, s.recv)
    own_rows = pl.ds(pl.multiple_of(member * own, own), own)

    def enter():
        barrier = pltpu.get_barrier_semaphore()
        for offset in range(1, count):
            pl.semaphore_signal(
                barrier, inc=1, device_id={"dp": lax.rem(me + offset, count)}, device_id_type=MESH
            )
        for offset in range(1, team):
            pl.semaphore_signal(
                barrier,
                inc=1,
                device_id={"tensor": lax.rem(member + offset, team)},
                device_id_type=MESH,
            )
        pl.semaphore_wait(barrier, count - 1 + team - 1)

    def team_copies(row, source, target):
        out = []
        for offset in range(1, team):
            peer = lax.rem(member + offset, team)
            out.append(
                pltpu.make_async_remote_copy(
                    src_ref=source(peer, offset),
                    dst_ref=target(peer, offset),
                    send_sem=s.team_send.at[row, offset - 1],
                    recv_sem=s.team_recv.at[row, offset - 1],
                    device_id={"tensor": peer},
                    device_id_type=MESH,
                )
            )
        return out

    def swap_copies(row, part, landing):
        out = []
        for offset in range(1, count):
            peer = lax.rem(me + offset, count)
            out.append(
                pltpu.make_async_remote_copy(
                    src_ref=part.at[peer],
                    dst_ref=landing.at[me],
                    send_sem=s.swap_send.at[row, offset - 1],
                    recv_sem=s.swap_recv.at[row, offset - 1],
                    device_id={"dp": peer},
                    device_id_type=MESH,
                )
            )
        return out

    def pieces_of(share, whole, row):
        out = []
        step = max(share.block // 384, 1) * LANES
        for n, first in enumerate(range(0, share.block, step)):
            order = (0, 1, 2) if n % 2 == 0 else (0, 2, 1)
            out.append((whole, pl.ds(first, min(step, share.block - first)), order, row + n, False))
        return out

    def forward_on(pieces, step):
        for piece in pieces:
            gather.arrive([piece], step)
            gather.start([piece], step + 1)

    def hand_out(share, columns, part, landing, row):
        for peer in range(count):
            part[peer, :, pl.ds(0, share.block)] = columns[:, pl.ds(peer * share.block, share.block)]
            part[peer, :, pl.ds(share.block, LANES)] = s.onehot[...]
        landing[me] = part[me]
        copies = swap_copies(row, part, landing)
        for copy in copies:
            copy.start()
        return copies

    def take_in(share, landing, total):
        for adapter in range(ADAPTER_COUNT):

            def add(source, value):
                mask = landing[source, adapter : adapter + 1, pl.ds(share.block, LANES)]
                mask = mask.astype(jnp.float32)[:, 0:1]
                return value + mask * landing[source, :, pl.ds(0, share.block)].astype(jnp.float32)

            value = lax.fori_loop(0, count, add, jnp.zeros((16, share.block), jnp.float32))
            total[pl.ds(adapter * 16, 16), :] = value.astype(jnp.bfloat16)

    loads = {}
    for slot, (name, source, target) in enumerate(
        [
            ("flat", s.ffn_flat, s.flat_a),
            ("gx", s.grad_x_two, s.gx),
            ("co", s.conv_out, s.co),
            ("w", s.io_whole, s.w),
            ("b", s.streams.at[0], s.st.at[0, pl.ds(8, length)]),
            ("c", s.streams.at[1], s.st.at[1, pl.ds(8, length)]),
            ("x", s.streams.at[2], s.st.at[2, pl.ds(8, length)]),
            ("na", s.norm_one, s.na),
            ("xo", s.x_own, s.xo),
        ]
    ):
        loads[name] = pltpu.make_async_copy(source, target, s.local.at[slot])
        loads[name].start()
    enter()
    loads["flat"].wait()
    sent_a = hand_out(early, s.flat_a, s.part_a, s.from_a, 0)
    s.st[0, pl.ds(0, 8), :] = jnp.zeros((8, channels), jnp.float32)
    s.st[2, pl.ds(0, 8), :] = jnp.zeros((8, channels), jnp.float32)
    s.ha[pl.ds(tile, 8), :] = jnp.zeros((8, channels), jnp.float32)
    s.hb[pl.ds(tile, 8), :] = jnp.zeros((8, channels), jnp.float32)
    loads["gx"].wait()

    def branch_rows(i, carry):
        local_rows = pl.ds(pl.multiple_of(i * own_tile, own_tile), own_tile)
        rows = pl.ds(pl.multiple_of(member * own + i * own_tile, own_tile), own_tile)
        upper, lower = split_pair(s.gx[local_rows, :])
        s.gb[rows, :] = upper
        code = dot_against(upper, s.out_lift[...]) + dot_against(lower, s.out_lift[...])
        s.gco[rows, :] = (code * s.mask[...]).astype(jnp.bfloat16)
        return carry

    lax.fori_loop(0, own // own_tile, branch_rows, 0)
    swaps = team_copies(0, lambda p, o: s.gb.at[own_rows], lambda p, o: s.gb.at[own_rows])
    swaps += team_copies(1, lambda p, o: s.gco.at[own_rows], lambda p, o: s.gco.at[own_rows])
    for copy in swaps:
        copy.start()
    upper, lower = split_pair(s.gx[...])
    s.rep_b[:, pl.ds(width, width)] = (
        dot(s.code_out[...], upper) + dot(s.code_out[...], lower)
    ).astype(jnp.bfloat16)
    for copy in swaps:
        copy.wait_recv()

    def turn(i, carry):
        rows = pl.ds(pl.multiple_of(i * tile, tile), tile)
        s.gcot[:, rows] = dot_against(s.pick[...], s.gco[rows, :]).astype(jnp.bfloat16)
        return carry

    lax.fori_loop(0, tiles, turn, 0)
    loads["co"].wait()
    s.flat_b[:, pl.ds(3 * channels, channels)] = dot(s.gcot[...], s.co[...]).astype(jnp.bfloat16)
    pieces_a = pieces_of(early, s.early, 0)
    pieces_b = pieces_of(late, s.late, len(pieces_a))
    place_a = pltpu.make_async_copy(s.sum_a, s.early.at[spot], s.local.at[0])
    place_b = pltpu.make_async_copy(s.sum_b, s.late.at[spot], s.local.at[1])

    for name in ("w", "b", "c", "x"):
        loads[name].wait()

    def weights(first, amount):
        return s.w[:, :, :, :, pl.ds(first, amount)].reshape(width, amount)

    def back(j, carry):
        i = tiles - 1 - j
        start = pl.multiple_of(i * tile, tile)
        rows = pl.ds(start, tile)
        later = pl.ds(pl.multiple_of(start + 8, 8), tile)
        grad = dot(s.gb[rows, :], weights(3 * channels, channels)) + dot_against(
            s.gco[rows, :], s.out_reduce[...]
        )
        s.halo[pl.ds(0, 8), :] = s.st[0, pl.ds(start, 8), :] * s.st[2, pl.ds(start, 8), :]
        product = s.st[0, later, :] * s.st[2, later, :]
        s.halo[pl.ds(8, tile), :] = product
        masks = s.same[rows, :]
        taps = s.taps[...].astype(jnp.float32)
        mixed = (
            taps[0:1, :] * product
            + taps[1:2, :] * s.halo[pl.ds(7, tile), :] * masks[:, 0:1]
            + taps[2:3, :] * s.halo[pl.ds(6, tile), :] * masks[:, 1:2]
        )
        grad_mixed = grad * s.st[1, later, :]
        s.ha[pl.ds(0, tile), :] = taps[1:2, :] * grad_mixed * masks[:, 0:1]
        s.hb[pl.ds(0, tile), :] = taps[2:3, :] * grad_mixed * masks[:, 1:2]
        grad_product = taps[0:1, :] * grad_mixed + s.ha[pl.ds(1, tile), :] + s.hb[pl.ds(2, tile), :]
        s.ha[pl.ds(tile, 8), :] = s.ha[pl.ds(0, 8), :]
        s.hb[pl.ds(tile, 8), :] = s.hb[pl.ds(0, 8), :]
        s.gs[rows, pl.ds(0, channels)] = (grad_product * s.st[2, later, :]).astype(jnp.bfloat16)
        s.gs[rows, pl.ds(channels, channels)] = (grad * mixed).astype(jnp.bfloat16)
        s.gs[rows, pl.ds(2 * channels, channels)] = (grad_product * s.st[0, later, :]).astype(
            jnp.bfloat16
        )
        upper, lower = split_pair(dot_against(s.gs[rows, :], s.in_lift[...]) * s.mask[...])
        s.gci[0, rows, :] = upper
        s.gci[1, rows, :] = lower
        s.gcit[0, :, rows] = dot_against(s.pick[...], upper).astype(jnp.bfloat16)
        s.gcit[1, :, rows] = dot_against(s.pick[...], lower).astype(jnp.bfloat16)

        @pl.when(j == 0)
        def _():
            for copy in sent_a:
                copy.wait_recv()
            take_in(early, s.from_a, s.sum_a)
            place_a.start()

        @pl.when(j == 1)
        def _():
            place_a.wait()
            gather.start(pieces_a, 0)

        return carry

    lax.fori_loop(0, tiles, back, 0)
    forward_on(pieces_a[:2], 0)
    loads["na"].wait()
    s.rep_b[:, pl.ds(0, width)] = (
        dot(s.gcit[0], s.na[...]) + dot(s.gcit[1], s.na[...])
    ).astype(jnp.bfloat16)
    share = late.share
    more = team_copies(
        2,
        lambda p, o: s.rep_b.at[:, pl.ds(pl.multiple_of(p * share, LANES), share)],
        lambda p, o: s.got_b.at[o - 1],
    )
    for copy in more:
        copy.start()
    s.flat_b[:, pl.ds(0, 3 * channels)] = dot(s.code_in[...], s.gs[...]).astype(jnp.bfloat16)
    for copy in more:
        copy.wait_recv()
    value = s.rep_b[:, pl.ds(pl.multiple_of(member * share, LANES), share)].astype(jnp.float32)
    for peer in range(team - 1):
        value = value + s.got_b[peer].astype(jnp.float32)
    s.flat_b[:, pl.ds(late.split, share)] = value.astype(jnp.bfloat16)
    rest = count * late.block - late.total
    if rest:
        s.flat_b[:, pl.ds(late.total, rest)] = jnp.zeros((16, rest), jnp.bfloat16)
    sent_b = hand_out(late, s.flat_b, s.part_b, s.from_b, 1)
    forward_on(pieces_a[2:], 0)
    grads = team_copies(
        3,
        lambda p, o: s.pb.at[pl.ds(pl.multiple_of(p * own, own), own)],
        lambda p, o: s.rb.at[o - 1],
    )
    per_own = own // tile

    def norm_grads(j, carry):
        i = lax.rem((member + 1) * per_own + j, tiles)
        rows = pl.ds(pl.multiple_of(i * tile, tile), tile)
        s.pb[rows, :] = (
            dot_against(s.gs[rows, :], weights(0, 3 * channels))
            + dot_against(s.gci[0, rows, :], s.in_reduce[...])
            + dot_against(s.gci[1, rows, :], s.in_reduce[...])
        ).astype(jnp.bfloat16)
        for offset in range(1, team):

            @pl.when(j == offset * per_own - 1)
            def _():
                grads[offset - 1].start()

        @pl.when(j == 0)
        def _():
            forward_on(pieces_a[:2], 1)

        @pl.when(j == 1)
        def _():
            for copy in sent_b:
                copy.wait_recv()
            take_in(late, s.from_b, s.sum_b)
            place_b.start()

        @pl.when(j == 2)
        def _():
            place_b.wait()
            gather.start(pieces_b, 0)
            forward_on(pieces_a[2:], 1)

        return carry

    lax.fori_loop(0, tiles, norm_grads, 0)
    loads["xo"].wait()
    forward_on(pieces_b, 0)
    for copy in grads:
        copy.wait_recv()

    def residual_rows(i, carry):
        local_rows = pl.ds(pl.multiple_of(i * own_tile, own_tile), own_tile)
        rows = pl.ds(pl.multiple_of(member * own + i * own_tile, own_tile), own_tile)
        values = s.xo[local_rows, :].astype(jnp.float32)
        grad = s.pb[rows, :].astype(jnp.float32)
        for peer in range(team - 1):
            grad = grad + s.rb[peer, local_rows, :].astype(jnp.float32)
        s.out[local_rows, :] = (
            s.gx[local_rows, :]
            + normalize_back(values, norm_factor(values), s.conv_gain[...], grad)
        ).astype(jnp.bfloat16)
        return carry

    lax.fori_loop(0, own // own_tile, residual_rows, 0)
    result = pltpu.make_async_copy(s.out, s.grad_residual, s.local.at[2])
    result.start()

    def pass_on(share, whole, reps, spare, base):
        lifts = []
        for block in range(share.blocks):
            here = whole.at[position(share.first + block, dims)]
            lifts.append(pltpu.make_async_copy(here, spare.at[block], s.local.at[3 + block]))
        for lift in lifts:
            lift.start()
        for lift in lifts:
            lift.wait()
        out = team_copies(base, lambda p, o: spare, lambda p, o: reps.at[member])
        for copy in out:
            copy.start()
        keep = pltpu.make_async_copy(spare, reps.at[member], s.local.at[3])
        keep.start()
        return out, keep

    forward_on(pieces_b, 1)
    gather.arrive(pieces_a, 2)
    out_a, keep_a = pass_on(early, s.early, s.early_rep, s.spare_a, 4)
    keep_a.wait()
    gather.arrive(pieces_b, 2)
    out_b, keep_b = pass_on(late, s.late, s.late_rep, s.spare_b, 5)
    for copy in out_a + out_b:
        copy.wait_recv()
    for copy in out_a + out_b + swaps + grads + more + sent_a + sent_b:
        copy.wait_send()
    gather.drain(pieces_a + pieces_b)
    keep_b.wait()
    result.wait()


def backward(dims, team, early, late, operands):
    _, _, io_whole, _, _, conv_out, x_own = operands[:7]
    count = dims[0] * dims[1] * dims[2]
    own, width = x_own.shape
    length, channels = conv_out.shape
    lanes = sum(d - 1 for d in dims)
    bf16, f32 = jnp.bfloat16, jnp.float32
    anywhere = pl.BlockSpec(memory_space=pl.ANY)
    vmem = pl.BlockSpec(memory_space=pltpu.VMEM)
    rows = ADAPTER_COUNT * 16
    peers = max(team - 1, 1)
    outs = [
        ((own, width), bf16),
        (dims + (rows, early.block), bf16),
        (dims + (rows, late.block), bf16),
        ((team, early.blocks, rows, early.block), bf16),
        ((team, late.blocks, rows, late.block), bf16),
    ]
    scratch = [
        pltpu.VMEM(io_whole.shape, bf16),
        pltpu.VMEM((own, width), f32),
        pltpu.VMEM((length, width), bf16),
        pltpu.VMEM((length, LANES), bf16),
        pltpu.VMEM((16, length), bf16),
        pltpu.VMEM((3, length + 8, channels), f32),
        pltpu.VMEM((length, 3 * channels), bf16),
        pltpu.VMEM((2, length, LANES), bf16),
        pltpu.VMEM((ROW_TILE + 8, channels), f32),
        pltpu.VMEM((ROW_TILE + 8, channels), f32),
        pltpu.VMEM((ROW_TILE + 8, channels), f32),
        pltpu.VMEM((length, width), bf16),
        pltpu.VMEM((length, channels), bf16),
        pltpu.VMEM((length, width), bf16),
        pltpu.VMEM((2, 16, length), bf16),
        pltpu.VMEM((own, width), bf16),
        pltpu.VMEM((peers, own, width), bf16),
        pltpu.VMEM((16, late.shared), bf16),
        pltpu.VMEM((peers, 16, late.share), bf16),
        pltpu.VMEM((16, count * early.block), bf16),
        pltpu.VMEM((16, count * late.block), bf16),
        pltpu.VMEM((count, 16, early.block + LANES), bf16),
        pltpu.VMEM((count, 16, late.block + LANES), bf16),
        pltpu.VMEM((count, 16, early.block + LANES), bf16),
        pltpu.VMEM((count, 16, late.block + LANES), bf16),
        pltpu.VMEM((rows, early.block), bf16),
        pltpu.VMEM((rows, late.block), bf16),
        pltpu.VMEM((early.blocks, rows, early.block), bf16),
        pltpu.VMEM((late.blocks, rows, late.block), bf16),
        pltpu.VMEM((own, width), bf16),
        pltpu.SemaphoreType.DMA((12, lanes)),
        pltpu.SemaphoreType.DMA((12, lanes)),
        pltpu.SemaphoreType.DMA((2, count - 1)),
        pltpu.SemaphoreType.DMA((2, count - 1)),
        pltpu.SemaphoreType.DMA((6, peers)),
        pltpu.SemaphoreType.DMA((6, peers)),
        pltpu.SemaphoreType.DMA((max(10, 3 + max(early.blocks, late.blocks)),)),
    ]
    return pl.pallas_call(
        functools.partial(backward_kernel, (dims, team, width, channels, length, early, late)),
        out_shape=[jax.ShapeDtypeStruct(*o) for o in outs],
        in_specs=[anywhere] * 7 + [vmem] * (len(operands) - 7),
        out_specs=[anywhere] * 5,
        scratch_shapes=scratch,
        compiler_params=pltpu.CompilerParams(
            collective_id=1, has_side_effects=True, vmem_limit_bytes=67043328
        ),
    )(*operands)


def lagged_segments(segment_ids, lag):
    shifted = jnp.pad(segment_ids, ((0, 0), (lag, 0)), constant_values=-1)[
        :, : segment_ids.shape[1]
    ]
    return (segment_ids == shifted).astype(jnp.float32)


def pad_axis(values, axis, size):
    widths = [(0, 0)] * values.ndim
    widths[axis] = (0, size - values.shape[axis])
    return jnp.pad(values, widths)


def per_device(
    residual,
    cotangent,
    segment_ids,
    adapter_ids,
    conv_gain,
    proj_in,
    conv_taps,
    proj_out,
    ffn_gain,
    gate_up,
    proj_down,
    in_shrink,
    input_lift_weight,
    output_reduce_weight,
    output_lift_weight,
    ffn_reduce_weight,
    ffn_expand,
    down_shrink,
    down_lift_weight,
):
    own, width = residual.shape
    length = segment_ids.shape[1]
    team = length // own
    count = lax.axis_size("dp")
    dims = split_ring(count)
    rows, _, channels = proj_in.shape
    hidden = proj_down.shape[1]
    hc = HIDDEN_CHUNK
    chunks = -(-hidden // hc)
    padded = chunks * hc
    adapter = adapter_ids[0]

    in_shard = proj_in.reshape(rows, 3 * channels)
    gu_shard = pad_axis(jnp.transpose(gate_up, (1, 0, 2)), 2, padded)
    down_shard = pad_axis(proj_down, 1, padded)
    codes = ADAPTER_COUNT * ADAPTER_RANK
    in_reduce = in_shrink.reshape(width, codes)
    in_lift = input_lift_weight.reshape(codes, 3 * channels)
    out_reduce = output_reduce_weight.reshape(channels, codes)
    out_lift = output_lift_weight.reshape(codes, width)
    ffn_reduce = ffn_reduce_weight.reshape(width, 2 * codes)
    expand = pad_axis(ffn_expand.reshape(2, codes, hidden), 2, padded)
    shrink = pad_axis(down_shrink.reshape(hidden, codes), 0, padded)
    down_lift = down_lift_weight.reshape(codes, width)
    lane = jnp.arange(codes, dtype=jnp.int32)[None, :]
    row = jnp.arange(ADAPTER_RANK, dtype=jnp.int32)[:, None]
    mask = (lane // ADAPTER_RANK == adapter).astype(jnp.float32)
    pick = (lane == adapter * ADAPTER_RANK + row).astype(jnp.bfloat16)
    marks = jnp.broadcast_to(row == adapter, (ADAPTER_RANK, LANES)).astype(jnp.bfloat16)
    first_same, second_same = lagged_segments(segment_ids, 1)[0], lagged_segments(segment_ids, 2)[0]
    same = jnp.stack([first_same, second_same], axis=1)
    early = Share(count, team, 3 * padded, 3 * width)
    late = Share(count, team, 4 * channels, 2 * width)
    (
        io_whole,
        _,
        streams,
        norm_one,
        conv_out,
        code_in,
        code_out,
        block_output,
        grad_x_two,
        ffn_flat,
    ) = forward_and_ffn(
        dims,
        team,
        early,
        (
            in_shard,
            proj_out,
            gu_shard,
            down_shard,
            residual,
            cotangent,
            expand,
            shrink,
            same,
            conv_gain.reshape(1, width),
            ffn_gain.reshape(1, width),
            conv_taps,
            in_reduce,
            in_lift,
            out_reduce,
            out_lift,
            ffn_reduce,
            down_lift,
            mask,
            pick,
        ),
    )
    grad_residual, early_sums, late_sums, early_shared, late_shared = backward(
        dims,
        team,
        early,
        late,
        (
            grad_x_two,
            ffn_flat,
            io_whole,
            streams,
            norm_one,
            conv_out,
            residual,
            code_in,
            code_out,
            same,
            conv_gain.reshape(1, width),
            conv_taps,
            in_reduce,
            in_lift,
            out_reduce,
            out_lift,
            mask,
            pick,
            marks,
        ),
    )

    def columns_of(sums, share):
        sums = sums.reshape(count, ADAPTER_COUNT, ADAPTER_RANK, share.block)
        return jnp.transpose(sums, (1, 2, 0, 3)).reshape(
            ADAPTER_COUNT, ADAPTER_RANK, count * share.block
        )

    def shared_columns(sums, share):
        sums = sums.reshape(team, share.blocks, ADAPTER_COUNT, ADAPTER_RANK, share.block)
        sums = jnp.transpose(sums, (2, 3, 0, 1, 4)).reshape(
            ADAPTER_COUNT, ADAPTER_RANK, team, share.blocks * share.block
        )
        skip = share.split - share.first * share.block
        return sums[..., skip : skip + share.share].reshape(
            ADAPTER_COUNT, ADAPTER_RANK, share.shared
        )

    def rows_first(values):
        return jnp.transpose(values, (2, 0, 1)).astype(jnp.float32)

    early_columns, late_columns = columns_of(early_sums, early), columns_of(late_sums, late)
    early_rest, late_rest = shared_columns(early_shared, early), shared_columns(late_shared, late)
    ffn_e = jnp.stack([early_columns[..., :hidden], early_columns[..., padded : padded + hidden]])
    ffn_e = ffn_e.astype(jnp.float32)
    down_s = rows_first(early_columns[..., 2 * padded : 2 * padded + hidden])
    out_s = rows_first(late_columns[..., 3 * channels : 4 * channels])
    ffn_s = jnp.stack(
        [rows_first(early_rest[..., :width]), rows_first(early_rest[..., width : 2 * width])],
        axis=1,
    )
    down_e = early_rest[..., 2 * width : 3 * width].astype(jnp.float32)
    out_e = late_rest[..., width:].astype(jnp.float32)
    in_e = late_columns[..., : 3 * channels].astype(jnp.float32)
    in_e = in_e.reshape(ADAPTER_COUNT, ADAPTER_RANK, 3, channels)
    in_s = rows_first(late_rest[..., :width])
    return (block_output, grad_residual, in_s, in_e, out_s, out_e, ffn_s, ffn_e, down_s, down_e)


def solution(mesh):
    rows = P(("dp", "tensor"), None)
    placed = (
        rows,
        rows,
        P("dp", None),
        P("dp"),
        P(),
        P("dp", None, "tensor"),
        P(None, "tensor"),
        P("dp", "tensor"),
        P(),
        P("dp", None, "tensor"),
        P("dp", "tensor"),
        P(),
        P(None, None, None, "tensor"),
        P("tensor", None, None),
        P(),
        P(),
        P(None, None, None, "tensor"),
        P("tensor", None, None),
        P(),
    )
    return jax.shard_map(
        per_device,
        mesh=mesh,
        in_specs=placed,
        out_specs=(
            rows,
            rows,
            P(),
            P(None, None, None, "tensor"),
            P("tensor", None, None),
            P(),
            P(),
            P(None, None, None, "tensor"),
            P("tensor", None, None),
            P(),
        ),
        check_vma=False,
    )
```

```python
import functools

import jax
import jax.numpy as jnp
from jax import lax
from jax.experimental import pallas as pl
from jax.experimental.pallas import tpu as pltpu
from jax.sharding import PartitionSpec as P

ADAPTER_COUNT = 8
ADAPTER_RANK = 16
EPSILON = 1e-05
MESH = pl.DeviceIdType.MESH
LANES = 128
HIDDEN_CHUNK = 384
ROW_TILE = 256


def dot(left, right):
    return jnp.dot(left, right, preferred_element_type=jnp.float32)


def dot_against(left, right):
    return lax.dot_general(
        left, right, (((1,), (1,)), ((), ())), preferred_element_type=jnp.float32
    )


def split_pair(values):
    upper = values.astype(jnp.bfloat16)
    lower = (values - upper.astype(jnp.float32)).astype(jnp.bfloat16)
    return (upper, lower)


def norm_factor(values):
    return lax.rsqrt(jnp.mean(values * values, axis=-1, keepdims=True) + EPSILON)


def normalize_back(values, factor, gain, grad):
    unit = values * factor
    scaled = grad * gain
    return factor * (scaled - unit * jnp.mean(scaled * unit, axis=-1, keepdims=True))


def split_ring(count):
    if count % 16 == 0:
        return (4, count // 8, 2)
    return (count, 1, 1)


def position(index, dims):
    return (index // (dims[1] * dims[2]), (index // dims[2]) % dims[1], index % dims[2])


def flat(spot, dims):
    return (spot[0] * dims[1] + spot[1]) * dims[2] + spot[2]


class Gather:
    def __init__(self, dims, spot, send, recv):
        self.dims, self.spot, self.send, self.recv = dims, spot, send, recv

    def place(self, piece, step, along=None):
        whole, columns, order = piece[:3]
        spot = list(self.spot)
        if along is not None:
            spot[order[step]] = along
        place = tuple(
            slice(None) if other in order[:step] else spot[other] for other in range(3)
        )
        return whole.at[place + (slice(None), columns)]

    def lined(self, piece, step):
        return piece[4] and piece[2][step] == 0 and self.dims[0] == 4

    def copies(self, piece, step, offsets=None):
        _, _, order, row, _ = piece
        axis = order[step]
        target = self.place(piece, step)
        base = sum(self.dims[other] - 1 for other in order[:step])
        out = []
        for offset in offsets or range(1, self.dims[axis]):
            peer = list(self.spot)
            peer[axis] = lax.rem(self.spot[axis] + offset, self.dims[axis])
            out.append(
                pltpu.make_async_remote_copy(
                    src_ref=target,
                    dst_ref=target,
                    send_sem=self.send.at[row, base + offset - 1],
                    recv_sem=self.recv.at[row, base + offset - 1],
                    device_id={"dp": flat(peer, self.dims)},
                    device_id_type=MESH,
                )
            )
        return out

    def passed(self, piece, step, here):
        _, _, order, row, _ = piece
        block = self.place(piece, step, 3 if here == 1 else 0)
        base = sum(self.dims[other] - 1 for other in order[:step])
        lanes = sum(d - 1 for d in self.dims)
        peer = list(self.spot)
        peer[0] = 0 if here == 1 else 3
        return pltpu.make_async_remote_copy(
            src_ref=block,
            dst_ref=block,
            send_sem=self.send.at[row, lanes],
            recv_sem=self.recv.at[row, base + (0 if here == 1 else 2)],
            device_id={"dp": flat(peer, self.dims)},
            device_id_type=MESH,
        )

    def own(self, piece, step, act):
        copies = self.copies(piece, step)
        if not self.lined(piece, step):
            for copy in copies:
                act(copy)
            return
        act(copies[1])
        pl.when(self.spot[0] != 3)(lambda: act(copies[0]))
        pl.when(self.spot[0] != 0)(lambda: act(copies[2]))

    def start(self, pieces, step):
        for piece in pieces:
            self.own(piece, step, lambda copy: copy.start())

    def relay(self, pieces, step):
        for piece in pieces:
            if self.lined(piece, step):
                self.copies(piece, step, (2,))[0].wait_recv()
                for here in (1, 2):
                    copy = self.passed(piece, step, here)
                    pl.when(self.spot[0] == here)(copy.start)

    def arrive(self, pieces, step):
        for piece in pieces:
            for copy in self.copies(piece, step, (1, 3) if self.lined(piece, step) else None):
                copy.wait_recv()

    def drain(self, pieces):
        for piece in pieces:
            for step in range(3):
                self.own(piece, step, lambda copy: copy.wait_send())
                if self.lined(piece, step):
                    for here in (1, 2):
                        copy = self.passed(piece, step, here)
                        pl.when(self.spot[0] == here)(copy.wait_send)


def greet(dims, spot, team, member):
    barrier = pltpu.get_barrier_semaphore()
    count = 0
    for axis in range(3):
        for offset in range(1, dims[axis]):
            peer = list(spot)
            peer[axis] = lax.rem(spot[axis] + offset, dims[axis])
            pl.semaphore_signal(
                barrier, inc=1, device_id={"dp": flat(peer, dims)}, device_id_type=MESH
            )
            count += 1
    for offset in range(1, team):
        pl.semaphore_signal(
            barrier,
            inc=1,
            device_id={"tensor": lax.rem(member + offset, team)},
            device_id_type=MESH,
        )
        count += 1
    pl.semaphore_wait(barrier, count)


class Plan:
    def __init__(self, chunks):
        self.crossed = [4, chunks - 2] if chunks >= 8 else [max(chunks - 2, 0)]
        self.plain = [k for k in range(chunks) if k not in self.crossed]
        self.top = [[] for _ in range(chunks)]
        self.bottom = [[] for _ in range(chunks)]
        for m, k in enumerate(self.plain):
            self.add(self.top, k, "second", m + 3)
            self.add(self.top, k, "relay", m + 4)
            self.add(self.top, k, "first", m + 6)
            self.add(self.bottom, k, "third", m + 2)
        for m, k in enumerate(self.crossed):
            self.top[1 + m].append(("cross_third", k))
            self.top[k - 1 - m].append(("cross_relay", k))

    def add(self, where, at, step, m):
        if m < len(self.plain):
            where[at].append((step, self.plain[m]))


def forward_kernel(
    shape,
    in_shard_ref,
    out_shard_ref,
    gu_shard_ref,
    down_shard_ref,
    x_own_ref,
    g_own_ref,
    expand_ref,
    down_shrink_ref,
    same_ref,
    conv_gain_ref,
    ffn_gain_ref,
    taps_ref,
    in_reduce_ref,
    in_lift_ref,
    out_reduce_ref,
    out_lift_ref,
    ffn_reduce_ref,
    down_lift_ref,
    mask_ref,
    pick_ref,
    io_whole_ref,
    ff_whole_ref,
    streams_ref,
    norm_one_ref,
    conv_out_ref,
    code_in_ref,
    code_out_ref,
    block_out_ref,
    grad_x_two_ref,
    ffn_flat_ref,
    x_all_ref,
    g_all_ref,
    na_ref,
    nb_ref,
    w_ref,
    acc_a_ref,
    acc_b_ref,
    x_two_ref,
    halo_ref,
    co_ref,
    cp_ref,
    gcf_ref,
    cf_ref,
    gd_ref,
    cft_ref,
    gdt_ref,
    act_ref,
    ggu_ref,
    eb_ref,
    dsb_ref,
    rb_ref,
    rc_ref,
    rd_ref,
    code_t_ref,
    flat_ref,
    rep_ref,
    got_ref,
    send_ref,
    recv_ref,
    team_send_ref,
    team_recv_ref,
    local_ref,
    load_sem_ref,
):
    dims, team, width, channels, length, chunks, early = shape
    own = length // team
    hc = HIDDEN_CHUNK
    tile = ROW_TILE
    tiles = length // tile
    own_tile = min(own, tile)
    per_own = own // tile
    member = lax.axis_index("tensor")
    spot = position(lax.axis_index("dp"), dims)
    gather = Gather(dims, spot, send_ref, recv_ref)
    own_rows = pl.ds(pl.multiple_of(member * own, own), own)
    plan = Plan(chunks)

    io_step = 4 * channels // 6
    half = io_step // 2
    io_pieces = [
        [
            (io_whole_ref, pl.ds(i * io_step, half), (0, 1, 2), 2 * i, False),
            (io_whole_ref, pl.ds(i * io_step + half, half), (0, 2, 1), 2 * i + 1, False),
        ]
        for i in range(6)
    ]
    cut = 640

    def chunk_pieces(k):
        orders = ((1, 2, 0), (2, 1, 0)) if k in plan.crossed else ((0, 1, 2), (0, 2, 1))
        whole = ff_whole_ref.at[k]
        return [
            (whole, pl.ds(0, cut), orders[0], 12 + 2 * k, True),
            (whole, pl.ds(cut, 3 * hc - cut), orders[1], 13 + 2 * k, True),
        ]

    def do(step, k):
        pieces = chunk_pieces(k)
        if step == "first" or step == "cross_first":
            gather.start(pieces, 0)
        elif step == "relay":
            gather.relay(pieces, 0)
        elif step == "second" or step == "cross_second":
            gather.arrive(pieces, 0)
            gather.start(pieces, 1)
        elif step == "third" or step == "cross_third":
            gather.arrive(pieces, 1)
            gather.start(pieces, 2)
        elif step == "cross_relay":
            gather.relay(pieces, 2)
        elif step == "last":
            gather.arrive(pieces, 2)

    def do_plain(step, m):
        if m < len(plan.plain):
            do(step, plan.plain[m])

    def team_copies(row, source, target):
        out = []
        for offset in range(1, team):
            peer = lax.rem(member + offset, team)
            out.append(
                pltpu.make_async_remote_copy(
                    src_ref=source(peer, offset),
                    dst_ref=target(peer, offset),
                    send_sem=team_send_ref.at[row, offset - 1],
                    recv_sem=team_recv_ref.at[row, offset - 1],
                    device_id={"tensor": peer},
                    device_id_type=MESH,
                )
            )
        return out

    def rows_of(ref):
        return lambda peer, offset: ref.at[pl.ds(pl.multiple_of(peer * own, own), own)]

    def slot_of(ref):
        return lambda peer, offset: ref.at[offset - 1]

    def spare(k):
        at = position(1 + k // 2, dims)
        return lambda first, amount: w_ref.at[at + (slice(None), pl.ds((k % 2) * 3 * hc + first, amount))]

    io_spare = w_ref.at[0, 0, 0, :, pl.ds(0, 4 * channels)]
    ins = [
        [
            pltpu.make_async_copy(
                in_shard_ref, w_ref.at[0, 0, 0, :, pl.ds(0, 3 * channels)], local_ref.at[2]
            ),
            pltpu.make_async_copy(
                out_shard_ref, w_ref.at[0, 0, 0, :, pl.ds(3 * channels, channels)], local_ref.at[3]
            ),
        ]
    ]
    outs = [pltpu.make_async_copy(io_spare, io_whole_ref.at[spot], local_ref.at[2])]
    for k in range(chunks):
        part = pl.ds(k * hc, hc)
        sources = (gu_shard_ref.at[0, :, part], gu_shard_ref.at[1, :, part], down_shard_ref.at[:, part])
        ins.append(
            [
                pltpu.make_async_copy(source, spare(k)(n * hc, hc), local_ref.at[4 + 3 * k + n])
                for n, source in enumerate(sources)
            ]
        )
        outs.append(
            pltpu.make_async_copy(
                spare(k)(0, 3 * hc), ff_whole_ref.at[(k,) + spot], local_ref.at[4 + 3 * k]
            )
        )
    for copies in ins:
        for copy in copies:
            copy.start()
    greet(dims, spot, team, member)
    x_copies = team_copies(0, lambda p, o: x_own_ref, lambda p, o: x_all_ref.at[own_rows])
    g_copies = team_copies(1, lambda p, o: g_own_ref, lambda p, o: g_all_ref.at[own_rows])
    for copy in x_copies + g_copies:
        copy.start()
    x_here = pltpu.make_async_copy(x_own_ref, x_all_ref.at[own_rows], local_ref.at[0])
    g_here = pltpu.make_async_copy(g_own_ref, g_all_ref.at[own_rows], local_ref.at[1])
    for first, second in zip(ins, outs):
        for copy in first:
            copy.wait()
        second.start()
    x_here.start()
    g_here.start()
    outs[0].wait()
    for pieces in io_pieces:
        gather.start(pieces, 0)
    for copy in outs[1:]:
        copy.wait()
    for k in plan.crossed:
        do("cross_first", k)
    do_plain("first", 0)
    do_plain("first", 1)

    x_here.wait()
    for copy in x_copies:
        copy.wait_recv()

    def first_norm(i, carry):
        rows = pl.ds(pl.multiple_of(i * tile, tile), tile)
        values = x_all_ref[rows, :].astype(jnp.float32)
        na_ref[rows, :] = (values * norm_factor(values) * conv_gain_ref[...]).astype(jnp.bfloat16)
        return carry

    def down_codes(i, carry):
        rows = pl.ds(pl.multiple_of(i * tile, tile), tile)
        code = dot_against(g_all_ref[rows, :], down_lift_ref[...]) * mask_ref[...]
        code = code.astype(jnp.bfloat16)
        gd_ref[rows, :] = code
        gdt_ref[:, rows] = dot_against(pick_ref[...], code).astype(jnp.bfloat16)
        return carry

    norm_store = pltpu.make_async_copy(na_ref, norm_one_ref, local_ref.at[0])
    for i in range(7):
        if i == 0:
            lax.fori_loop(0, tiles, first_norm, 0)
            norm_store.start()
            for k in plan.crossed:
                do("cross_second", k)
        if i == 1:
            g_here.wait()
            for copy in g_copies:
                copy.wait_recv()
            lax.fori_loop(0, tiles, down_codes, 0)
        if i < 6:
            gather.arrive(io_pieces[i], 0)
            gather.start(io_pieces[i], 1)
        if i > 0:
            gather.arrive(io_pieces[i - 1], 1)
            gather.start(io_pieces[i - 1], 2)
    do_plain("relay", 0)
    do_plain("relay", 1)
    do_plain("first", 2)
    do_plain("second", 0)
    io_loads = []
    for i in range(6):
        gather.arrive(io_pieces[i], 2)
        columns = pl.ds(i * io_step, io_step)
        load = pltpu.make_async_copy(
            io_whole_ref.at[:, :, :, :, columns], w_ref.at[:, :, :, :, columns], load_sem_ref.at[i]
        )
        load.start()
        io_loads.append(load)
    do_plain("second", 1)
    do_plain("first", 3)
    norm_store.wait()
    for load in io_loads:
        load.wait()

    def weights(first, count):
        return w_ref[:, :, :, :, pl.ds(first, count)].reshape(width, count)

    halo_ref[pl.ds(0, 8), :] = jnp.zeros((8, channels), jnp.float32)

    def convolve(i, carry):
        rows = pl.ds(pl.multiple_of(i * tile, tile), tile)
        normed = na_ref[rows, :]
        code = (dot(normed, in_reduce_ref[...]) * mask_ref[...]).astype(jnp.bfloat16)
        code_in_ref[:, rows] = dot_against(pick_ref[...], code).astype(jnp.bfloat16)
        lanes = []
        for lane in range(3):
            value = dot(normed, weights(lane * channels, channels)) + dot(
                code, in_lift_ref[:, pl.ds(lane * channels, channels)]
            )
            lanes.append(value)
            if lane < 2:
                acc_a_ref[rows, pl.ds(lane * channels, channels)] = value
            else:
                acc_b_ref[rows, pl.ds(0, channels)] = value
        product = lanes[0] * lanes[2]
        halo_ref[pl.ds(8, tile), :] = product
        masks = same_ref[rows, :]
        taps = taps_ref[...].astype(jnp.float32)
        mixed = (
            taps[0:1, :] * product
            + taps[1:2, :] * halo_ref[pl.ds(7, tile), :] * masks[:, 0:1]
            + taps[2:3, :] * halo_ref[pl.ds(6, tile), :] * masks[:, 1:2]
        )
        halo_ref[pl.ds(0, 8), :] = halo_ref[pl.ds(tile, 8), :]
        convolved = (lanes[1] * mixed).astype(jnp.bfloat16)
        co_ref[rows, :] = convolved
        na_ref[rows, :] = dot_against(convolved, weights(3 * channels, channels)).astype(jnp.bfloat16)
        cp_ref[rows, :] = dot(convolved, out_reduce_ref[...])

        @pl.when(i == 1)
        def _():
            do_plain("relay", 2)
            do_plain("third", 0)

        @pl.when(i == 2)
        def _():
            do_plain("first", 4)
            do_plain("second", 2)

        return carry

    lax.fori_loop(0, tiles, convolve, 0)
    stores = [
        pltpu.make_async_copy(acc_a_ref.at[:, pl.ds(0, channels)], streams_ref.at[0], local_ref.at[3]),
        pltpu.make_async_copy(
            acc_a_ref.at[:, pl.ds(channels, channels)], streams_ref.at[1], local_ref.at[4]
        ),
        pltpu.make_async_copy(acc_b_ref.at[:, pl.ds(0, channels)], streams_ref.at[2], local_ref.at[5]),
        pltpu.make_async_copy(co_ref, conv_out_ref, local_ref.at[6]),
    ]
    branch = team_copies(2, rows_of(na_ref), slot_of(rb_ref))
    codes = team_copies(3, rows_of(cp_ref), slot_of(rc_ref))
    for copy in codes + branch + stores:
        copy.start()
    do_plain("relay", 3)
    do_plain("first", 5)
    do_plain("third", 1)

    def load(c):
        slot = lax.rem(c, 2)
        columns = pl.ds(pl.multiple_of(slot * 3 * hc, LANES), 3 * hc)
        part = pl.ds(pl.multiple_of(c * hc, LANES), hc)
        return [
            pltpu.make_async_copy(
                ff_whole_ref.at[c], w_ref.at[:, :, :, :, columns], load_sem_ref.at[3 * slot]
            ),
            pltpu.make_async_copy(
                expand_ref.at[:, :, part], eb_ref.at[slot], load_sem_ref.at[3 * slot + 1]
            ),
            pltpu.make_async_copy(down_shrink_ref.at[part], dsb_ref.at[slot], load_sem_ref.at[3 * slot + 2]),
        ]

    for copy in branch + codes:
        copy.wait_recv()
    code = cp_ref[own_rows, :]
    for peer in range(team - 1):
        code = code + rc_ref[peer]
    code = (code * mask_ref[...]).astype(jnp.bfloat16)
    code_out_ref[...] = dot_against(pick_ref[...], code).astype(jnp.bfloat16)
    cf_ref[pl.ds(0, own), pl.ds(0, LANES)] = code

    def second_norm(i, carry):
        local_rows = pl.ds(pl.multiple_of(i * own_tile, own_tile), own_tile)
        rows = pl.ds(pl.multiple_of(member * own + i * own_tile, own_tile), own_tile)
        values = x_all_ref[rows, :].astype(jnp.float32) + na_ref[rows, :].astype(jnp.float32)
        for peer in range(team - 1):
            values = values + rb_ref[peer, local_rows, :].astype(jnp.float32)
        values = values + dot(cf_ref[local_rows, pl.ds(0, LANES)], out_lift_ref[...])
        x_two_ref[local_rows, :] = values
        nb_ref[rows, :] = (values * norm_factor(values) * ffn_gain_ref[...]).astype(jnp.bfloat16)
        return carry

    lax.fori_loop(0, own // own_tile, second_norm, 0)
    norms = team_copies(4, lambda p, o: nb_ref.at[own_rows], lambda p, o: nb_ref.at[own_rows])
    for copy in norms:
        copy.start()
    do("last", 0)
    for copy in load(0):
        copy.start()
    for copy in stores:
        copy.wait()
    acc_a_ref[...] = jnp.zeros_like(acc_a_ref)
    acc_b_ref[...] = jnp.zeros_like(acc_b_ref)
    for copy in branch + codes:
        copy.wait_send()
    cp_ref[...] = jnp.zeros_like(cp_ref)
    gcf_ref[...] = jnp.zeros_like(gcf_ref)
    for copy in norms:
        copy.wait_recv()

    def ffn_codes(i, carry):
        rows = pl.ds(pl.multiple_of(i * tile, tile), tile)
        value = dot(nb_ref[rows, :], ffn_reduce_ref[...])
        for n in range(2):
            code = (value[:, n * LANES : (n + 1) * LANES] * mask_ref[...]).astype(jnp.bfloat16)
            cf_ref[rows, pl.ds(n * LANES, LANES)] = code
            cft_ref[pl.ds(16 * n, 16), rows] = dot_against(pick_ref[...], code).astype(jnp.bfloat16)
        return carry

    lax.fori_loop(0, tiles, ffn_codes, 0)

    codes = team_copies(7, rows_of(cp_ref), slot_of(rc_ref))
    grads = team_copies(5, rows_of(x_all_ref), slot_of(rd_ref))
    downs = team_copies(6, rows_of(na_ref), slot_of(rb_ref))

    def finish(rows):
        na_ref[rows, :] = acc_a_ref[rows, :].astype(jnp.bfloat16)
        total = acc_b_ref[rows, :]
        for n in range(2):
            lanes = pl.ds(n * LANES, LANES)
            upper, lower = split_pair(gcf_ref[rows, lanes] * mask_ref[...])
            code_t_ref[0, pl.ds(16 * n, 16), rows] = dot_against(pick_ref[...], upper).astype(
                jnp.bfloat16
            )
            code_t_ref[1, pl.ds(16 * n, 16), rows] = dot_against(pick_ref[...], lower).astype(
                jnp.bfloat16
            )
            total = (
                total
                + dot_against(upper, ffn_reduce_ref[:, lanes])
                + dot_against(lower, ffn_reduce_ref[:, lanes])
            )
        acc_b_ref[rows, :] = total
        x_all_ref[rows, :] = total.astype(jnp.bfloat16)

    def chunk(c, carry):
        for k in range(chunks):
            if plan.top[k]:

                @pl.when(c == k)
                def _():
                    for step, which in plan.top[k]:
                        do(step, which)

        for copy in load(c):
            copy.wait()
        slot = lax.rem(c, 2)
        first = pl.multiple_of(slot * 3 * hc, LANES)
        down_first = pl.multiple_of(slot * 3 * hc + 2 * hc, LANES)

        def row_tile(j, inner):
            i = lax.rem((member + 1) * per_own + j, tiles)
            rows = pl.ds(pl.multiple_of(i * tile, tile), tile)
            both = dot(nb_ref[rows, :], weights(first, 2 * hc))
            grad = dot(g_all_ref[rows, :], weights(down_first, hc)) + dot_against(
                gd_ref[rows, :], dsb_ref[slot]
            )
            gate = both[:, :hc] + dot(cf_ref[rows, pl.ds(0, LANES)], eb_ref[slot, 0])
            up = both[:, hc:] + dot(cf_ref[rows, pl.ds(LANES, LANES)], eb_ref[slot, 1])
            gated = jax.nn.sigmoid(gate)
            silu = gate * gated
            act = (silu * up).astype(jnp.bfloat16)
            act_ref[rows, :] = act
            grad_gate = (grad * up * gated * (1.0 + gate * (1.0 - gated))).astype(jnp.bfloat16)
            grad_up = (grad * silu).astype(jnp.bfloat16)
            ggu_ref[rows, pl.ds(0, hc)] = grad_gate
            ggu_ref[rows, pl.ds(hc, hc)] = grad_up
            acc_a_ref[rows, :] += dot_against(act, weights(down_first, hc))
            cp_ref[rows, :] += dot(act, dsb_ref[slot])
            acc_b_ref[rows, :] += dot_against(ggu_ref[rows, :], weights(first, 2 * hc))
            gcf_ref[rows, pl.ds(0, LANES)] += dot_against(grad_gate, eb_ref[slot, 0])
            gcf_ref[rows, pl.ds(LANES, LANES)] += dot_against(grad_up, eb_ref[slot, 1])

            @pl.when(c == chunks - 1)
            def _():
                finish(rows)
                for offset in range(1, team):

                    @pl.when(j == offset * per_own - 1)
                    def _():
                        for copies in (codes, grads, downs):
                            copies[offset - 1].start()

            return inner

        lax.fori_loop(0, tiles, row_tile, 0)
        for k in range(chunks - 1):

            @pl.when(c == k)
            def _():
                for step, which in plan.bottom[k]:
                    do(step, which)
                do("last", k + 1)

        @pl.when(c + 1 < chunks)
        def _():
            for copy in load(c + 1):
                copy.start()

        at = pl.multiple_of(c * hc, LANES)
        padded = chunks * hc
        for n in range(2):
            value = dot(cft_ref[pl.ds(16 * n, 16), :], ggu_ref[:, pl.ds(n * hc, hc)])
            flat_ref[:, pl.ds(n * padded + at, hc)] = value.astype(jnp.bfloat16)
        value = dot(gdt_ref[...], act_ref[...])
        flat_ref[:, pl.ds(2 * padded + at, hc)] = value.astype(jnp.bfloat16)
        return carry

    lax.fori_loop(0, chunks, chunk, 0)

    for copy in codes:
        copy.wait_recv()
    code = cp_ref[own_rows, :]
    for peer in range(team - 1):
        code = code + rc_ref[peer]
    rounded = (code * mask_ref[...]).astype(jnp.bfloat16)
    cf_ref[pl.ds(0, own), pl.ds(0, LANES)] = rounded
    turned = dot_against(pick_ref[...], rounded).astype(jnp.bfloat16)
    shrunk = (dot(code_t_ref[0], nb_ref[...]) + dot(code_t_ref[1], nb_ref[...])).astype(jnp.bfloat16)
    rep_ref[:, pl.ds(0, width)] = shrunk[:16]
    rep_ref[:, pl.ds(width, width)] = shrunk[16:]
    rep_ref[:, pl.ds(2 * width, width)] = dot(turned, g_all_ref[own_rows, :]).astype(jnp.bfloat16)
    share = early.share
    reps = team_copies(
        8,
        lambda p, o: rep_ref.at[:, pl.ds(pl.multiple_of(p * share, LANES), share)],
        slot_of(got_ref),
    )
    for copy in reps:
        copy.start()
    for copy in grads + downs:
        copy.wait_recv()
    for copy in norms + grads + downs:
        copy.wait_send()

    def last_rows(i, carry):
        local_rows = pl.ds(pl.multiple_of(i * own_tile, own_tile), own_tile)
        rows = pl.ds(pl.multiple_of(member * own + i * own_tile, own_tile), own_tile)
        values = x_two_ref[local_rows, :]
        down = acc_a_ref[rows, :]
        grad = acc_b_ref[rows, :]
        for peer in range(team - 1):
            down = down + rb_ref[peer, local_rows, :].astype(jnp.float32)
            grad = grad + rd_ref[peer, local_rows, :].astype(jnp.float32)
        out = values + down + dot(cf_ref[local_rows, pl.ds(0, LANES)], down_lift_ref[...])
        nb_ref[local_rows, :] = out.astype(jnp.bfloat16)
        x_two_ref[local_rows, :] = g_all_ref[rows, :].astype(jnp.float32) + normalize_back(
            values, norm_factor(values), ffn_gain_ref[...], grad
        )
        return carry

    lax.fori_loop(0, own // own_tile, last_rows, 0)
    results = [
        pltpu.make_async_copy(nb_ref.at[pl.ds(0, own)], block_out_ref, local_ref.at[0]),
        pltpu.make_async_copy(x_two_ref, grad_x_two_ref, local_ref.at[1]),
    ]
    for copy in results:
        copy.start()
    for copy in reps:
        copy.wait_recv()
    value = rep_ref[:, pl.ds(pl.multiple_of(member * share, LANES), share)].astype(jnp.float32)
    for peer in range(team - 1):
        value = value + got_ref[peer].astype(jnp.float32)
    flat_ref[:, pl.ds(early.split, share)] = value.astype(jnp.bfloat16)
    rest = flat_ref.shape[1] - early.total
    if rest:
        flat_ref[:, pl.ds(early.total, rest)] = jnp.zeros((16, rest), jnp.bfloat16)
    flat_store = pltpu.make_async_copy(flat_ref, ffn_flat_ref, local_ref.at[2])
    flat_store.start()
    for copy in x_copies + g_copies + codes + reps:
        copy.wait_send()
    for pieces in io_pieces:
        gather.drain(pieces)
    for k in range(chunks):
        gather.drain(chunk_pieces(k))
    for copy in results:
        copy.wait()
    flat_store.wait()


def forward_and_ffn(dims, team, early, operands):
    in_shard, out_shard, gu_shard, down_shard, x_own = operands[:5]
    rows, channels = out_shard.shape
    hc = HIDDEN_CHUNK
    chunks = down_shard.shape[1] // hc
    own, width = x_own.shape
    length = own * team
    count = dims[0] * dims[1] * dims[2]
    columns = max(4 * channels, 6 * hc)
    lanes = sum(d - 1 for d in dims) + 1
    shape = (dims, team, width, channels, length, chunks, early)
    bf16, f32 = jnp.bfloat16, jnp.float32
    anywhere = pl.BlockSpec(memory_space=pl.ANY)
    vmem = pl.BlockSpec(memory_space=pltpu.VMEM)
    outs = [
        (dims + (rows, 4 * channels), bf16, anywhere),
        ((chunks,) + dims + (rows, 3 * hc), bf16, anywhere),
        ((3, length, channels), f32, anywhere),
        ((length, width), bf16, anywhere),
        ((length, channels), bf16, anywhere),
        ((16, length), bf16, vmem),
        ((16, own), bf16, vmem),
        ((own, width), bf16, anywhere),
        ((own, width), f32, anywhere),
        ((16, count * early.block), bf16, anywhere),
    ]
    peers = max(team - 1, 1)
    row_count = 12 + 2 * chunks
    scratch = [
        pltpu.VMEM((length, width), bf16),
        pltpu.VMEM((length, width), bf16),
        pltpu.VMEM((length, width), bf16),
        pltpu.VMEM((length, width), bf16),
        pltpu.VMEM(dims + (rows, columns), bf16),
        pltpu.VMEM((length, width), f32),
        pltpu.VMEM((length, width), f32),
        pltpu.VMEM((own, width), f32),
        pltpu.VMEM((ROW_TILE + 8, channels), f32),
        pltpu.VMEM((length, channels), bf16),
        pltpu.VMEM((length, LANES), f32),
        pltpu.VMEM((length, 2 * LANES), f32),
        pltpu.VMEM((length, 2 * LANES), bf16),
        pltpu.VMEM((length, LANES), bf16),
        pltpu.VMEM((32, length), bf16),
        pltpu.VMEM((16, length), bf16),
        pltpu.VMEM((length, hc), bf16),
        pltpu.VMEM((length, 2 * hc), bf16),
        pltpu.VMEM((2, 2, LANES, hc), bf16),
        pltpu.VMEM((2, hc, LANES), bf16),
        pltpu.VMEM((peers, own, width), bf16),
        pltpu.VMEM((peers, own, LANES), f32),
        pltpu.VMEM((peers, own, width), bf16),
        pltpu.VMEM((2, 32, length), bf16),
        pltpu.VMEM((16, count * early.block), bf16),
        pltpu.VMEM((16, 3 * width), bf16),
        pltpu.VMEM((peers, 16, 3 * width // team), bf16),
        pltpu.SemaphoreType.DMA((row_count, lanes)),
        pltpu.SemaphoreType.DMA((row_count, lanes)),
        pltpu.SemaphoreType.DMA((9, peers)),
        pltpu.SemaphoreType.DMA((9, peers)),
        pltpu.SemaphoreType.DMA((max(4 + 3 * chunks, 8),)),
        pltpu.SemaphoreType.DMA((6,)),
    ]
    return pl.pallas_call(
        functools.partial(forward_kernel, shape),
        out_shape=[jax.ShapeDtypeStruct(o[0], o[1]) for o in outs],
        in_specs=[anywhere] * 8 + [vmem] * 12,
        out_specs=[o[2] for o in outs],
        scratch_shapes=scratch,
        compiler_params=pltpu.CompilerParams(
            collective_id=0, has_side_effects=True, vmem_limit_bytes=67043328
        ),
    )(*operands)


class Share:
    def __init__(self, count, team, split, shared):
        self.split, self.shared, self.share = split, shared, shared // team
        self.total = split + self.share
        self.block = -(-self.total // (LANES * count)) * LANES
        self.first = split // self.block
        self.blocks = -(-self.total // self.block) - self.first


def backward_kernel(
    shape,
    grad_x_two_ref,
    ffn_flat_ref,
    io_whole_ref,
    streams_ref,
    norm_one_ref,
    conv_out_ref,
    x_own_ref,
    code_in_ref,
    code_out_ref,
    same_ref,
    conv_gain_ref,
    taps_ref,
    in_reduce_ref,
    in_lift_ref,
    out_reduce_ref,
    out_lift_ref,
    mask_ref,
    pick_ref,
    grad_residual_ref,
    early_ref,
    late_ref,
    early_rep_ref,
    w_ref,
    gx_ref,
    gb_ref,
    gco_ref,
    gcot_ref,
    st_ref,
    gs_ref,
    gci_ref,
    ha_ref,
    hb_ref,
    halo_ref,
    na_ref,
    co_ref,
    pb_ref,
    gcit_ref,
    xo_ref,
    rb_ref,
    rep_b_ref,
    got_b_ref,
    flat_a_ref,
    flat_b_ref,
    part_a_ref,
    part_b_ref,
    from_a_ref,
    from_b_ref,
    sum_a_ref,
    sum_b_ref,
    spare_a_ref,
    out_ref,
    send_ref,
    recv_ref,
    swap_send_ref,
    swap_recv_ref,
    team_send_ref,
    team_recv_ref,
    local_ref,
):
    dims, team, width, channels, length, early, late = shape
    count = dims[0] * dims[1] * dims[2]
    own = length // team
    tile = ROW_TILE
    tiles = length // tile
    own_tile = min(own, tile)
    member = lax.axis_index("tensor")
    me = lax.axis_index("dp")
    spot = position(me, dims)
    gather = Gather(dims, spot, send_ref, recv_ref)
    own_rows = pl.ds(pl.multiple_of(member * own, own), own)

    def enter():
        barrier = pltpu.get_barrier_semaphore()
        for offset in range(1, count):
            pl.semaphore_signal(
                barrier, inc=1, device_id={"dp": lax.rem(me + offset, count)}, device_id_type=MESH
            )
        for offset in range(1, team):
            pl.semaphore_signal(
                barrier,
                inc=1,
                device_id={"tensor": lax.rem(member + offset, team)},
                device_id_type=MESH,
            )
        pl.semaphore_wait(barrier, count - 1 + team - 1)

    def team_copies(row, source, target):
        out = []
        for offset in range(1, team):
            peer = lax.rem(member + offset, team)
            out.append(
                pltpu.make_async_remote_copy(
                    src_ref=source(peer, offset),
                    dst_ref=target(peer, offset),
                    send_sem=team_send_ref.at[row, offset - 1],
                    recv_sem=team_recv_ref.at[row, offset - 1],
                    device_id={"tensor": peer},
                    device_id_type=MESH,
                )
            )
        return out

    def swap_copies(row, part, landing):
        out = []
        for offset in range(1, count):
            peer = lax.rem(me + offset, count)
            out.append(
                pltpu.make_async_remote_copy(
                    src_ref=part.at[peer],
                    dst_ref=landing.at[me],
                    send_sem=swap_send_ref.at[row, offset - 1],
                    recv_sem=swap_recv_ref.at[row, offset - 1],
                    device_id={"dp": peer},
                    device_id_type=MESH,
                )
            )
        return out

    def pieces_of(share, whole, row):
        out = []
        step = max(share.block // 384, 1) * LANES
        for n, first in enumerate(range(0, share.block, step)):
            order = (0, 1, 2) if n % 2 == 0 else (0, 2, 1)
            out.append((whole, pl.ds(first, min(step, share.block - first)), order, row + n, False))
        return out

    def forward_on(pieces, step):
        for piece in pieces:
            gather.arrive([piece], step)
            gather.start([piece], step + 1)

    def hand_out(share, columns, part, landing, row):
        for peer in range(count):
            part[peer, :, pl.ds(0, share.block)] = columns[:, pl.ds(peer * share.block, share.block)]
            part[peer, :, pl.ds(share.block, LANES)] = pick_ref[...]
        landing[me] = part[me]
        copies = swap_copies(row, part, landing)
        for copy in copies:
            copy.start()
        return copies

    def take_in(share, landing, total):
        marks = landing[:, :, pl.ds(share.block, LANES)].reshape(count * 16, LANES)
        marks = jnp.transpose(marks.astype(jnp.float32)).astype(jnp.bfloat16)
        blocks = landing[:, :, pl.ds(0, share.block)].reshape(count * 16, share.block)
        total[...] = dot(marks, blocks).astype(jnp.bfloat16)

    first_columns, later_columns = pl.ds(0, 3 * channels), pl.ds(3 * channels, channels)
    loads = {}
    for slot, (name, source, target) in enumerate(
        [
            ("flat", ffn_flat_ref, flat_a_ref),
            ("gx", grad_x_two_ref, gx_ref),
            ("co", conv_out_ref, co_ref),
            ("w", io_whole_ref.at[:, :, :, :, later_columns], w_ref.at[:, :, :, :, later_columns]),
            ("b", streams_ref.at[0], st_ref.at[0, pl.ds(8, length)]),
            ("c", streams_ref.at[1], st_ref.at[1, pl.ds(8, length)]),
            ("x", streams_ref.at[2], st_ref.at[2, pl.ds(8, length)]),
            ("na", norm_one_ref, na_ref),
            ("xo", x_own_ref, xo_ref),
            ("in", io_whole_ref.at[:, :, :, :, first_columns], w_ref.at[:, :, :, :, first_columns]),
        ]
    ):
        loads[name] = pltpu.make_async_copy(source, target, local_ref.at[slot])
        loads[name].start()
    enter()
    loads["flat"].wait()
    sent_a = hand_out(early, flat_a_ref, part_a_ref, from_a_ref, 0)
    st_ref[0, pl.ds(0, 8), :] = jnp.zeros((8, channels), jnp.float32)
    st_ref[2, pl.ds(0, 8), :] = jnp.zeros((8, channels), jnp.float32)
    ha_ref[pl.ds(tile, 8), :] = jnp.zeros((8, channels), jnp.float32)
    hb_ref[pl.ds(tile, 8), :] = jnp.zeros((8, channels), jnp.float32)
    loads["gx"].wait()

    def branch_rows(i, carry):
        local_rows = pl.ds(pl.multiple_of(i * own_tile, own_tile), own_tile)
        rows = pl.ds(pl.multiple_of(member * own + i * own_tile, own_tile), own_tile)
        upper, lower = split_pair(gx_ref[local_rows, :])
        gb_ref[rows, :] = upper
        code = dot_against(upper, out_lift_ref[...]) + dot_against(lower, out_lift_ref[...])
        gco_ref[rows, :] = (code * mask_ref[...]).astype(jnp.bfloat16)
        return carry

    lax.fori_loop(0, own // own_tile, branch_rows, 0)
    swaps = team_copies(0, lambda p, o: gb_ref.at[own_rows], lambda p, o: gb_ref.at[own_rows])
    swaps += team_copies(1, lambda p, o: gco_ref.at[own_rows], lambda p, o: gco_ref.at[own_rows])
    for copy in swaps:
        copy.start()
    upper, lower = split_pair(gx_ref[...])
    rep_b_ref[:, pl.ds(width, width)] = (
        dot(code_out_ref[...], upper) + dot(code_out_ref[...], lower)
    ).astype(jnp.bfloat16)
    for copy in swaps:
        copy.wait_recv()

    def turn(i, carry):
        rows = pl.ds(pl.multiple_of(i * tile, tile), tile)
        gcot_ref[:, rows] = dot_against(pick_ref[...], gco_ref[rows, :]).astype(jnp.bfloat16)
        return carry

    lax.fori_loop(0, tiles, turn, 0)
    loads["co"].wait()
    flat_b_ref[:, pl.ds(3 * channels, channels)] = dot(gcot_ref[...], co_ref[...]).astype(jnp.bfloat16)
    pieces_a = pieces_of(early, early_ref, 0)
    pieces_b = pieces_of(late, late_ref, len(pieces_a))
    place_a = pltpu.make_async_copy(sum_a_ref, early_ref.at[spot], local_ref.at[0])
    place_b = pltpu.make_async_copy(sum_b_ref, late_ref.at[spot], local_ref.at[1])

    for name in ("w", "b", "c", "x"):
        loads[name].wait()

    def weights(first, amount):
        return w_ref[:, :, :, :, pl.ds(first, amount)].reshape(width, amount)

    for copy in sent_a:
        copy.wait_recv()
    take_in(early, from_a_ref, sum_a_ref)
    place_a.start()

    def back(j, carry):
        i = tiles - 1 - j
        start = pl.multiple_of(i * tile, tile)
        rows = pl.ds(start, tile)
        later = pl.ds(pl.multiple_of(start + 8, 8), tile)
        grad = dot(gb_ref[rows, :], weights(3 * channels, channels)) + dot_against(
            gco_ref[rows, :], out_reduce_ref[...]
        )
        halo_ref[pl.ds(0, 8), :] = st_ref[0, pl.ds(start, 8), :] * st_ref[2, pl.ds(start, 8), :]
        product = st_ref[0, later, :] * st_ref[2, later, :]
        halo_ref[pl.ds(8, tile), :] = product
        masks = same_ref[rows, :]
        taps = taps_ref[...].astype(jnp.float32)
        mixed = (
            taps[0:1, :] * product
            + taps[1:2, :] * halo_ref[pl.ds(7, tile), :] * masks[:, 0:1]
            + taps[2:3, :] * halo_ref[pl.ds(6, tile), :] * masks[:, 1:2]
        )
        grad_mixed = grad * st_ref[1, later, :]
        ha_ref[pl.ds(0, tile), :] = taps[1:2, :] * grad_mixed * masks[:, 0:1]
        hb_ref[pl.ds(0, tile), :] = taps[2:3, :] * grad_mixed * masks[:, 1:2]
        grad_product = taps[0:1, :] * grad_mixed + ha_ref[pl.ds(1, tile), :] + hb_ref[pl.ds(2, tile), :]
        ha_ref[pl.ds(tile, 8), :] = ha_ref[pl.ds(0, 8), :]
        hb_ref[pl.ds(tile, 8), :] = hb_ref[pl.ds(0, 8), :]
        gs_ref[rows, pl.ds(0, channels)] = (grad_product * st_ref[2, later, :]).astype(jnp.bfloat16)
        gs_ref[rows, pl.ds(channels, channels)] = (grad * mixed).astype(jnp.bfloat16)
        gs_ref[rows, pl.ds(2 * channels, channels)] = (grad_product * st_ref[0, later, :]).astype(
            jnp.bfloat16
        )
        upper, lower = split_pair(dot_against(gs_ref[rows, :], in_lift_ref[...]) * mask_ref[...])
        gci_ref[0, rows, :] = upper
        gci_ref[1, rows, :] = lower
        gcit_ref[0, :, rows] = dot_against(pick_ref[...], upper).astype(jnp.bfloat16)
        gcit_ref[1, :, rows] = dot_against(pick_ref[...], lower).astype(jnp.bfloat16)

        @pl.when(j == 0)
        def _():
            place_a.wait()
            gather.start(pieces_a, 0)

        for n in (2, 3):

            @pl.when(j == n)
            def _():
                forward_on(pieces_a[n - 2 : n - 1], 0)

        return carry

    lax.fori_loop(0, tiles, back, 0)
    loads["na"].wait()
    rep_b_ref[:, pl.ds(0, width)] = (
        dot(gcit_ref[0], na_ref[...]) + dot(gcit_ref[1], na_ref[...])
    ).astype(jnp.bfloat16)
    more = team_copies(2, lambda p, o: rep_b_ref, lambda p, o: got_b_ref.at[o - 1])
    for copy in more:
        copy.start()
    forward_on(pieces_a[2:3], 0)
    flat_b_ref[:, pl.ds(0, 3 * channels)] = dot(code_in_ref[...], gs_ref[...]).astype(jnp.bfloat16)
    for copy in more:
        copy.wait_recv()
    value = rep_b_ref[...].astype(jnp.float32)
    for peer in range(team - 1):
        value = value + got_b_ref[peer].astype(jnp.float32)
    flat_b_ref[:, pl.ds(late.split, 2 * width)] = value.astype(jnp.bfloat16)
    rest = count * late.block - late.total
    if rest:
        flat_b_ref[:, pl.ds(late.total, rest)] = jnp.zeros((16, rest), jnp.bfloat16)
    sent_b = hand_out(late, flat_b_ref, part_b_ref, from_b_ref, 1)
    forward_on(pieces_a[:1], 1)
    loads["in"].wait()
    grads = team_copies(
        6,
        lambda p, o: pb_ref.at[pl.ds(pl.multiple_of(p * own, own), own)],
        lambda p, o: rb_ref.at[o - 1],
    )
    per_own = own // tile

    def norm_grads(j, carry):
        i = lax.rem((member + 1) * per_own + j, tiles)
        rows = pl.ds(pl.multiple_of(i * tile, tile), tile)
        pb_ref[rows, :] = (
            dot_against(gs_ref[rows, :], weights(0, 3 * channels))
            + dot_against(gci_ref[0, rows, :], in_reduce_ref[...])
            + dot_against(gci_ref[1, rows, :], in_reduce_ref[...])
        ).astype(jnp.bfloat16)
        for offset in range(1, team):

            @pl.when(j == offset * per_own - 1)
            def _():
                grads[offset - 1].start()

        @pl.when(j == 0)
        def _():
            forward_on(pieces_a[3:], 0)
            forward_on(pieces_a[1:2], 1)

        @pl.when(j == 1)
        def _():
            for copy in sent_b:
                copy.wait_recv()
            take_in(late, from_b_ref, sum_b_ref)
            place_b.start()

        @pl.when(j == 2)
        def _():
            place_b.wait()
            gather.start(pieces_b, 0)
            forward_on(pieces_a[2:3], 1)

        return carry

    lax.fori_loop(0, tiles, norm_grads, 0)
    loads["xo"].wait()
    forward_on(pieces_a[3:], 1)
    forward_on(pieces_b, 0)
    for copy in grads:
        copy.wait_recv()

    def residual_rows(i, carry):
        local_rows = pl.ds(pl.multiple_of(i * own_tile, own_tile), own_tile)
        rows = pl.ds(pl.multiple_of(member * own + i * own_tile, own_tile), own_tile)
        values = xo_ref[local_rows, :].astype(jnp.float32)
        grad = pb_ref[rows, :].astype(jnp.float32)
        for peer in range(team - 1):
            grad = grad + rb_ref[peer, local_rows, :].astype(jnp.float32)
        out_ref[local_rows, :] = (
            gx_ref[local_rows, :]
            + normalize_back(values, norm_factor(values), conv_gain_ref[...], grad)
        ).astype(jnp.bfloat16)
        return carry

    lax.fori_loop(0, own // own_tile, residual_rows, 0)
    result = pltpu.make_async_copy(out_ref, grad_residual_ref, local_ref.at[2])
    result.start()

    def pass_on(share, whole, reps, spare, base):
        lifts = []
        for block in range(share.blocks):
            here = whole.at[position(share.first + block, dims)]
            lifts.append(pltpu.make_async_copy(here, spare.at[block], local_ref.at[3 + block]))
        for lift in lifts:
            lift.start()
        for lift in lifts:
            lift.wait()
        out = team_copies(base, lambda p, o: spare, lambda p, o: reps.at[member])
        for copy in out:
            copy.start()
        keep = pltpu.make_async_copy(spare, reps.at[member], local_ref.at[3])
        keep.start()
        return out, keep

    forward_on(pieces_b, 1)
    gather.arrive(pieces_a, 2)
    out_a, keep_a = pass_on(early, early_ref, early_rep_ref, spare_a_ref, 4)
    gather.arrive(pieces_b, 2)
    for copy in out_a:
        copy.wait_recv()
    for copy in out_a + swaps + grads + more + sent_a + sent_b:
        copy.wait_send()
    gather.drain(pieces_a + pieces_b)
    keep_a.wait()
    result.wait()


def backward(dims, team, early, late, operands):
    _, _, io_whole, _, _, conv_out, x_own = operands[:7]
    count = dims[0] * dims[1] * dims[2]
    own, width = x_own.shape
    length, channels = conv_out.shape
    lanes = sum(d - 1 for d in dims)
    bf16, f32 = jnp.bfloat16, jnp.float32
    anywhere = pl.BlockSpec(memory_space=pl.ANY)
    vmem = pl.BlockSpec(memory_space=pltpu.VMEM)
    rows = ADAPTER_COUNT * 16
    peers = max(team - 1, 1)
    outs = [
        ((own, width), bf16),
        (dims + (rows, early.block), bf16),
        (dims + (rows, late.block), bf16),
        ((team, early.blocks, rows, early.block), bf16),
    ]
    scratch = [
        pltpu.VMEM(io_whole.shape, bf16),
        pltpu.VMEM((own, width), f32),
        pltpu.VMEM((length, width), bf16),
        pltpu.VMEM((length, LANES), bf16),
        pltpu.VMEM((16, length), bf16),
        pltpu.VMEM((3, length + 8, channels), f32),
        pltpu.VMEM((length, 3 * channels), bf16),
        pltpu.VMEM((2, length, LANES), bf16),
        pltpu.VMEM((ROW_TILE + 8, channels), f32),
        pltpu.VMEM((ROW_TILE + 8, channels), f32),
        pltpu.VMEM((ROW_TILE + 8, channels), f32),
        pltpu.VMEM((length, width), bf16),
        pltpu.VMEM((length, channels), bf16),
        pltpu.VMEM((length, width), bf16),
        pltpu.VMEM((2, 16, length), bf16),
        pltpu.VMEM((own, width), bf16),
        pltpu.VMEM((peers, own, width), bf16),
        pltpu.VMEM((16, 2 * width), bf16),
        pltpu.VMEM((peers, 16, 2 * width), bf16),
        pltpu.VMEM((16, count * early.block), bf16),
        pltpu.VMEM((16, count * late.block), bf16),
        pltpu.VMEM((count, 16, early.block + LANES), bf16),
        pltpu.VMEM((count, 16, late.block + LANES), bf16),
        pltpu.VMEM((count, 16, early.block + LANES), bf16),
        pltpu.VMEM((count, 16, late.block + LANES), bf16),
        pltpu.VMEM((rows, early.block), bf16),
        pltpu.VMEM((rows, late.block), bf16),
        pltpu.VMEM((early.blocks, rows, early.block), bf16),
        pltpu.VMEM((own, width), bf16),
        pltpu.SemaphoreType.DMA((12, lanes)),
        pltpu.SemaphoreType.DMA((12, lanes)),
        pltpu.SemaphoreType.DMA((2, count - 1)),
        pltpu.SemaphoreType.DMA((2, count - 1)),
        pltpu.SemaphoreType.DMA((7, peers)),
        pltpu.SemaphoreType.DMA((7, peers)),
        pltpu.SemaphoreType.DMA((max(10, 3 + early.blocks),)),
    ]
    return pl.pallas_call(
        functools.partial(backward_kernel, (dims, team, width, channels, length, early, late)),
        out_shape=[jax.ShapeDtypeStruct(*o) for o in outs],
        in_specs=[anywhere] * 7 + [vmem] * (len(operands) - 7),
        out_specs=[anywhere] * 4,
        scratch_shapes=scratch,
        compiler_params=pltpu.CompilerParams(
            collective_id=1, has_side_effects=True, vmem_limit_bytes=67043328
        ),
    )(*operands)


def lagged_segments(segment_ids, lag):
    shifted = jnp.pad(segment_ids, ((0, 0), (lag, 0)), constant_values=-1)[
        :, : segment_ids.shape[1]
    ]
    return (segment_ids == shifted).astype(jnp.float32)


def pad_axis(values, axis, size):
    widths = [(0, 0)] * values.ndim
    widths[axis] = (0, size - values.shape[axis])
    return jnp.pad(values, widths)


def per_device(
    residual,
    cotangent,
    segment_ids,
    adapter_ids,
    conv_gain,
    proj_in,
    conv_taps,
    proj_out,
    ffn_gain,
    gate_up,
    proj_down,
    in_shrink,
    input_lift_weight,
    output_reduce_weight,
    output_lift_weight,
    ffn_reduce_weight,
    ffn_expand,
    down_shrink,
    down_lift_weight,
):
    own, width = residual.shape
    length = segment_ids.shape[1]
    team = length // own
    count = lax.axis_size("dp")
    dims = split_ring(count)
    rows, _, channels = proj_in.shape
    hidden = proj_down.shape[1]
    hc = HIDDEN_CHUNK
    chunks = -(-hidden // hc)
    padded = chunks * hc
    adapter = adapter_ids[0]

    in_shard = proj_in.reshape(rows, 3 * channels)
    gu_shard = pad_axis(jnp.transpose(gate_up, (1, 0, 2)), 2, padded)
    down_shard = pad_axis(proj_down, 1, padded)
    codes = ADAPTER_COUNT * ADAPTER_RANK
    in_reduce = in_shrink.reshape(width, codes)
    in_lift = input_lift_weight.reshape(codes, 3 * channels)
    out_reduce = output_reduce_weight.reshape(channels, codes)
    out_lift = output_lift_weight.reshape(codes, width)
    ffn_reduce = ffn_reduce_weight.reshape(width, 2 * codes)
    expand = pad_axis(ffn_expand.reshape(2, codes, hidden), 2, padded)
    shrink = pad_axis(down_shrink.reshape(hidden, codes), 0, padded)
    down_lift = down_lift_weight.reshape(codes, width)
    lane = jnp.arange(codes, dtype=jnp.int32)[None, :]
    row = jnp.arange(ADAPTER_RANK, dtype=jnp.int32)[:, None]
    mask = (lane // ADAPTER_RANK == adapter).astype(jnp.float32)
    pick = (lane == adapter * ADAPTER_RANK + row).astype(jnp.bfloat16)
    first_same, second_same = lagged_segments(segment_ids, 1)[0], lagged_segments(segment_ids, 2)[0]
    same = jnp.stack([first_same, second_same], axis=1)
    early = Share(count, team, 3 * padded, 3 * width)
    late = Share(count, 1, 4 * channels, 2 * width)
    (
        io_whole,
        _,
        streams,
        norm_one,
        conv_out,
        code_in,
        code_out,
        block_output,
        grad_x_two,
        ffn_flat,
    ) = forward_and_ffn(
        dims,
        team,
        early,
        (
            in_shard,
            proj_out,
            gu_shard,
            down_shard,
            residual,
            cotangent,
            expand,
            shrink,
            same,
            conv_gain.reshape(1, width),
            ffn_gain.reshape(1, width),
            conv_taps,
            in_reduce,
            in_lift,
            out_reduce,
            out_lift,
            ffn_reduce,
            down_lift,
            mask,
            pick,
        ),
    )
    grad_residual, early_sums, late_sums, early_shared = backward(
        dims,
        team,
        early,
        late,
        (
            grad_x_two,
            ffn_flat,
            io_whole,
            streams,
            norm_one,
            conv_out,
            residual,
            code_in,
            code_out,
            same,
            conv_gain.reshape(1, width),
            conv_taps,
            in_reduce,
            in_lift,
            out_reduce,
            out_lift,
            mask,
            pick,
        ),
    )

    def columns_of(sums, share):
        sums = sums.reshape(count, ADAPTER_COUNT, ADAPTER_RANK, share.block)
        return jnp.transpose(sums, (1, 2, 0, 3)).reshape(
            ADAPTER_COUNT, ADAPTER_RANK, count * share.block
        )

    def shared_columns(sums, share):
        sums = sums.reshape(team, share.blocks, ADAPTER_COUNT, ADAPTER_RANK, share.block)
        sums = jnp.transpose(sums, (2, 3, 0, 1, 4)).reshape(
            ADAPTER_COUNT, ADAPTER_RANK, team, share.blocks * share.block
        )
        skip = share.split - share.first * share.block
        return sums[..., skip : skip + share.share]

    def joined(values):
        return values.reshape(ADAPTER_COUNT, ADAPTER_RANK, team * values.shape[-1])

    def rows_first(values):
        return jnp.transpose(values, (2, 0, 1)).astype(jnp.float32)

    early_columns, late_columns = columns_of(early_sums, early), columns_of(late_sums, late)
    early_rest = joined(shared_columns(early_shared, early))
    ffn_e = jnp.stack([early_columns[..., :hidden], early_columns[..., padded : padded + hidden]])
    ffn_e = ffn_e.astype(jnp.float32)
    down_s = rows_first(early_columns[..., 2 * padded : 2 * padded + hidden])
    ffn_s = jnp.stack(
        [rows_first(early_rest[..., :width]), rows_first(early_rest[..., width : 2 * width])],
        axis=1,
    )
    down_e = early_rest[..., 2 * width :].astype(jnp.float32)
    in_e = late_columns[..., : 3 * channels].astype(jnp.float32)
    in_e = in_e.reshape(ADAPTER_COUNT, ADAPTER_RANK, 3, channels)
    out_s = rows_first(late_columns[..., 3 * channels : 4 * channels])
    in_s = rows_first(late_columns[..., 4 * channels : 4 * channels + width])
    out_e = late_columns[..., 4 * channels + width : 4 * channels + 2 * width].astype(jnp.float32)
    return (block_output, grad_residual, in_s, in_e, out_s, out_e, ffn_s, ffn_e, down_s, down_e)


def solution(mesh):
    rows = P(("dp", "tensor"), None)
    placed = (
        rows,
        rows,
        P("dp", None),
        P("dp"),
        P(),
        P("dp", None, "tensor"),
        P(None, "tensor"),
        P("dp", "tensor"),
        P(),
        P("dp", None, "tensor"),
        P("dp", "tensor"),
        P(),
        P(None, None, None, "tensor"),
        P("tensor", None, None),
        P(),
        P(),
        P(None, None, None, "tensor"),
        P("tensor", None, None),
        P(),
    )
    return jax.shard_map(
        per_device,
        mesh=mesh,
        in_specs=placed,
        out_specs=(
            rows,
            rows,
            P(),
            P(None, None, None, "tensor"),
            P("tensor", None, None),
            P(),
            P(),
            P(None, None, None, "tensor"),
            P("tensor", None, None),
            P(),
        ),
        check_vma=False,
    )
```

```python
import functools

import jax
import jax.numpy as jnp
from jax import lax
from jax.experimental import pallas as pl
from jax.experimental.pallas import tpu as pltpu
from jax.sharding import PartitionSpec as P

ADAPTER_COUNT = 8
ADAPTER_RANK = 16
EPSILON = 1e-05
MESH = pl.DeviceIdType.MESH
LANES = 128
HIDDEN_CHUNK = 384
ROW_TILE = 256


def dot(left, right):
    return jnp.dot(left, right, preferred_element_type=jnp.float32)


def dot_against(left, right):
    return lax.dot_general(
        left, right, (((1,), (1,)), ((), ())), preferred_element_type=jnp.float32
    )


def split_pair(values):
    upper = values.astype(jnp.bfloat16)
    lower = (values - upper.astype(jnp.float32)).astype(jnp.bfloat16)
    return (upper, lower)


def norm_factor(values):
    return lax.rsqrt(jnp.mean(values * values, axis=-1, keepdims=True) + EPSILON)


def normalize_back(values, factor, gain, grad):
    unit = values * factor
    scaled = grad * gain
    return factor * (scaled - unit * jnp.mean(scaled * unit, axis=-1, keepdims=True))


def split_ring(count):
    if count % 16 == 0:
        return (4, count // 8, 2)
    return (count, 1, 1)


def position(index, dims):
    return (index // (dims[1] * dims[2]), (index // dims[2]) % dims[1], index % dims[2])


def flat(spot, dims):
    return (spot[0] * dims[1] + spot[1]) * dims[2] + spot[2]


class Gather:
    def __init__(self, dims, spot, send, recv):
        self.dims, self.spot, self.send, self.recv = dims, spot, send, recv

    def place(self, piece, step, along=None):
        whole, columns, order = piece[:3]
        spot = list(self.spot)
        if along is not None:
            spot[order[step]] = along
        place = tuple(
            slice(None) if other in order[:step] else spot[other] for other in range(3)
        )
        return whole.at[place + (slice(None), columns)]

    def lined(self, piece, step):
        return piece[4] and piece[2][step] == 0 and self.dims[0] == 4

    def copies(self, piece, step, offsets=None):
        _, _, order, row, _ = piece
        axis = order[step]
        target = self.place(piece, step)
        base = sum(self.dims[other] - 1 for other in order[:step])
        out = []
        for offset in offsets or range(1, self.dims[axis]):
            peer = list(self.spot)
            peer[axis] = lax.rem(self.spot[axis] + offset, self.dims[axis])
            out.append(
                pltpu.make_async_remote_copy(
                    src_ref=target,
                    dst_ref=target,
                    send_sem=self.send.at[row, base + offset - 1],
                    recv_sem=self.recv.at[row, base + offset - 1],
                    device_id={"dp": flat(peer, self.dims)},
                    device_id_type=MESH,
                )
            )
        return out

    def passed(self, piece, step, here):
        _, _, order, row, _ = piece
        block = self.place(piece, step, 3 if here == 1 else 0)
        base = sum(self.dims[other] - 1 for other in order[:step])
        lanes = sum(d - 1 for d in self.dims)
        peer = list(self.spot)
        peer[0] = 0 if here == 1 else 3
        return pltpu.make_async_remote_copy(
            src_ref=block,
            dst_ref=block,
            send_sem=self.send.at[row, lanes],
            recv_sem=self.recv.at[row, base + (0 if here == 1 else 2)],
            device_id={"dp": flat(peer, self.dims)},
            device_id_type=MESH,
        )

    def own(self, piece, step, act):
        copies = self.copies(piece, step)
        if not self.lined(piece, step):
            for copy in copies:
                act(copy)
            return
        act(copies[1])
        pl.when(self.spot[0] != 3)(lambda: act(copies[0]))
        pl.when(self.spot[0] != 0)(lambda: act(copies[2]))

    def start(self, pieces, step):
        for piece in pieces:
            self.own(piece, step, lambda copy: copy.start())

    def relay(self, pieces, step):
        for piece in pieces:
            if self.lined(piece, step):
                self.copies(piece, step, (2,))[0].wait_recv()
                for here in (1, 2):
                    copy = self.passed(piece, step, here)
                    pl.when(self.spot[0] == here)(copy.start)

    def arrive(self, pieces, step):
        for piece in pieces:
            for copy in self.copies(piece, step, (1, 3) if self.lined(piece, step) else None):
                copy.wait_recv()

    def drain(self, pieces):
        for piece in pieces:
            for step in range(3):
                self.own(piece, step, lambda copy: copy.wait_send())
                if self.lined(piece, step):
                    for here in (1, 2):
                        copy = self.passed(piece, step, here)
                        pl.when(self.spot[0] == here)(copy.wait_send)


def greet(dims, spot, team, member):
    barrier = pltpu.get_barrier_semaphore()
    count = 0
    for axis in range(3):
        for offset in range(1, dims[axis]):
            peer = list(spot)
            peer[axis] = lax.rem(spot[axis] + offset, dims[axis])
            pl.semaphore_signal(
                barrier, inc=1, device_id={"dp": flat(peer, dims)}, device_id_type=MESH
            )
            count += 1
    for offset in range(1, team):
        pl.semaphore_signal(
            barrier,
            inc=1,
            device_id={"tensor": lax.rem(member + offset, team)},
            device_id_type=MESH,
        )
        count += 1
    pl.semaphore_wait(barrier, count)


class Plan:
    def __init__(self, chunks):
        self.crossed = [4, chunks - 2] if chunks >= 8 else [max(chunks - 2, 0)]
        self.plain = [k for k in range(chunks) if k not in self.crossed]
        self.top = [[] for _ in range(chunks)]
        self.bottom = [[] for _ in range(chunks)]
        for m, k in enumerate(self.plain):
            self.add(self.top, k, "second", m + 3)
            self.add(self.top, k, "relay", m + 4)
            self.add(self.top, k, "first", m + 6)
            self.add(self.bottom, k, "third", m + 2)
        for m, k in enumerate(self.crossed):
            self.top[1 + m].append(("cross_third", k))
            self.top[k - 1 - m].append(("cross_relay", k))

    def add(self, where, at, step, m):
        if m < len(self.plain):
            where[at].append((step, self.plain[m]))


def forward_kernel(
    shape,
    in_shard_ref,
    out_shard_ref,
    gu_shard_ref,
    down_shard_ref,
    x_own_ref,
    g_own_ref,
    expand_ref,
    down_shrink_ref,
    same_ref,
    conv_gain_ref,
    ffn_gain_ref,
    taps_ref,
    in_reduce_ref,
    in_lift_ref,
    out_reduce_ref,
    out_lift_ref,
    ffn_reduce_ref,
    down_lift_ref,
    mask_ref,
    pick_ref,
    io_whole_ref,
    ff_left_ref,
    ff_right_ref,
    streams_ref,
    norm_one_ref,
    conv_out_ref,
    code_in_ref,
    code_out_ref,
    block_out_ref,
    grad_x_two_ref,
    ffn_flat_ref,
    x_all_ref,
    g_all_ref,
    na_ref,
    nb_ref,
    w_ref,
    acc_a_ref,
    acc_b_ref,
    x_two_ref,
    halo_ref,
    co_ref,
    cp_ref,
    gcf_ref,
    cf_ref,
    gd_ref,
    cft_ref,
    gdt_ref,
    act_ref,
    ggu_ref,
    eb_ref,
    dsb_ref,
    rb_ref,
    rc_ref,
    rd_ref,
    code_t_ref,
    flat_ref,
    rep_ref,
    got_ref,
    send_ref,
    recv_ref,
    team_send_ref,
    team_recv_ref,
    local_ref,
    load_sem_ref,
):
    dims, team, width, channels, length, chunks, early = shape
    own = length // team
    hc = HIDDEN_CHUNK
    tile = ROW_TILE
    tiles = length // tile
    own_tile = min(own, tile)
    per_own = own // tile
    member = lax.axis_index("tensor")
    spot = position(lax.axis_index("dp"), dims)
    gather = Gather(dims, spot, send_ref, recv_ref)
    own_rows = pl.ds(pl.multiple_of(member * own, own), own)
    plan = Plan(chunks)

    io_step = 4 * channels // 6
    half = io_step // 2
    every = pl.ds(0, half)
    io_pieces = []
    for i in range(6):
        orders = ((0, 1, 2), (0, 2, 1)) if i < 5 else ((1, 2, 0), (2, 1, 0))
        io_pieces.append(
            [
                (io_whole_ref.at[2 * i], every, orders[0], 2 * i, i > 1),
                (io_whole_ref.at[2 * i + 1], every, orders[1], 2 * i + 1, i > 1),
            ]
        )
    io_crossed = io_pieces[5]
    cut = ff_left_ref.shape[-1]

    def chunk_pieces(k):
        orders = ((1, 2, 0), (2, 1, 0)) if k in plan.crossed else ((0, 1, 2), (0, 2, 1))
        return [
            (ff_left_ref.at[k], pl.ds(0, cut), orders[0], 12 + 2 * k, True),
            (ff_right_ref.at[k], pl.ds(0, 3 * hc - cut), orders[1], 13 + 2 * k, True),
        ]

    def do(step, k):
        pieces = chunk_pieces(k)
        if step == "first" or step == "cross_first":
            gather.start(pieces, 0)
        elif step == "relay":
            gather.relay(pieces, 0)
        elif step == "second" or step == "cross_second":
            gather.arrive(pieces, 0)
            gather.start(pieces, 1)
        elif step == "third" or step == "cross_third":
            gather.arrive(pieces, 1)
            gather.start(pieces, 2)
        elif step == "cross_relay":
            gather.relay(pieces, 2)
        elif step == "last":
            gather.arrive(pieces, 2)

    def do_plain(step, m):
        if m < len(plan.plain):
            do(step, plan.plain[m])

    def team_copies(row, source, target):
        out = []
        for offset in range(1, team):
            peer = lax.rem(member + offset, team)
            out.append(
                pltpu.make_async_remote_copy(
                    src_ref=source(peer, offset),
                    dst_ref=target(peer, offset),
                    send_sem=team_send_ref.at[row, offset - 1],
                    recv_sem=team_recv_ref.at[row, offset - 1],
                    device_id={"tensor": peer},
                    device_id_type=MESH,
                )
            )
        return out

    def rows_of(ref):
        return lambda peer, offset: ref.at[pl.ds(pl.multiple_of(peer * own, own), own)]

    def slot_of(ref):
        return lambda peer, offset: ref.at[offset - 1]

    def spare(k):
        at = position(1 + k // 2, dims)
        return lambda first, amount: w_ref.at[at + (slice(None), pl.ds((k % 2) * 3 * hc + first, amount))]

    ins = [
        [
            pltpu.make_async_copy(
                in_shard_ref, w_ref.at[0, 0, 0, :, pl.ds(0, 3 * channels)], local_ref.at[2]
            ),
            pltpu.make_async_copy(
                out_shard_ref, w_ref.at[0, 0, 0, :, pl.ds(3 * channels, channels)], local_ref.at[3]
            ),
        ]
    ]
    outs = [
        [
            pltpu.make_async_copy(
                w_ref.at[0, 0, 0, :, pl.ds(i * half, half)],
                io_whole_ref.at[(i,) + spot],
                local_ref.at[4 + 3 * chunks + i],
            )
            for i in range(12)
        ]
    ]
    for k in range(chunks):
        part = pl.ds(k * hc, hc)
        sources = (gu_shard_ref.at[0, :, part], gu_shard_ref.at[1, :, part], down_shard_ref.at[:, part])
        ins.append(
            [
                pltpu.make_async_copy(source, spare(k)(n * hc, hc), local_ref.at[4 + 3 * k + n])
                for n, source in enumerate(sources)
            ]
        )
        outs.append(
            [
                pltpu.make_async_copy(
                    spare(k)(0, cut), ff_left_ref.at[(k,) + spot], local_ref.at[4 + 3 * k]
                ),
                pltpu.make_async_copy(
                    spare(k)(cut, 3 * hc - cut),
                    ff_right_ref.at[(k,) + spot],
                    local_ref.at[5 + 3 * k],
                ),
            ]
        )
    for copies in ins:
        for copy in copies:
            copy.start()
    greet(dims, spot, team, member)
    x_copies = team_copies(0, lambda p, o: x_own_ref, lambda p, o: x_all_ref.at[own_rows])
    g_copies = team_copies(1, lambda p, o: g_own_ref, lambda p, o: g_all_ref.at[own_rows])
    for copy in x_copies + g_copies:
        copy.start()
    x_here = pltpu.make_async_copy(x_own_ref, x_all_ref.at[own_rows], local_ref.at[0])
    g_here = pltpu.make_async_copy(g_own_ref, g_all_ref.at[own_rows], local_ref.at[1])
    for first, second in zip(ins, outs):
        for copy in first:
            copy.wait()
        for copy in second:
            copy.start()
    x_here.start()
    g_here.start()
    for i, pieces in enumerate(io_pieces):
        outs[0][2 * i].wait()
        outs[0][2 * i + 1].wait()
        gather.start(pieces, 0)
    for copies in outs[1:]:
        for copy in copies:
            copy.wait()
    for k in plan.crossed:
        do("cross_first", k)

    x_here.wait()
    for copy in x_copies:
        copy.wait_recv()

    def first_norm(i, carry):
        rows = pl.ds(pl.multiple_of(i * tile, tile), tile)
        values = x_all_ref[rows, :].astype(jnp.float32)
        na_ref[rows, :] = (values * norm_factor(values) * conv_gain_ref[...]).astype(jnp.bfloat16)
        return carry

    def down_codes(i, carry):
        rows = pl.ds(pl.multiple_of(i * tile, tile), tile)
        code = dot_against(g_all_ref[rows, :], down_lift_ref[...]) * mask_ref[...]
        code = code.astype(jnp.bfloat16)
        gd_ref[rows, :] = code
        gdt_ref[:, rows] = dot_against(pick_ref[...], code).astype(jnp.bfloat16)
        return carry

    norm_store = pltpu.make_async_copy(na_ref, norm_one_ref, local_ref.at[0])
    for i in range(6):
        if i == 0:
            lax.fori_loop(0, tiles, first_norm, 0)
            norm_store.start()
            gather.arrive(io_crossed, 0)
            gather.start(io_crossed, 1)
            for k in plan.crossed:
                do("cross_second", k)
        if i == 1:
            g_here.wait()
            for copy in g_copies:
                copy.wait_recv()
            lax.fori_loop(0, tiles, down_codes, 0)
            gather.arrive(io_crossed, 1)
            gather.start(io_crossed, 2)
            do_plain("first", 0)
            do_plain("first", 1)
        if i == 5:
            gather.relay(io_crossed, 2)
        if i < 5:
            gather.arrive(io_pieces[i], 0)
            gather.start(io_pieces[i], 1)
        if i > 0:
            gather.arrive(io_pieces[i - 1], 1)
            gather.start(io_pieces[i - 1], 2)
        if 1 <= i < 4:
            gather.relay(io_pieces[i + 1], 0)
    do_plain("relay", 0)
    do_plain("relay", 1)
    do_plain("first", 2)
    do_plain("second", 0)
    io_loads = []
    for i in range(6):
        gather.arrive(io_pieces[i], 2)
        for part in (2 * i, 2 * i + 1):
            load = pltpu.make_async_copy(
                io_whole_ref.at[part],
                w_ref.at[:, :, :, :, pl.ds(part * half, half)],
                load_sem_ref.at[part],
            )
            load.start()
            io_loads.append(load)
    do_plain("second", 1)
    do_plain("first", 3)
    norm_store.wait()
    for load in io_loads:
        load.wait()

    def weights(first, count):
        return w_ref[:, :, :, :, pl.ds(first, count)].reshape(width, count)

    halo_ref[pl.ds(0, 8), :] = jnp.zeros((8, channels), jnp.float32)

    def convolve(i, carry):
        rows = pl.ds(pl.multiple_of(i * tile, tile), tile)
        normed = na_ref[rows, :]
        code = (dot(normed, in_reduce_ref[...]) * mask_ref[...]).astype(jnp.bfloat16)
        code_in_ref[:, rows] = dot_against(pick_ref[...], code).astype(jnp.bfloat16)
        lanes = []
        for lane in range(3):
            value = dot(normed, weights(lane * channels, channels)) + dot(
                code, in_lift_ref[:, pl.ds(lane * channels, channels)]
            )
            lanes.append(value)
            if lane < 2:
                acc_a_ref[rows, pl.ds(lane * channels, channels)] = value
            else:
                acc_b_ref[rows, pl.ds(0, channels)] = value
        product = lanes[0] * lanes[2]
        halo_ref[pl.ds(8, tile), :] = product
        masks = same_ref[rows, :]
        taps = taps_ref[...].astype(jnp.float32)
        mixed = (
            taps[0:1, :] * product
            + taps[1:2, :] * halo_ref[pl.ds(7, tile), :] * masks[:, 0:1]
            + taps[2:3, :] * halo_ref[pl.ds(6, tile), :] * masks[:, 1:2]
        )
        halo_ref[pl.ds(0, 8), :] = halo_ref[pl.ds(tile, 8), :]
        convolved = (lanes[1] * mixed).astype(jnp.bfloat16)
        co_ref[rows, :] = convolved
        na_ref[rows, :] = dot_against(convolved, weights(3 * channels, channels)).astype(jnp.bfloat16)
        cp_ref[rows, :] = dot(convolved, out_reduce_ref[...])

        @pl.when(i == 1)
        def _():
            do_plain("relay", 2)
            do_plain("third", 0)

        @pl.when(i == 2)
        def _():
            do_plain("first", 4)
            do_plain("second", 2)

        return carry

    lax.fori_loop(0, tiles, convolve, 0)
    stores = [
        pltpu.make_async_copy(acc_a_ref.at[:, pl.ds(0, channels)], streams_ref.at[0], local_ref.at[3]),
        pltpu.make_async_copy(
            acc_a_ref.at[:, pl.ds(channels, channels)], streams_ref.at[1], local_ref.at[4]
        ),
        pltpu.make_async_copy(acc_b_ref.at[:, pl.ds(0, channels)], streams_ref.at[2], local_ref.at[5]),
        pltpu.make_async_copy(co_ref, conv_out_ref, local_ref.at[6]),
    ]
    branch = team_copies(2, rows_of(na_ref), slot_of(rb_ref))
    codes = team_copies(3, rows_of(cp_ref), slot_of(rc_ref))
    for copy in codes + branch + stores:
        copy.start()
    do_plain("relay", 3)
    do_plain("first", 5)
    do_plain("third", 1)

    def load(c):
        slot = lax.rem(c, 2)
        left = pl.ds(pl.multiple_of(slot * 3 * hc, LANES), cut)
        right = pl.ds(pl.multiple_of(slot * 3 * hc + cut, LANES), 3 * hc - cut)
        part = pl.ds(pl.multiple_of(c * hc, LANES), hc)
        pairs = [
            (ff_left_ref.at[c], w_ref.at[:, :, :, :, left]),
            (ff_right_ref.at[c], w_ref.at[:, :, :, :, right]),
            (expand_ref.at[:, :, part], eb_ref.at[slot]),
            (down_shrink_ref.at[part], dsb_ref.at[slot]),
        ]
        return [
            pltpu.make_async_copy(source, target, load_sem_ref.at[4 * slot + n])
            for n, (source, target) in enumerate(pairs)
        ]

    for copy in branch + codes:
        copy.wait_recv()
    code = cp_ref[own_rows, :]
    for peer in range(team - 1):
        code = code + rc_ref[peer]
    code = (code * mask_ref[...]).astype(jnp.bfloat16)
    code_out_ref[...] = dot_against(pick_ref[...], code).astype(jnp.bfloat16)
    cf_ref[pl.ds(0, own), pl.ds(0, LANES)] = code

    def second_norm(i, carry):
        local_rows = pl.ds(pl.multiple_of(i * own_tile, own_tile), own_tile)
        rows = pl.ds(pl.multiple_of(member * own + i * own_tile, own_tile), own_tile)
        values = x_all_ref[rows, :].astype(jnp.float32) + na_ref[rows, :].astype(jnp.float32)
        for peer in range(team - 1):
            values = values + rb_ref[peer, local_rows, :].astype(jnp.float32)
        values = values + dot(cf_ref[local_rows, pl.ds(0, LANES)], out_lift_ref[...])
        x_two_ref[local_rows, :] = values
        nb_ref[rows, :] = (values * norm_factor(values) * ffn_gain_ref[...]).astype(jnp.bfloat16)
        return carry

    lax.fori_loop(0, own // own_tile, second_norm, 0)
    norms = team_copies(4, lambda p, o: nb_ref.at[own_rows], lambda p, o: nb_ref.at[own_rows])
    for copy in norms:
        copy.start()
    do("last", 0)
    for copy in load(0):
        copy.start()
    for copy in stores:
        copy.wait()
    acc_a_ref[...] = jnp.zeros_like(acc_a_ref)
    acc_b_ref[...] = jnp.zeros_like(acc_b_ref)
    for copy in branch + codes:
        copy.wait_send()
    cp_ref[...] = jnp.zeros_like(cp_ref)
    gcf_ref[...] = jnp.zeros_like(gcf_ref)
    for copy in norms:
        copy.wait_recv()

    def ffn_codes(i, carry):
        rows = pl.ds(pl.multiple_of(i * tile, tile), tile)
        value = dot(nb_ref[rows, :], ffn_reduce_ref[...])
        for n in range(2):
            code = (value[:, n * LANES : (n + 1) * LANES] * mask_ref[...]).astype(jnp.bfloat16)
            cf_ref[rows, pl.ds(n * LANES, LANES)] = code
            cft_ref[pl.ds(16 * n, 16), rows] = dot_against(pick_ref[...], code).astype(jnp.bfloat16)
        return carry

    lax.fori_loop(0, tiles, ffn_codes, 0)

    codes = team_copies(7, rows_of(cp_ref), slot_of(rc_ref))
    grads = team_copies(5, rows_of(x_all_ref), slot_of(rd_ref))
    downs = team_copies(6, rows_of(na_ref), slot_of(rb_ref))

    def finish(rows):
        na_ref[rows, :] = acc_a_ref[rows, :].astype(jnp.bfloat16)
        total = acc_b_ref[rows, :]
        for n in range(2):
            lanes = pl.ds(n * LANES, LANES)
            upper, lower = split_pair(gcf_ref[rows, lanes] * mask_ref[...])
            code_t_ref[0, pl.ds(16 * n, 16), rows] = dot_against(pick_ref[...], upper).astype(
                jnp.bfloat16
            )
            code_t_ref[1, pl.ds(16 * n, 16), rows] = dot_against(pick_ref[...], lower).astype(
                jnp.bfloat16
            )
            total = (
                total
                + dot_against(upper, ffn_reduce_ref[:, lanes])
                + dot_against(lower, ffn_reduce_ref[:, lanes])
            )
        acc_b_ref[rows, :] = total
        x_all_ref[rows, :] = total.astype(jnp.bfloat16)

    def chunk(c, carry):
        for k in range(chunks):
            if plan.top[k]:

                @pl.when(c == k)
                def _():
                    for step, which in plan.top[k]:
                        do(step, which)

        for copy in load(c):
            copy.wait()
        slot = lax.rem(c, 2)
        first = pl.multiple_of(slot * 3 * hc, LANES)
        down_first = pl.multiple_of(slot * 3 * hc + 2 * hc, LANES)

        def row_tile(j, inner):
            i = lax.rem((member + 1) * per_own + j, tiles)
            rows = pl.ds(pl.multiple_of(i * tile, tile), tile)
            both = dot(nb_ref[rows, :], weights(first, 2 * hc))
            grad = dot(g_all_ref[rows, :], weights(down_first, hc)) + dot_against(
                gd_ref[rows, :], dsb_ref[slot]
            )
            gate = both[:, :hc] + dot(cf_ref[rows, pl.ds(0, LANES)], eb_ref[slot, 0])
            up = both[:, hc:] + dot(cf_ref[rows, pl.ds(LANES, LANES)], eb_ref[slot, 1])
            gated = jax.nn.sigmoid(gate)
            silu = gate * gated
            act = (silu * up).astype(jnp.bfloat16)
            act_ref[rows, :] = act
            grad_gate = (grad * up * gated * (1.0 + gate * (1.0 - gated))).astype(jnp.bfloat16)
            grad_up = (grad * silu).astype(jnp.bfloat16)
            ggu_ref[rows, pl.ds(0, hc)] = grad_gate
            ggu_ref[rows, pl.ds(hc, hc)] = grad_up
            acc_a_ref[rows, :] += dot_against(act, weights(down_first, hc))
            cp_ref[rows, :] += dot(act, dsb_ref[slot])
            acc_b_ref[rows, :] += dot_against(ggu_ref[rows, :], weights(first, 2 * hc))
            gcf_ref[rows, pl.ds(0, LANES)] += dot_against(grad_gate, eb_ref[slot, 0])
            gcf_ref[rows, pl.ds(LANES, LANES)] += dot_against(grad_up, eb_ref[slot, 1])

            @pl.when(c == chunks - 1)
            def _():
                finish(rows)
                for offset in range(1, team):

                    @pl.when(j == offset * per_own - 1)
                    def _():
                        for copies in (codes, grads, downs):
                            copies[offset - 1].start()

            return inner

        lax.fori_loop(0, tiles, row_tile, 0)
        for k in range(chunks - 1):

            @pl.when(c == k)
            def _():
                for step, which in plan.bottom[k]:
                    do(step, which)
                do("last", k + 1)

        @pl.when(c + 1 < chunks)
        def _():
            for copy in load(c + 1):
                copy.start()

        at = pl.multiple_of(c * hc, LANES)
        padded = chunks * hc
        for n in range(2):
            value = dot(cft_ref[pl.ds(16 * n, 16), :], ggu_ref[:, pl.ds(n * hc, hc)])
            flat_ref[:, pl.ds(n * padded + at, hc)] = value.astype(jnp.bfloat16)
        value = dot(gdt_ref[...], act_ref[...])
        flat_ref[:, pl.ds(2 * padded + at, hc)] = value.astype(jnp.bfloat16)
        return carry

    lax.fori_loop(0, chunks, chunk, 0)

    for copy in codes:
        copy.wait_recv()
    code = cp_ref[own_rows, :]
    for peer in range(team - 1):
        code = code + rc_ref[peer]
    rounded = (code * mask_ref[...]).astype(jnp.bfloat16)
    cf_ref[pl.ds(0, own), pl.ds(0, LANES)] = rounded
    turned = dot_against(pick_ref[...], rounded).astype(jnp.bfloat16)
    shrunk = (dot(code_t_ref[0], nb_ref[...]) + dot(code_t_ref[1], nb_ref[...])).astype(jnp.bfloat16)
    rep_ref[:, pl.ds(0, width)] = shrunk[:16]
    rep_ref[:, pl.ds(width, width)] = shrunk[16:]
    rep_ref[:, pl.ds(2 * width, width)] = dot(turned, g_all_ref[own_rows, :]).astype(jnp.bfloat16)
    share = early.share
    reps = team_copies(
        8,
        lambda p, o: rep_ref.at[:, pl.ds(pl.multiple_of(p * share, LANES), share)],
        slot_of(got_ref),
    )
    for copy in reps:
        copy.start()
    for copy in grads + downs:
        copy.wait_recv()
    for copy in norms + grads + downs:
        copy.wait_send()

    def last_rows(i, carry):
        local_rows = pl.ds(pl.multiple_of(i * own_tile, own_tile), own_tile)
        rows = pl.ds(pl.multiple_of(member * own + i * own_tile, own_tile), own_tile)
        values = x_two_ref[local_rows, :]
        down = acc_a_ref[rows, :]
        grad = acc_b_ref[rows, :]
        for peer in range(team - 1):
            down = down + rb_ref[peer, local_rows, :].astype(jnp.float32)
            grad = grad + rd_ref[peer, local_rows, :].astype(jnp.float32)
        out = values + down + dot(cf_ref[local_rows, pl.ds(0, LANES)], down_lift_ref[...])
        nb_ref[local_rows, :] = out.astype(jnp.bfloat16)
        x_two_ref[local_rows, :] = g_all_ref[rows, :].astype(jnp.float32) + normalize_back(
            values, norm_factor(values), ffn_gain_ref[...], grad
        )
        return carry

    lax.fori_loop(0, own // own_tile, last_rows, 0)
    results = [
        pltpu.make_async_copy(nb_ref.at[pl.ds(0, own)], block_out_ref, local_ref.at[0]),
        pltpu.make_async_copy(x_two_ref, grad_x_two_ref, local_ref.at[1]),
    ]
    for copy in results:
        copy.start()
    for copy in reps:
        copy.wait_recv()
    value = rep_ref[:, pl.ds(pl.multiple_of(member * share, LANES), share)].astype(jnp.float32)
    for peer in range(team - 1):
        value = value + got_ref[peer].astype(jnp.float32)
    flat_ref[:, pl.ds(early.split, share)] = value.astype(jnp.bfloat16)
    rest = flat_ref.shape[1] - early.total
    if rest:
        flat_ref[:, pl.ds(early.total, rest)] = jnp.zeros((16, rest), jnp.bfloat16)
    flat_store = pltpu.make_async_copy(flat_ref, ffn_flat_ref, local_ref.at[2])
    flat_store.start()
    for copy in x_copies + g_copies + codes + reps:
        copy.wait_send()
    for pieces in io_pieces:
        gather.drain(pieces)
    for k in range(chunks):
        gather.drain(chunk_pieces(k))
    for copy in results:
        copy.wait()
    flat_store.wait()


def forward_and_ffn(dims, team, early, operands):
    in_shard, out_shard, gu_shard, down_shard, x_own = operands[:5]
    rows, channels = out_shard.shape
    hc = HIDDEN_CHUNK
    chunks = down_shard.shape[1] // hc
    own, width = x_own.shape
    length = own * team
    count = dims[0] * dims[1] * dims[2]
    columns = max(4 * channels, 6 * hc)
    lanes = sum(d - 1 for d in dims) + 1
    shape = (dims, team, width, channels, length, chunks, early)
    bf16, f32 = jnp.bfloat16, jnp.float32
    anywhere = pl.BlockSpec(memory_space=pl.ANY)
    vmem = pl.BlockSpec(memory_space=pltpu.VMEM)
    outs = [
        ((12,) + dims + (rows, 4 * channels // 12), bf16, anywhere),
        ((chunks,) + dims + (rows, 640), bf16, anywhere),
        ((chunks,) + dims + (rows, 3 * hc - 640), bf16, anywhere),
        ((3, length, channels), f32, anywhere),
        ((length, width), bf16, anywhere),
        ((length, channels), bf16, anywhere),
        ((16, length), bf16, vmem),
        ((16, own), bf16, vmem),
        ((own, width), bf16, anywhere),
        ((own, width), f32, anywhere),
        ((16, count * early.block), bf16, anywhere),
    ]
    peers = max(team - 1, 1)
    row_count = 12 + 2 * chunks
    scratch = [
        pltpu.VMEM((length, width), bf16),
        pltpu.VMEM((length, width), bf16),
        pltpu.VMEM((length, width), bf16),
        pltpu.VMEM((length, width), bf16),
        pltpu.VMEM(dims + (rows, columns), bf16),
        pltpu.VMEM((length, width), f32),
        pltpu.VMEM((length, width), f32),
        pltpu.VMEM((own, width), f32),
        pltpu.VMEM((ROW_TILE + 8, channels), f32),
        pltpu.VMEM((length, channels), bf16),
        pltpu.VMEM((length, LANES), f32),
        pltpu.VMEM((length, 2 * LANES), f32),
        pltpu.VMEM((length, 2 * LANES), bf16),
        pltpu.VMEM((length, LANES), bf16),
        pltpu.VMEM((32, length), bf16),
        pltpu.VMEM((16, length), bf16),
        pltpu.VMEM((length, hc), bf16),
        pltpu.VMEM((length, 2 * hc), bf16),
        pltpu.VMEM((2, 2, LANES, hc), bf16),
        pltpu.VMEM((2, hc, LANES), bf16),
        pltpu.VMEM((peers, own, width), bf16),
        pltpu.VMEM((peers, own, LANES), f32),
        pltpu.VMEM((peers, own, width), bf16),
        pltpu.VMEM((2, 32, length), bf16),
        pltpu.VMEM((16, count * early.block), bf16),
        pltpu.VMEM((16, 3 * width), bf16),
        pltpu.VMEM((peers, 16, 3 * width // team), bf16),
        pltpu.SemaphoreType.DMA((row_count, lanes)),
        pltpu.SemaphoreType.DMA((row_count, lanes)),
        pltpu.SemaphoreType.DMA((9, peers)),
        pltpu.SemaphoreType.DMA((9, peers)),
        pltpu.SemaphoreType.DMA((16 + 3 * chunks,)),
        pltpu.SemaphoreType.DMA((12,)),
    ]
    return pl.pallas_call(
        functools.partial(forward_kernel, shape),
        out_shape=[jax.ShapeDtypeStruct(o[0], o[1]) for o in outs],
        in_specs=[anywhere] * 8 + [vmem] * 12,
        out_specs=[o[2] for o in outs],
        scratch_shapes=scratch,
        compiler_params=pltpu.CompilerParams(
            collective_id=0, has_side_effects=True, vmem_limit_bytes=67043328
        ),
    )(*operands)


class Share:
    def __init__(self, count, team, split, shared):
        self.split, self.shared, self.share = split, shared, shared // team
        self.total = split + self.share
        self.block = -(-self.total // (LANES * count)) * LANES
        self.first = split // self.block
        self.blocks = -(-self.total // self.block) - self.first


def backward_kernel(
    shape,
    grad_x_two_ref,
    ffn_flat_ref,
    io_whole_ref,
    streams_ref,
    norm_one_ref,
    conv_out_ref,
    x_own_ref,
    code_in_ref,
    code_out_ref,
    same_ref,
    conv_gain_ref,
    taps_ref,
    in_reduce_ref,
    in_lift_ref,
    out_reduce_ref,
    out_lift_ref,
    mask_ref,
    pick_ref,
    grad_residual_ref,
    early_ref,
    late_ref,
    early_rep_ref,
    w_ref,
    gx_ref,
    gb_ref,
    gco_ref,
    gcot_ref,
    st_ref,
    gs_ref,
    gci_ref,
    ha_ref,
    hb_ref,
    halo_ref,
    na_ref,
    co_ref,
    pb_ref,
    gcit_ref,
    xo_ref,
    rb_ref,
    rep_b_ref,
    got_b_ref,
    flat_a_ref,
    flat_b_ref,
    part_a_ref,
    part_b_ref,
    from_a_ref,
    from_b_ref,
    sum_a_ref,
    sum_b_ref,
    spare_a_ref,
    out_ref,
    send_ref,
    recv_ref,
    swap_send_ref,
    swap_recv_ref,
    team_send_ref,
    team_recv_ref,
    local_ref,
    weight_sem_ref,
):
    dims, team, width, channels, length, early, late = shape
    count = dims[0] * dims[1] * dims[2]
    own = length // team
    tile = ROW_TILE
    tiles = length // tile
    own_tile = min(own, tile)
    member = lax.axis_index("tensor")
    me = lax.axis_index("dp")
    spot = position(me, dims)
    gather = Gather(dims, spot, send_ref, recv_ref)
    own_rows = pl.ds(pl.multiple_of(member * own, own), own)

    def enter():
        barrier = pltpu.get_barrier_semaphore()
        for offset in range(1, count):
            pl.semaphore_signal(
                barrier, inc=1, device_id={"dp": lax.rem(me + offset, count)}, device_id_type=MESH
            )
        for offset in range(1, team):
            pl.semaphore_signal(
                barrier,
                inc=1,
                device_id={"tensor": lax.rem(member + offset, team)},
                device_id_type=MESH,
            )
        pl.semaphore_wait(barrier, count - 1 + team - 1)

    def team_copies(row, source, target):
        out = []
        for offset in range(1, team):
            peer = lax.rem(member + offset, team)
            out.append(
                pltpu.make_async_remote_copy(
                    src_ref=source(peer, offset),
                    dst_ref=target(peer, offset),
                    send_sem=team_send_ref.at[row, offset - 1],
                    recv_sem=team_recv_ref.at[row, offset - 1],
                    device_id={"tensor": peer},
                    device_id_type=MESH,
                )
            )
        return out

    def swap_copies(row, part, landing):
        out = []
        for offset in range(1, count):
            peer = lax.rem(me + offset, count)
            out.append(
                pltpu.make_async_remote_copy(
                    src_ref=part.at[peer],
                    dst_ref=landing.at[me],
                    send_sem=swap_send_ref.at[row, offset - 1],
                    recv_sem=swap_recv_ref.at[row, offset - 1],
                    device_id={"dp": peer},
                    device_id_type=MESH,
                )
            )
        return out

    def pieces_of(share, whole, row):
        out = []
        step = max(share.block // 384, 1) * LANES
        for n, first in enumerate(range(0, share.block, step)):
            order = (0, 1, 2) if n % 2 == 0 else (0, 2, 1)
            out.append((whole, pl.ds(first, min(step, share.block - first)), order, row + n, False))
        return out

    def forward_on(pieces, step):
        for piece in pieces:
            gather.arrive([piece], step)
            gather.start([piece], step + 1)

    def hand_out(share, columns, part, landing, row):
        for peer in range(count):
            part[peer, :, pl.ds(0, share.block)] = columns[:, pl.ds(peer * share.block, share.block)]
            part[peer, :, pl.ds(share.block, LANES)] = pick_ref[...]
        landing[me] = part[me]
        copies = swap_copies(row, part, landing)
        for copy in copies:
            copy.start()
        return copies

    def take_in(share, landing, total):
        marks = landing[:, :, pl.ds(share.block, LANES)].reshape(count * 16, LANES)
        marks = jnp.transpose(marks.astype(jnp.float32)).astype(jnp.bfloat16)
        blocks = landing[:, :, pl.ds(0, share.block)].reshape(count * 16, share.block)
        total[...] = dot(marks, blocks).astype(jnp.bfloat16)

    piece = 4 * channels // 12

    def weight_loads(parts):
        return [
            pltpu.make_async_copy(
                io_whole_ref.at[part],
                w_ref.at[:, :, :, :, pl.ds(part * piece, piece)],
                weight_sem_ref.at[part],
            )
            for part in parts
        ]

    out_loads, in_loads = weight_loads(range(9, 12)), weight_loads(range(9))
    loads = {}
    for slot, (name, source, target) in enumerate(
        [
            ("flat", ffn_flat_ref, flat_a_ref),
            ("gx", grad_x_two_ref, gx_ref),
            ("co", conv_out_ref, co_ref),
            ("b", streams_ref.at[0], st_ref.at[0, pl.ds(8, length)]),
            ("c", streams_ref.at[1], st_ref.at[1, pl.ds(8, length)]),
            ("x", streams_ref.at[2], st_ref.at[2, pl.ds(8, length)]),
            ("na", norm_one_ref, na_ref),
            ("xo", x_own_ref, xo_ref),
        ]
    ):
        loads[name] = pltpu.make_async_copy(source, target, local_ref.at[slot])
        loads[name].start()
        if name == "co":
            for copy in out_loads:
                copy.start()
    for copy in in_loads:
        copy.start()
    enter()
    loads["flat"].wait()
    sent_a = hand_out(early, flat_a_ref, part_a_ref, from_a_ref, 0)
    st_ref[0, pl.ds(0, 8), :] = jnp.zeros((8, channels), jnp.float32)
    st_ref[2, pl.ds(0, 8), :] = jnp.zeros((8, channels), jnp.float32)
    ha_ref[pl.ds(tile, 8), :] = jnp.zeros((8, channels), jnp.float32)
    hb_ref[pl.ds(tile, 8), :] = jnp.zeros((8, channels), jnp.float32)
    loads["gx"].wait()

    def branch_rows(i, carry):
        local_rows = pl.ds(pl.multiple_of(i * own_tile, own_tile), own_tile)
        rows = pl.ds(pl.multiple_of(member * own + i * own_tile, own_tile), own_tile)
        upper, lower = split_pair(gx_ref[local_rows, :])
        gb_ref[rows, :] = upper
        code = dot_against(upper, out_lift_ref[...]) + dot_against(lower, out_lift_ref[...])
        gco_ref[rows, :] = (code * mask_ref[...]).astype(jnp.bfloat16)
        return carry

    lax.fori_loop(0, own // own_tile, branch_rows, 0)
    swaps = team_copies(0, lambda p, o: gb_ref.at[own_rows], lambda p, o: gb_ref.at[own_rows])
    swaps += team_copies(1, lambda p, o: gco_ref.at[own_rows], lambda p, o: gco_ref.at[own_rows])
    for copy in swaps:
        copy.start()
    upper, lower = split_pair(gx_ref[...])
    rep_b_ref[:, pl.ds(width, width)] = (
        dot(code_out_ref[...], upper) + dot(code_out_ref[...], lower)
    ).astype(jnp.bfloat16)
    for copy in swaps:
        copy.wait_recv()

    def turn(i, carry):
        rows = pl.ds(pl.multiple_of(i * tile, tile), tile)
        gcot_ref[:, rows] = dot_against(pick_ref[...], gco_ref[rows, :]).astype(jnp.bfloat16)
        return carry

    lax.fori_loop(0, tiles, turn, 0)
    loads["co"].wait()
    flat_b_ref[:, pl.ds(3 * channels, channels)] = dot(gcot_ref[...], co_ref[...]).astype(jnp.bfloat16)
    pieces_a = pieces_of(early, early_ref, 0)
    pieces_b = pieces_of(late, late_ref, len(pieces_a))
    place_a = pltpu.make_async_copy(sum_a_ref, early_ref.at[spot], local_ref.at[0])
    place_b = pltpu.make_async_copy(sum_b_ref, late_ref.at[spot], local_ref.at[1])

    for copy in out_loads:
        copy.wait()
    for name in ("b", "c", "x"):
        loads[name].wait()

    def weights(first, amount):
        return w_ref[:, :, :, :, pl.ds(first, amount)].reshape(width, amount)

    for copy in sent_a:
        copy.wait_recv()
    take_in(early, from_a_ref, sum_a_ref)
    place_a.start()

    def back(j, carry):
        i = tiles - 1 - j
        start = pl.multiple_of(i * tile, tile)
        rows = pl.ds(start, tile)
        later = pl.ds(pl.multiple_of(start + 8, 8), tile)
        grad = dot(gb_ref[rows, :], weights(3 * channels, channels)) + dot_against(
            gco_ref[rows, :], out_reduce_ref[...]
        )
        halo_ref[pl.ds(0, 8), :] = st_ref[0, pl.ds(start, 8), :] * st_ref[2, pl.ds(start, 8), :]
        product = st_ref[0, later, :] * st_ref[2, later, :]
        halo_ref[pl.ds(8, tile), :] = product
        masks = same_ref[rows, :]
        taps = taps_ref[...].astype(jnp.float32)
        mixed = (
            taps[0:1, :] * product
            + taps[1:2, :] * halo_ref[pl.ds(7, tile), :] * masks[:, 0:1]
            + taps[2:3, :] * halo_ref[pl.ds(6, tile), :] * masks[:, 1:2]
        )
        grad_mixed = grad * st_ref[1, later, :]
        ha_ref[pl.ds(0, tile), :] = taps[1:2, :] * grad_mixed * masks[:, 0:1]
        hb_ref[pl.ds(0, tile), :] = taps[2:3, :] * grad_mixed * masks[:, 1:2]
        grad_product = taps[0:1, :] * grad_mixed + ha_ref[pl.ds(1, tile), :] + hb_ref[pl.ds(2, tile), :]
        ha_ref[pl.ds(tile, 8), :] = ha_ref[pl.ds(0, 8), :]
        hb_ref[pl.ds(tile, 8), :] = hb_ref[pl.ds(0, 8), :]
        gs_ref[rows, pl.ds(0, channels)] = (grad_product * st_ref[2, later, :]).astype(jnp.bfloat16)
        gs_ref[rows, pl.ds(channels, channels)] = (grad * mixed).astype(jnp.bfloat16)
        gs_ref[rows, pl.ds(2 * channels, channels)] = (grad_product * st_ref[0, later, :]).astype(
            jnp.bfloat16
        )
        upper, lower = split_pair(dot_against(gs_ref[rows, :], in_lift_ref[...]) * mask_ref[...])
        gci_ref[0, rows, :] = upper
        gci_ref[1, rows, :] = lower
        gcit_ref[0, :, rows] = dot_against(pick_ref[...], upper).astype(jnp.bfloat16)
        gcit_ref[1, :, rows] = dot_against(pick_ref[...], lower).astype(jnp.bfloat16)

        @pl.when(j == 0)
        def _():
            place_a.wait()
            gather.start(pieces_a, 0)

        for n in (2, 3):

            @pl.when(j == n)
            def _():
                forward_on(pieces_a[n - 2 : n - 1], 0)

        return carry

    lax.fori_loop(0, tiles, back, 0)
    loads["na"].wait()
    rep_b_ref[:, pl.ds(0, width)] = (
        dot(gcit_ref[0], na_ref[...]) + dot(gcit_ref[1], na_ref[...])
    ).astype(jnp.bfloat16)
    more = team_copies(2, lambda p, o: rep_b_ref, lambda p, o: got_b_ref.at[o - 1])
    for copy in more:
        copy.start()
    forward_on(pieces_a[2:3], 0)
    flat_b_ref[:, pl.ds(0, 3 * channels)] = dot(code_in_ref[...], gs_ref[...]).astype(jnp.bfloat16)
    for copy in more:
        copy.wait_recv()
    value = rep_b_ref[...].astype(jnp.float32)
    for peer in range(team - 1):
        value = value + got_b_ref[peer].astype(jnp.float32)
    flat_b_ref[:, pl.ds(late.split, 2 * width)] = value.astype(jnp.bfloat16)
    rest = count * late.block - late.total
    if rest:
        flat_b_ref[:, pl.ds(late.total, rest)] = jnp.zeros((16, rest), jnp.bfloat16)
    sent_b = hand_out(late, flat_b_ref, part_b_ref, from_b_ref, 1)
    forward_on(pieces_a[:1], 1)
    for copy in in_loads:
        copy.wait()
    grads = team_copies(
        6,
        lambda p, o: pb_ref.at[pl.ds(pl.multiple_of(p * own, own), own)],
        lambda p, o: rb_ref.at[o - 1],
    )
    per_own = own // tile

    def norm_grads(j, carry):
        i = lax.rem((member + 1) * per_own + j, tiles)
        rows = pl.ds(pl.multiple_of(i * tile, tile), tile)
        pb_ref[rows, :] = (
            dot_against(gs_ref[rows, :], weights(0, 3 * channels))
            + dot_against(gci_ref[0, rows, :], in_reduce_ref[...])
            + dot_against(gci_ref[1, rows, :], in_reduce_ref[...])
        ).astype(jnp.bfloat16)
        for offset in range(1, team):

            @pl.when(j == offset * per_own - 1)
            def _():
                grads[offset - 1].start()

        @pl.when(j == 0)
        def _():
            forward_on(pieces_a[3:], 0)
            forward_on(pieces_a[1:2], 1)

        @pl.when(j == 1)
        def _():
            for copy in sent_b:
                copy.wait_recv()
            take_in(late, from_b_ref, sum_b_ref)
            place_b.start()

        @pl.when(j == 2)
        def _():
            place_b.wait()
            gather.start(pieces_b, 0)
            forward_on(pieces_a[2:3], 1)

        return carry

    lax.fori_loop(0, tiles, norm_grads, 0)
    loads["xo"].wait()
    forward_on(pieces_a[3:], 1)
    forward_on(pieces_b, 0)
    for copy in grads:
        copy.wait_recv()

    def residual_rows(i, carry):
        local_rows = pl.ds(pl.multiple_of(i * own_tile, own_tile), own_tile)
        rows = pl.ds(pl.multiple_of(member * own + i * own_tile, own_tile), own_tile)
        values = xo_ref[local_rows, :].astype(jnp.float32)
        grad = pb_ref[rows, :].astype(jnp.float32)
        for peer in range(team - 1):
            grad = grad + rb_ref[peer, local_rows, :].astype(jnp.float32)
        out_ref[local_rows, :] = (
            gx_ref[local_rows, :]
            + normalize_back(values, norm_factor(values), conv_gain_ref[...], grad)
        ).astype(jnp.bfloat16)
        return carry

    lax.fori_loop(0, own // own_tile, residual_rows, 0)
    result = pltpu.make_async_copy(out_ref, grad_residual_ref, local_ref.at[2])
    result.start()

    def pass_on(share, whole, reps, spare, base):
        lifts = []
        for block in range(share.blocks):
            here = whole.at[position(share.first + block, dims)]
            lifts.append(pltpu.make_async_copy(here, spare.at[block], local_ref.at[3 + block]))
        for lift in lifts:
            lift.start()
        for lift in lifts:
            lift.wait()
        out = team_copies(base, lambda p, o: spare, lambda p, o: reps.at[member])
        for copy in out:
            copy.start()
        keep = pltpu.make_async_copy(spare, reps.at[member], local_ref.at[3])
        keep.start()
        return out, keep

    forward_on(pieces_b, 1)
    gather.arrive(pieces_a, 2)
    out_a, keep_a = pass_on(early, early_ref, early_rep_ref, spare_a_ref, 4)
    gather.arrive(pieces_b, 2)
    for copy in out_a:
        copy.wait_recv()
    for copy in out_a + swaps + grads + more + sent_a + sent_b:
        copy.wait_send()
    gather.drain(pieces_a + pieces_b)
    keep_a.wait()
    result.wait()


def backward(dims, team, early, late, operands):
    _, _, io_whole, _, _, conv_out, x_own = operands[:7]
    count = dims[0] * dims[1] * dims[2]
    own, width = x_own.shape
    length, channels = conv_out.shape
    lanes = sum(d - 1 for d in dims)
    bf16, f32 = jnp.bfloat16, jnp.float32
    anywhere = pl.BlockSpec(memory_space=pl.ANY)
    vmem = pl.BlockSpec(memory_space=pltpu.VMEM)
    rows = ADAPTER_COUNT * 16
    peers = max(team - 1, 1)
    outs = [
        ((own, width), bf16),
        (dims + (rows, early.block), bf16),
        (dims + (rows, late.block), bf16),
        ((team, early.blocks, rows, early.block), bf16),
    ]
    scratch = [
        pltpu.VMEM(dims + (io_whole.shape[4], 4 * channels), bf16),
        pltpu.VMEM((own, width), f32),
        pltpu.VMEM((length, width), bf16),
        pltpu.VMEM((length, LANES), bf16),
        pltpu.VMEM((16, length), bf16),
        pltpu.VMEM((3, length + 8, channels), f32),
        pltpu.VMEM((length, 3 * channels), bf16),
        pltpu.VMEM((2, length, LANES), bf16),
        pltpu.VMEM((ROW_TILE + 8, channels), f32),
        pltpu.VMEM((ROW_TILE + 8, channels), f32),
        pltpu.VMEM((ROW_TILE + 8, channels), f32),
        pltpu.VMEM((length, width), bf16),
        pltpu.VMEM((length, channels), bf16),
        pltpu.VMEM((length, width), bf16),
        pltpu.VMEM((2, 16, length), bf16),
        pltpu.VMEM((own, width), bf16),
        pltpu.VMEM((peers, own, width), bf16),
        pltpu.VMEM((16, 2 * width), bf16),
        pltpu.VMEM((peers, 16, 2 * width), bf16),
        pltpu.VMEM((16, count * early.block), bf16),
        pltpu.VMEM((16, count * late.block), bf16),
        pltpu.VMEM((count, 16, early.block + LANES), bf16),
        pltpu.VMEM((count, 16, late.block + LANES), bf16),
        pltpu.VMEM((count, 16, early.block + LANES), bf16),
        pltpu.VMEM((count, 16, late.block + LANES), bf16),
        pltpu.VMEM((rows, early.block), bf16),
        pltpu.VMEM((rows, late.block), bf16),
        pltpu.VMEM((early.blocks, rows, early.block), bf16),
        pltpu.VMEM((own, width), bf16),
        pltpu.SemaphoreType.DMA((12, lanes)),
        pltpu.SemaphoreType.DMA((12, lanes)),
        pltpu.SemaphoreType.DMA((2, count - 1)),
        pltpu.SemaphoreType.DMA((2, count - 1)),
        pltpu.SemaphoreType.DMA((7, peers)),
        pltpu.SemaphoreType.DMA((7, peers)),
        pltpu.SemaphoreType.DMA((max(10, 3 + early.blocks),)),
        pltpu.SemaphoreType.DMA((12,)),
    ]
    return pl.pallas_call(
        functools.partial(backward_kernel, (dims, team, width, channels, length, early, late)),
        out_shape=[jax.ShapeDtypeStruct(*o) for o in outs],
        in_specs=[anywhere] * 7 + [vmem] * (len(operands) - 7),
        out_specs=[anywhere] * 4,
        scratch_shapes=scratch,
        compiler_params=pltpu.CompilerParams(
            collective_id=1, has_side_effects=True, vmem_limit_bytes=67043328
        ),
    )(*operands)


def lagged_segments(segment_ids, lag):
    shifted = jnp.pad(segment_ids, ((0, 0), (lag, 0)), constant_values=-1)[
        :, : segment_ids.shape[1]
    ]
    return (segment_ids == shifted).astype(jnp.float32)


def pad_axis(values, axis, size):
    widths = [(0, 0)] * values.ndim
    widths[axis] = (0, size - values.shape[axis])
    return jnp.pad(values, widths)


def per_device(
    residual,
    cotangent,
    segment_ids,
    adapter_ids,
    conv_gain,
    proj_in,
    conv_taps,
    proj_out,
    ffn_gain,
    gate_up,
    proj_down,
    in_shrink,
    input_lift_weight,
    output_reduce_weight,
    output_lift_weight,
    ffn_reduce_weight,
    ffn_expand,
    down_shrink,
    down_lift_weight,
):
    own, width = residual.shape
    length = segment_ids.shape[1]
    team = length // own
    count = lax.axis_size("dp")
    dims = split_ring(count)
    rows, _, channels = proj_in.shape
    hidden = proj_down.shape[1]
    hc = HIDDEN_CHUNK
    chunks = -(-hidden // hc)
    padded = chunks * hc
    adapter = adapter_ids[0]

    in_shard = proj_in.reshape(rows, 3 * channels)
    gu_shard = pad_axis(jnp.transpose(gate_up, (1, 0, 2)), 2, padded)
    down_shard = pad_axis(proj_down, 1, padded)
    codes = ADAPTER_COUNT * ADAPTER_RANK
    in_reduce = in_shrink.reshape(width, codes)
    in_lift = input_lift_weight.reshape(codes, 3 * channels)
    out_reduce = output_reduce_weight.reshape(channels, codes)
    out_lift = output_lift_weight.reshape(codes, width)
    ffn_reduce = ffn_reduce_weight.reshape(width, 2 * codes)
    expand = pad_axis(ffn_expand.reshape(2, codes, hidden), 2, padded)
    shrink = pad_axis(down_shrink.reshape(hidden, codes), 0, padded)
    down_lift = down_lift_weight.reshape(codes, width)
    lane = jnp.arange(codes, dtype=jnp.int32)[None, :]
    row = jnp.arange(ADAPTER_RANK, dtype=jnp.int32)[:, None]
    mask = (lane // ADAPTER_RANK == adapter).astype(jnp.float32)
    pick = (lane == adapter * ADAPTER_RANK + row).astype(jnp.bfloat16)
    first_same, second_same = lagged_segments(segment_ids, 1)[0], lagged_segments(segment_ids, 2)[0]
    same = jnp.stack([first_same, second_same], axis=1)
    early = Share(count, team, 3 * padded, 3 * width)
    late = Share(count, 1, 4 * channels, 2 * width)
    (
        io_whole,
        _,
        _,
        streams,
        norm_one,
        conv_out,
        code_in,
        code_out,
        block_output,
        grad_x_two,
        ffn_flat,
    ) = forward_and_ffn(
        dims,
        team,
        early,
        (
            in_shard,
            proj_out,
            gu_shard,
            down_shard,
            residual,
            cotangent,
            expand,
            shrink,
            same,
            conv_gain.reshape(1, width),
            ffn_gain.reshape(1, width),
            conv_taps,
            in_reduce,
            in_lift,
            out_reduce,
            out_lift,
            ffn_reduce,
            down_lift,
            mask,
            pick,
        ),
    )
    grad_residual, early_sums, late_sums, early_shared = backward(
        dims,
        team,
        early,
        late,
        (
            grad_x_two,
            ffn_flat,
            io_whole,
            streams,
            norm_one,
            conv_out,
            residual,
            code_in,
            code_out,
            same,
            conv_gain.reshape(1, width),
            conv_taps,
            in_reduce,
            in_lift,
            out_reduce,
            out_lift,
            mask,
            pick,
        ),
    )

    def columns_of(sums, share):
        sums = sums.reshape(count, ADAPTER_COUNT, ADAPTER_RANK, share.block)
        return jnp.transpose(sums, (1, 2, 0, 3)).reshape(
            ADAPTER_COUNT, ADAPTER_RANK, count * share.block
        )

    def shared_columns(sums, share):
        sums = sums.reshape(team, share.blocks, ADAPTER_COUNT, ADAPTER_RANK, share.block)
        sums = jnp.transpose(sums, (2, 3, 0, 1, 4)).reshape(
            ADAPTER_COUNT, ADAPTER_RANK, team, share.blocks * share.block
        )
        skip = share.split - share.first * share.block
        return sums[..., skip : skip + share.share]

    def joined(values):
        return values.reshape(ADAPTER_COUNT, ADAPTER_RANK, team * values.shape[-1])

    def rows_first(values):
        return jnp.transpose(values, (2, 0, 1)).astype(jnp.float32)

    early_columns, late_columns = columns_of(early_sums, early), columns_of(late_sums, late)
    early_rest = joined(shared_columns(early_shared, early))
    ffn_e = jnp.stack([early_columns[..., :hidden], early_columns[..., padded : padded + hidden]])
    ffn_e = ffn_e.astype(jnp.float32)
    down_s = rows_first(early_columns[..., 2 * padded : 2 * padded + hidden])
    ffn_s = jnp.stack(
        [rows_first(early_rest[..., :width]), rows_first(early_rest[..., width : 2 * width])],
        axis=1,
    )
    down_e = early_rest[..., 2 * width :].astype(jnp.float32)
    in_e = late_columns[..., : 3 * channels].astype(jnp.float32)
    in_e = in_e.reshape(ADAPTER_COUNT, ADAPTER_RANK, 3, channels)
    out_s = rows_first(late_columns[..., 3 * channels : 4 * channels])
    in_s = rows_first(late_columns[..., 4 * channels : 4 * channels + width])
    out_e = late_columns[..., 4 * channels + width : 4 * channels + 2 * width].astype(jnp.float32)
    return (block_output, grad_residual, in_s, in_e, out_s, out_e, ffn_s, ffn_e, down_s, down_e)


def solution(mesh):
    rows = P(("dp", "tensor"), None)
    placed = (
        rows,
        rows,
        P("dp", None),
        P("dp"),
        P(),
        P("dp", None, "tensor"),
        P(None, "tensor"),
        P("dp", "tensor"),
        P(),
        P("dp", None, "tensor"),
        P("dp", "tensor"),
        P(),
        P(None, None, None, "tensor"),
        P("tensor", None, None),
        P(),
        P(),
        P(None, None, None, "tensor"),
        P("tensor", None, None),
        P(),
    )
    return jax.shard_map(
        per_device,
        mesh=mesh,
        in_specs=placed,
        out_specs=(
            rows,
            rows,
            P(),
            P(None, None, None, "tensor"),
            P("tensor", None, None),
            P(),
            P(),
            P(None, None, None, "tensor"),
            P("tensor", None, None),
            P(),
        ),
        check_vma=False,
    )
```
